32 devices in a mesh: rad: 4 (over x, core), harm: 8 (over z, y).
Axes of the slice: x: 2, y: 2, z: 4, core: 2. Of those that a mesh axis runs over, the one named last changes fastest.
Arguments:
- velocity: bfloat16 [3, 16, 2, 256, 256], P(None, 'rad', None, 'harm'), may hold values from -6 to 6
- magnetic: bfloat16 [3, 16, 2, 256, 256], P(None, 'rad', None, 'harm'), may hold values from -6 to 6
- vorticity: bfloat16 [3, 16, 2, 256, 256], P(None, 'rad', None, 'harm'), may hold values from -6 to 6
- current: bfloat16 [3, 16, 2, 256, 256], P(None, 'rad', None, 'harm'), may hold values from -6 to 6
Outputs:
- advection: bfloat16 [3, 16, 2, 256, 256], P(None, 'rad', None, 'harm')
- induction_gradient: bfloat16 [3, 16, 2, 256, 256], P(None, 'rad', None, 'harm')
- energy_spectra: float32 [2, 16, 256], P(None, 'rad')
The draws below stay inside these ranges and needn't reach their ends.
All inputs are finite; a program needn't handle non-finite values.
Results may differ from the reference program's by a relative error of at most 0.01.
Values may be sent and summed in bfloat16 or wider, within the bound.
A program may use at most 64 MiB of HBM per device.

```python
import jax
import jax.numpy as jnp
from jax import lax

L = 256
NTHETA = 384
NPHI = 768
NR = 16


def block_scale(stream_key, extent, split, low, largest):
    factor_of = 1.0
    for axis_at, parts in split:
        draws = jax.random.uniform(jax.random.fold_in(jax.random.fold_in(stream_key, 6), axis_at), (parts,), jnp.float32, low / len(split), largest / len(split))
        factor_of = factor_of * jnp.repeat(jnp.exp(draws), extent[axis_at] // parts).reshape((-1,) + (1,) * (len(extent) - 1 - axis_at))
    return factor_of


def scatter_about(own_key, dims, scale, most, shards=(), held_as=jnp.bfloat16):
    level = block_scale(own_key, dims, shards, -0.22, 0.18) if shards else 1.0
    values = jax.random.normal(own_key, dims, jnp.float32) * scale * level
    return jnp.minimum(jnp.maximum(values, -most), most).astype(held_as)


def setup_inputs(seed: int = 0) -> dict:
    splits = jax.random.split(jax.random.key(seed), 5)
    return {
        "velocity": scatter_about(splits[0], (3, NR, 2, L, L), 1.0, 6.0, ((1, 4), (3, 8))),
        "magnetic": scatter_about(splits[1], (3, NR, 2, L, L), 1.0, 6.0, ((1, 4), (3, 8))),
        "vorticity": scatter_about(splits[2], (3, NR, 2, L, L), 1.0, 6.0, ((1, 4), (3, 8))),
        "current": scatter_about(splits[3], (3, NR, 2, L, L), 1.0, 6.0, ((1, 4), (3, 8))),
    }


def north_table(order_ints, degree_count, theta_count):
    half_rows = theta_count // 2
    row_index = jnp.arange(half_rows, dtype=jnp.float32)
    angles = jnp.pi * (row_index + 0.5) / theta_count
    cosine = jnp.cos(angles)
    sine_theta = jnp.sin(angles)
    order_float = order_ints.astype(jnp.float32)[:, None]
    steps_k = jnp.arange(1, degree_count, dtype=jnp.int32)
    steps_float = steps_k.astype(jnp.float32)
    log_terms = 0.5 * jnp.log((2.0 * steps_float + 1.0) / (2.0 * steps_float))
    log_taken = jnp.where(steps_k[None, :] <= order_ints[:, None], log_terms[None, :], 0.0)
    log_start = 0.5 * jnp.log(jnp.float32(0.5)) + lax.optimization_barrier(jnp.sum(log_taken, axis=1))
    log_sector = log_start[:, None] + order_float * jnp.log(sine_theta)[None, :]
    sectoral = jnp.exp(jnp.maximum(log_sector, -60.0))
    unscale = jnp.exp(jnp.minimum(log_sector + 60.0, 0.0))
    order_col = order_ints[:, None]
    blocks = 16
    per_block = degree_count // blocks

    def advance(state_pair, block_index):
        latest, before = state_pair
        produced = []
        for inner_step in range(per_block):
            degree = block_index * per_block + inner_step
            degree_float = degree.astype(jnp.float32)
            general = degree > order_col + 1
            degree_square = degree_float * degree_float
            order_square = order_float * order_float
            ratio_upper = jnp.where(general, (4.0 * degree_square - 1.0) / jnp.where(general, degree_square - order_square, 1.0), 1.0)
            lower_degree = degree_float - 1.0
            ratio_lower = jnp.where(general, (lower_degree * lower_degree - order_square) / (4.0 * lower_degree * lower_degree - 1.0), 0.0)
            value_general = jnp.sqrt(ratio_upper) * (cosine[None, :] * latest - jnp.sqrt(ratio_lower) * before)
            first_up = jnp.sqrt(2.0 * order_float + 3.0) * cosine[None, :] * sectoral
            new_value = jnp.where(degree < order_col, 0.0, jnp.where(degree == order_col, sectoral, jnp.where(degree == order_col + 1, first_up, value_general)))
            before = latest
            latest = new_value
            produced.append(new_value)
        return ((latest, before), jnp.stack(produced))
    zero_rows = jnp.zeros((order_ints.shape[0], half_rows), jnp.float32)
    state_pair, legendre_raw = lax.scan(advance, (zero_rows, zero_rows), jnp.arange(blocks, dtype=jnp.int32))
    legendre_raw = legendre_raw.reshape(degree_count, order_ints.shape[0], half_rows)
    return jnp.transpose(legendre_raw, (1, 0, 2)) * unscale[:, None, :]

def full_table(north_rows, order_ints):
    degree_count = north_rows.shape[1]
    degrees = jnp.arange(degree_count, dtype=jnp.int32)
    parity = (degrees[None, :] + order_ints[:, None]) % 2
    sign_factor = (1 - 2 * parity).astype(jnp.float32)[:, :, None]
    return jnp.concatenate([north_rows, sign_factor * jnp.flip(north_rows, 2)], 2)

def quadrature(theta_count):
    half_rows = theta_count // 2
    row_index = jnp.arange(half_rows, dtype=jnp.float32)
    angles = jnp.pi * (row_index + 0.5) / theta_count
    wave_number = jnp.arange(1, half_rows + 1, dtype=jnp.float32)
    series = jnp.cos(2.0 * wave_number[None, :] * angles[:, None]) / (4.0 * wave_number[None, :] * wave_number[None, :] - 1.0)
    north_weights = 2.0 / theta_count * (1.0 - 2.0 * lax.optimization_barrier(jnp.sum(series, axis=1)))
    return jnp.concatenate([north_weights, jnp.flip(north_weights, 0)], 0)

def trig_table(degree_count, phi_count):
    orders = jnp.arange(degree_count, dtype=jnp.int32)[:, None]
    points = jnp.arange(phi_count, dtype=jnp.int32)[None, :]
    phase_angle = 2.0 * jnp.pi * (orders * points % phi_count).astype(jnp.float32) / phi_count
    return jnp.stack([jnp.cos(phase_angle), jnp.sin(phase_angle)]).astype(jnp.bfloat16)

def analysis_factor(order_ints, row_weights, degree_count, phi_count):
    mode_weight = jnp.where(order_ints == 0, 1.0, 2.0).astype(jnp.float32)
    return mode_weight[:, None] * float(degree_count) * row_weights[None, :] / float(phi_count)

def energy_weights(order_ints, degree_count):
    degrees = jnp.arange(degree_count, dtype=jnp.int32)
    order_col = order_ints[:, None]
    live_part = (degrees[None, :] >= order_col).astype(jnp.float32)
    inverse_modes = 1.0 / (2.0 * degrees.astype(jnp.float32) + 1.0)
    cosine_weight = jnp.where(order_col == 0, 0.5, 1.0)
    sine_weight = jnp.where(order_col == 0, 0.0, 1.0)
    return jnp.stack([cosine_weight * live_part * inverse_modes[None, :], sine_weight * live_part * inverse_modes[None, :]]).astype(jnp.float32)

def cross_product(first_vec, second_vec):
    return [first_vec[1] * second_vec[2] - first_vec[2] * second_vec[1], first_vec[2] * second_vec[0] - first_vec[0] * second_vec[2], first_vec[0] * second_vec[1] - first_vec[1] * second_vec[0]]

def nonlinear_terms(components):
    velocity_vec = components[0:3]
    magnetic_vec = components[3:6]
    vorticity_vec = components[6:9]
    current_vec = components[9:12]
    lamb_term = cross_product(velocity_vec, vorticity_vec)
    lorentz_term = cross_product(current_vec, magnetic_vec)
    induced = cross_product(velocity_vec, magnetic_vec)
    return [lamb_term[index_c] + lorentz_term[index_c] for index_c in range(3)] + induced

def rounded(values):
    return lax.optimization_barrier(values.astype(jnp.bfloat16)).astype(jnp.float32)

def reference(velocity, magnetic, vorticity, current):
    all_orders = jnp.arange(L, dtype=jnp.int32)
    north_rows = north_table(all_orders, L, NTHETA)
    legendre = rounded(full_table(north_rows, all_orders))
    trig_rows = lax.optimization_barrier(trig_table(L, NPHI)).astype(jnp.float32)
    factor = analysis_factor(all_orders, quadrature(NTHETA), L, NPHI)
    energy_weight = energy_weights(all_orders, L)
    fields = jnp.concatenate([velocity, magnetic, vorticity, current], 0)
    per_shell = jnp.moveaxis(fields, 1, 0)

    def one_shell(spectrum):
        mode_rows = jnp.einsum('crml,mlt->crmt', spectrum.astype(jnp.float32), legendre) * (1.0 / L)
        mode_rows = rounded(mode_rows)
        grid_values = jnp.einsum('crmt,rmp->ctp', mode_rows, trig_rows)
        products = rounded(jnp.stack(nonlinear_terms([grid_values[index_c] for index_c in range(12)])))
        analysed = jnp.einsum('ctp,rmp->crmt', products, trig_rows) * factor[None, None]
        analysed = rounded(analysed)
        spectra = jnp.einsum('crmt,mlt->crml', analysed, legendre)
        square = spectrum[:6].astype(jnp.float32) ** 2
        kinetic = lax.optimization_barrier(jnp.sum(square[:3] * energy_weight[None], axis=(0, 1, 2)))
        magnetic_energy = lax.optimization_barrier(jnp.sum(square[3:] * energy_weight[None], axis=(0, 1, 2)))
        return (spectra[:3].astype(jnp.bfloat16), spectra[3:].astype(jnp.bfloat16), jnp.stack([kinetic, magnetic_energy]))
    advection, induction, energy = lax.map(one_shell, per_shell)
    induction_wide = induction.astype(jnp.float32)
    padded = jnp.pad(induction_wide, ((1, 1), (0, 0), (0, 0), (0, 0), (0, 0)))
    gradient = ((padded[2:] - padded[:-2]) * 0.5).astype(jnp.bfloat16)
    return (jnp.moveaxis(advection, 0, 1), jnp.moveaxis(gradient, 0, 1), jnp.moveaxis(energy, 0, 1))
```

```python
import functools

import jax
import jax.numpy as jnp
import numpy as np
from jax import lax
from jax.experimental import pallas as pl
from jax.experimental.pallas import tpu as pltpu
from jax.sharding import PartitionSpec as P

MESH = pl.DeviceIdType.MESH
PASSES = 2
BF = jnp.bfloat16
F32 = jnp.float32


def tables(degrees, thetas, points, harm_count):
    half = thetas // 2
    angles = np.pi * (np.arange(half) + 0.5) / thetas
    cosine = np.concatenate([np.cos(angles), -np.cos(angles)[::-1]])
    sine = np.concatenate([np.sin(angles), np.sin(angles)[::-1]])
    orders = np.arange(degrees)
    steps = np.arange(1, degrees)
    terms = 0.5 * np.log((2.0 * steps + 1.0) / (2.0 * steps))
    start = 0.5 * np.log(0.5) + np.concatenate([[0.0], np.cumsum(terms)])
    log_sector = start[:, None] + orders[:, None] * np.log(sine)[None, :]
    sectoral = np.exp(np.maximum(log_sector, -60.0)).astype(np.float32)
    unscale = np.exp(np.minimum(log_sector + 60.0, 0.0)).astype(np.float32)
    wave = np.arange(1, half + 1)
    series = np.cos(2.0 * wave[None, :] * angles[:, None]) / (4.0 * wave[None, :] ** 2 - 1.0)
    north = 2.0 / thetas * (1.0 - 2.0 * series.sum(axis=1))
    weights = np.concatenate([north, north[::-1]])
    weights = (weights * degrees / points).astype(np.float32)
    phase = 2.0 * np.pi * ((orders[:, None] * np.arange(points)[None, :]) % points) / points
    trig = np.stack([np.cos(phase), np.sin(phase)])
    trig = trig.reshape(2, harm_count, degrees // harm_count, points)
    trig = trig.transpose(1, 0, 2, 3).reshape(2 * degrees, points).astype(jnp.bfloat16)
    doubled = np.where(orders == 0, 1.0, 2.0).reshape(harm_count, 1, -1)
    doubled = np.broadcast_to(doubled, (harm_count, 2, degrees // harm_count)).reshape(-1, 1)
    analysis = (trig.astype(np.float32) * doubled).astype(jnp.bfloat16)
    return cosine.astype(np.float32), sectoral, unscale, weights, trig.T.copy(), analysis


def wide(column, width):
    return jnp.concatenate([column] * (width // column.shape[1]), axis=1)


def kernel(
    dims,
    cm_ref, x_ref, sect_ref, unscale_ref, w_ref, trig_ref, back_ref, energy_ref,
    out_ref, energy_out,
    tab, rows, outs, send, recv, grid, prod, send2, recv2, folded, spread, energy_all,
    ssem, rsem, ssem2, rsem2, esend, erecv,
):
    harm, shells, groups, modes, degrees, thetas, points, span = dims
    me = lax.axis_index("harm")
    pair_width = 2 * span
    block = min(16, modes)
    q_pairs = 6 // PASSES
    q_rows = 12 // PASSES * shells * 2

    barrier = pltpu.get_barrier_semaphore()
    for step in range(1, harm):
        peer = lax.rem(me + step, harm)
        pl.semaphore_signal(barrier, inc=1, device_id={"harm": peer}, device_id_type=MESH)

    order = (me * modes + lax.broadcasted_iota(jnp.int32, (modes, 128), 0)).astype(F32)
    order_square = order * order
    own = pl.ds(pl.multiple_of(me * modes, modes), modes)
    energy_all[me] = energy_ref[...]

    def table_block(step, carry):
        latest, before, inverse = carry
        for inner in range(16):
            degree = step * 16 + inner
            lf = jnp.full((modes, 128), degree, jnp.int32).astype(F32)
            dd = jnp.maximum(lf * lf - order_square, 1.0) / (4.0 * lf * lf - 1.0)
            guess = lax.rsqrt(dd)
            guess = guess * (1.5 - 0.5 * dd * guess * guess)
            live = lf > order
            alpha = jnp.where(live, guess, 0.0)
            starts = jnp.where(lf == order, 1.0, 0.0)
            new = wide(alpha, thetas) * (x_ref[...] * latest - wide(inverse, thetas) * before)
            new = new + wide(starts, thetas) * sect_ref[own, :]
            rows[inner] = new * unscale_ref[own, :]
            before, latest = latest, new
            inverse = jnp.where(live, dd * guess, 0.0)
        tab[:, pl.ds(pl.multiple_of(step * 16, 16), 16), :] = jnp.swapaxes(rows[...], 0, 1).astype(BF)
        return latest, before, inverse

    zero = jnp.zeros((modes, thetas), F32)
    lax.fori_loop(0, degrees // 16, table_block, (zero, zero, jnp.zeros((modes, 128), F32)))

    pl.semaphore_wait(barrier, harm - 1)

    def energy_copy(step):
        peer = lax.rem(me + step, harm)
        return pltpu.make_async_remote_copy(
            src_ref=energy_all.at[me], dst_ref=energy_all.at[me],
            send_sem=esend.at[step], recv_sem=erecv.at[step],
            device_id={"harm": peer}, device_id_type=MESH,
        )

    def forward(q, step):
        peer = lax.rem(me + step, harm)
        return pltpu.make_async_remote_copy(
            src_ref=send.at[peer, pl.ds(q * q_pairs, q_pairs)],
            dst_ref=recv.at[me, pl.ds(q * q_pairs, q_pairs)],
            send_sem=ssem.at[q, step], recv_sem=rsem.at[q, step],
            device_id={"harm": peer}, device_id_type=MESH,
        )

    def backward(pair, step):
        peer = lax.rem(me + step, harm)
        return pltpu.make_async_remote_copy(
            src_ref=send2.at[peer, pair], dst_ref=recv2.at[me, pair],
            send_sem=ssem2.at[pair, step], recv_sem=rsem2.at[pair, step],
            device_id={"harm": peer}, device_id_type=MESH,
        )

    for q in range(PASSES):
        def mode_block(mb, _, q=q):
            def one(i, _):
                m = mb * block + i
                outs[i] = jnp.dot(cm_ref[q, m], tab[m], preferred_element_type=F32) * (1.0 / degrees)
                return 0

            lax.fori_loop(0, block, one, 0, unroll=4)
            turned = jnp.swapaxes(outs[...], 0, 1)
            for s in range(shells):
                for pair in range(q_pairs):
                    for r in range(2):
                        k = (pair * 2 * shells + s) * 2 + r
                        first, second = turned[k], turned[k + 2 * shells]
                        for g in range(groups):
                            cut = slice(g * span, (g + 1) * span)
                            piece = jnp.concatenate([first[:, cut], second[:, cut]], axis=1).astype(BF)
                            at = pl.multiple_of(r * modes + mb * block, block)
                            send[s * groups + g, q * q_pairs + pair, pl.ds(at, block), :] = piece
            return 0

        lax.fori_loop(0, modes // block, mode_block, 0)
        for step in range(1, harm):
            forward(q, step).start()
        recv[me, pl.ds(q * q_pairs, q_pairs)] = send[me, pl.ds(q * q_pairs, q_pairs)]
    for step in range(1, harm):
        energy_copy(step).start()

    chunk = points // 3
    for q in range(PASSES):
        for step in range(1, harm):
            forward(q, step).wait_recv()
        for pair in range(q * q_pairs, (q + 1) * q_pairs):
            arrived = recv[:, pair].reshape(2 * degrees, pair_width)
            for part in range(3):
                cut = pl.ds(part * chunk, chunk)
                grid[pair, cut, :] = jnp.dot(trig_ref[cut, :], arrived, preferred_element_type=F32)

    piece_rows = 32

    def product_rows(i, _):
        at = pl.ds(pl.multiple_of(i * piece_rows, piece_rows), piece_rows)
        both = [grid[pair, at, :] for pair in range(6)]
        c = []
        for pair in range(6):
            c += [both[pair][:, :span], both[pair][:, span:]]
        u, b, w, j = c[0:3], c[3:6], c[6:9], c[9:12]

        def cross(a, d):
            return [a[1] * d[2] - a[2] * d[1], a[2] * d[0] - a[0] * d[2], a[0] * d[1] - a[1] * d[0]]

        lamb, lorentz, induced = cross(u, w), cross(j, b), cross(u, b)
        six = [lamb[n] + lorentz[n] for n in range(3)] + induced
        for pair in range(3):
            prod[pair, at, :] = jnp.concatenate([six[2 * pair], six[2 * pair + 1]], axis=1).astype(BF)
        return 0

    lax.fori_loop(0, points // piece_rows, product_rows, 0)

    per = 2 * modes
    for pair in range(3):
        analysed = jnp.dot(back_ref[...], prod[pair], preferred_element_type=F32)
        analysed = (analysed * w_ref[lax.rem(me, groups)]).astype(BF)
        send2[:, pair] = analysed.reshape(harm, per, pair_width)
        for step in range(1, harm):
            backward(pair, step).start()
        recv2[me, pair] = send2[me, pair]

    for pair in range(3):
        for step in range(1, harm):
            backward(pair, step).wait_recv()

        def fold_block(mb, _, pair=pair):
            for s in range(shells):
                for r in range(2):
                    at = pl.ds(pl.multiple_of(r * modes + mb * block, block), block)
                    got = [recv2[s * groups + g, pair, at, :].astype(F32) for g in range(groups)]
                    for c in range(2):
                        cut = slice(c * span, (c + 1) * span)
                        spread[(c * shells + s) * 2 + r] = jnp.concatenate([v[:, cut] for v in got], axis=1)
            here = pl.ds(pl.multiple_of(mb * block, block), block)
            folded[here, pl.ds(pair * 4 * shells, 4 * shells), :] = jnp.swapaxes(spread[...], 0, 1).astype(BF)
            return 0

        lax.fori_loop(0, modes // block, fold_block, 0)

    def spectrum(m, _):
        out_ref[m] = lax.dot_general(
            folded[m], tab[m], (((1,), (1,)), ((), ())), preferred_element_type=F32
        ).astype(BF)
        return 0

    lax.fori_loop(0, modes, spectrum, 0, unroll=4)

    for step in range(1, harm):
        energy_copy(step).wait_recv()
    energy_out[...] = jnp.sum(energy_all[...], axis=0)
    for step in range(1, harm):
        energy_copy(step).wait_send()
        for q in range(PASSES):
            forward(q, step).wait_send()
        for pair in range(3):
            backward(pair, step).wait_send()


def with_halo(block, axis):
    count = lax.axis_size(axis)
    up = [(i, i + 1) for i in range(count - 1)]
    down = [(b, a) for a, b in up]
    low = lax.ppermute(block[:, -1:], axis, up)
    high = lax.ppermute(block[:, :1], axis, down)
    return jnp.concatenate([low, block, high], axis=1)


def energy_weights(order_ints, degree_count):
    degrees = jnp.arange(degree_count, dtype=jnp.int32)
    order_col = order_ints[:, None]
    live_part = (degrees[None, :] >= order_col).astype(F32)
    inverse_modes = 1.0 / (2.0 * degrees.astype(F32) + 1.0)
    cosine_weight = jnp.where(order_col == 0, 0.5, 1.0)
    sine_weight = jnp.where(order_col == 0, 0.0, 1.0)
    scaled = live_part * inverse_modes[None, :]
    return jnp.stack([cosine_weight * scaled, sine_weight * scaled])


def local(velocity, magnetic, vorticity, current):
    harm = lax.axis_size("harm")
    me = lax.axis_index("harm")
    _, shells, _, modes, degrees = velocity.shape
    thetas, points = 3 * degrees // 2, 3 * degrees
    groups = harm // shells
    span = thetas // groups
    cosine, sectoral, unscale, weights, synthesis, analysis = tables(degrees, thetas, points, harm)

    own = me * modes + jnp.arange(modes, dtype=jnp.int32)
    energy_weight = energy_weights(own, degrees)
    energy = jnp.stack([
        jnp.sum(field.astype(F32) ** 2 * energy_weight[None, None], axis=(0, 2, 3))
        for field in (velocity, magnetic)
    ])

    fields = jnp.concatenate([velocity, magnetic, vorticity, current], axis=0)
    q_rows = 12 // PASSES * shells * 2
    cm = fields.reshape(PASSES, q_rows, modes, degrees).transpose(0, 2, 1, 3)
    x = jnp.asarray(np.broadcast_to(cosine[None, :], (modes, thetas)).copy())
    cut_weights = weights.reshape(groups, 1, span)
    w = jnp.asarray(np.concatenate([cut_weights, cut_weights], axis=2))

    block = min(16, modes)
    vmem = pl.BlockSpec(memory_space=pltpu.VMEM)
    dims = (harm, shells, groups, modes, degrees, thetas, points, span)
    spectra, total = pl.pallas_call(
        functools.partial(kernel, dims),
        name="dynamo",
        out_shape=(
            jax.ShapeDtypeStruct((modes, 12 * shells, degrees), BF),
            jax.ShapeDtypeStruct((2, shells, degrees), F32),
        ),
        in_specs=[vmem] * 8,
        out_specs=(vmem, vmem),
        scratch_shapes=[
            pltpu.VMEM((modes, degrees, thetas), BF),
            pltpu.VMEM((16, modes, thetas), F32),
            pltpu.VMEM((block, q_rows, thetas), F32),
            pltpu.VMEM((harm, 6, 2 * modes, 2 * span), BF),
            pltpu.VMEM((harm, 6, 2 * modes, 2 * span), BF),
            pltpu.VMEM((6, points, 2 * span), F32),
            pltpu.VMEM((3, points, 2 * span), BF),
            pltpu.VMEM((harm, 3, 2 * modes, 2 * span), BF),
            pltpu.VMEM((harm, 3, 2 * modes, 2 * span), BF),
            pltpu.VMEM((modes, 12 * shells, thetas), BF),
            pltpu.VMEM((4 * shells, block, thetas), F32),
            pltpu.VMEM((harm, 2, shells, degrees), F32),
            pltpu.SemaphoreType.DMA((PASSES, harm)),
            pltpu.SemaphoreType.DMA((PASSES, harm)),
            pltpu.SemaphoreType.DMA((3, harm)),
            pltpu.SemaphoreType.DMA((3, harm)),
            pltpu.SemaphoreType.DMA((harm,)),
            pltpu.SemaphoreType.DMA((harm,)),
        ],
        compiler_params=pltpu.CompilerParams(
            collective_id=0, has_side_effects=True, vmem_limit_bytes=60 * 1024 * 1024
        ),
    )(cm, x, jnp.asarray(sectoral), jnp.asarray(unscale), w, jnp.asarray(synthesis), jnp.asarray(analysis), energy)

    spectra = spectra.transpose(1, 0, 2).reshape(6, shells, 2, modes, degrees)
    rimmed = with_halo(spectra[3:], "rad").astype(F32)
    gradient = ((rimmed[:, 2:] - rimmed[:, :-2]) * 0.5).astype(BF)
    return spectra[:3], gradient, total


LANES = 128


def relay_tables(degrees, thetas, points, groups):
    half = thetas // 2
    rows = half // groups
    wide_rows = -(-rows // LANES) * LANES
    cosine, sectoral, unscale, weights, _, _ = tables(degrees, thetas, points, groups)

    def cut(array):
        parts = array[:, :half].reshape(-1, groups, rows).transpose(1, 0, 2)
        return np.pad(parts, ((0, 0), (0, 0), (0, wide_rows - rows)))

    x = cut(np.broadcast_to(cosine[None, :], (8, thetas)))
    w = np.tile(cut(np.broadcast_to(weights[None, :], (8, thetas))), (1, 1, 2))
    orders = np.arange(degrees)
    phase = 2.0 * np.pi * ((orders[:, None] * np.arange(points // 2)[None, :]) % points) / points
    trig = np.stack([np.cos(phase), np.sin(phase)]).astype(jnp.bfloat16).astype(np.float32)
    trig = trig.reshape(2, degrees // 2, 2, points // 2).transpose(2, 0, 1, 3)
    trig = trig.reshape(2, degrees, points // 2)
    doubled = np.where(orders == 0, 1.0, 2.0).reshape(degrees // 2, 2).T
    doubled = np.concatenate([doubled, doubled], axis=1)[:, :, None]
    synthesis = (trig.transpose(0, 2, 1) / degrees).astype(jnp.bfloat16)
    analysis = (trig * doubled).astype(jnp.bfloat16)
    return x, cut(sectoral), cut(unscale), w, synthesis, analysis


def cross(a, d):
    return [a[1] * d[2] - a[2] * d[1], a[2] * d[0] - a[0] * d[2], a[0] * d[1] - a[1] * d[0]]


def relay_kernel(
    dims,
    vel_ref, mag_ref, vor_ref, cur_ref, x_ref, sect_ref, unscale_ref, w_ref, trig_ref, back_ref, energy_ref,
    adv_ref, grad_ref, energy_out,
    tab, rows, rx, cs, outs, modes_buf, grid, prod, asc, souts, own, ysend, yrecv, zsend, land, halo, energy_all,
    lsem, zss, zrs, rss, rrs, yss, yrs, bss, brs, hss, hrs, esend, erecv,
):
    rads, harm, shells, groups, modes, degrees, thetas, points = dims
    me = lax.axis_index("harm")
    rad = lax.axis_index("rad")
    z, y = me // groups, me % groups
    other = 1 - y
    block = groups * modes
    top = degrees // 2
    fields = (vel_ref, mag_ref, vor_ref, cur_ref)
    low_half = [src * block < top for src in range(shells)]

    def at(zz, yy):
        return {"harm": zz * groups + yy}

    rad_up = {"rad": lax.rem(rad + 1, rads)}
    rad_down = {"rad": lax.rem(rad + rads - 1, rads)}

    barrier = pltpu.get_barrier_semaphore()
    for step in range(1, harm):
        pl.semaphore_signal(barrier, inc=1, device_id={"harm": lax.rem(me + step, harm)}, device_id_type=MESH)
    for target in (rad_up, rad_down):
        pl.semaphore_signal(barrier, inc=1, device_id=target, device_id_type=MESH)

    def lanes(low):
        return pl.ds(0, degrees) if low else pl.ds(top, degrees - top)

    def zcopy(f, dest, low, source):
        return pltpu.make_async_remote_copy(
            src_ref=fields[f].at[:, dest, :, :, lanes(low)],
            dst_ref=rx.at[source * groups + y, f, :, :, :, lanes(low)],
            send_sem=zss.at[dest, f], recv_sem=zrs.at[source, f],
            device_id=at(dest, y), device_id_type=MESH,
        )

    def relay_own(f, low):
        return pltpu.make_async_remote_copy(
            src_ref=fields[f].at[:, z, :, :, lanes(low)],
            dst_ref=rx.at[me, f, :, :, :, lanes(low)],
            send_sem=rss.at[z, f], recv_sem=rrs.at[z, f],
            device_id=at(z, other), device_id_type=MESH,
        )

    def relay(f, source, yy):
        slot = rx.at[source * groups + yy, f, :, :, :, lanes(low_half[source])]
        return pltpu.make_async_remote_copy(
            src_ref=slot, dst_ref=slot,
            send_sem=rss.at[source, f], recv_sem=rrs.at[source, f],
            device_id=at(z, other), device_id_type=MESH,
        )

    def local_copy(f):
        return pltpu.make_async_copy(fields[f].at[:, z], rx.at[me, f], lsem.at[f])

    for f in range(4):
        local_copy(f).start()
    energy_all[me] = energy_ref[...]
    pl.semaphore_wait(barrier, harm - 1 + 2)

    def dest_of(j):
        mark = shells - 1 - j
        return mark - jnp.where(mark <= z, 1, 0)

    for low in (True, False):
        @pl.when((z * block < top) == low)
        def _(low=low):
            for j in range(shells - 1):
                for f in range(4):
                    zcopy(f, dest_of(j), low, z).start()
            for f in range(4):
                relay_own(f, low).start()

    def energy_copy(step):
        peer = lax.rem(me + step, harm)
        return pltpu.make_async_remote_copy(
            src_ref=energy_all.at[me], dst_ref=energy_all.at[me],
            send_sem=esend.at[step], recv_sem=erecv.at[step],
            device_id={"harm": peer}, device_id_type=MESH,
        )

    for step in range(1, harm):
        energy_copy(step).start()

    def pass_on(source, f):
        zcopy(f, source, low_half[source], source).wait_recv()
        relay(f, source, y).start()

    early = z * (shells - 1 - z) == 0

    def pass_early(source, f):
        @pl.when(jnp.logical_and(early, z != source))
        def _():
            pass_on(source, f)

    def pass_late(source, f):
        @pl.when(jnp.logical_and(jnp.logical_not(early), z != source))
        def _():
            pass_on(source, f)

    x = x_ref[y, 0:1, :]
    width = x.shape[1]
    per = 16

    def table_block(source, starting, step, carry):
        first = source * block
        order = (first + lax.broadcasted_iota(jnp.int32, (block, width), 0)).astype(F32)
        square = order * order
        latest, before, inverse = carry
        for inner in range(per):
            degree = step * per + inner
            lf = jnp.full((1, width), degree, jnp.int32).astype(F32)
            scale = 1.0 / (4.0 * lf * lf - 1.0)
            gap = lf * lf - square
            if starting:
                gap = jnp.maximum(gap, 1.0)
            dd = gap * scale
            guess = lax.rsqrt(dd)
            guess = guess * (1.5 - 0.5 * dd * guess * guess)
            root = dd * guess
            if starting:
                live = lf > order
                guess = jnp.where(live, guess, 0.0)
                root = jnp.where(live, root, 0.0)
            new = guess * (x * latest - inverse * before)
            if starting:
                new = new + jnp.where(lf == order, sect_ref[y, pl.ds(first, block), :], 0.0)
            rows[inner] = new * unscale_ref[y, pl.ds(first, block), :]
            before, latest = latest, new
            inverse = root
        here = pl.ds(pl.multiple_of(step * per, per), per)
        tab[pl.ds(first, block), here, :] = jnp.swapaxes(rows[...], 0, 1).astype(BF)
        return latest, before, inverse

    def table_start(source):
        first = source * block
        floor = 0 if low_half[source] else top
        if first > floor:
            tab[pl.ds(first, block), pl.ds(floor, first - floor), :] = jnp.zeros((block, first - floor, width), BF)
        zero = jnp.zeros((block, width), F32)
        return lax.fori_loop(
            first // per, (first + block) // per, functools.partial(table_block, source, True), (zero, zero, zero))

    def table_rest(source, carry, low, high):
        return lax.fori_loop(low, high, functools.partial(table_block, source, False), carry)

    steps = degrees // per
    for source in reversed(range(shells)):
        first = (source + 1) * block // per
        carry = table_start(source)
        if low_half[source]:
            count = 4
            edges = [first + (steps - first) * i // count for i in range(count + 1)]
            for f in range(count):
                carry = table_rest(source, carry, edges[f], edges[f + 1])
                pass_early(source, f)
        else:
            table_rest(source, carry, first, steps)
            for f in range(4):
                @pl.when(z != source)
                def _(f=f):
                    pass_on(source, f)
    for f in range(4):
        for source in reversed(range(shells)):
            if low_half[source]:
                pass_late(source, f)

    lane = lax.broadcasted_iota(jnp.int32, (24, degrees), 1) % 2
    half_modes = modes // 2

    def transform(b, low):
        cut = slice(0, degrees) if low else slice(top, degrees)
        cs[:, :, cut] = jnp.swapaxes(
            rx[b].reshape(24, modes, degrees)[:, :, cut].astype(F32), 0, 1)
        for par in range(2):
            for i in range(half_modes):
                c = cs[2 * i + par, :, cut]
                even = lane[:, cut] == par
                left = jnp.concatenate([jnp.where(even, c, 0.0), jnp.where(even, 0.0, c)], axis=0).astype(BF)
                m = b * modes + 2 * i + par
                eo = jnp.dot(left, tab[m, cut, :], preferred_element_type=F32)
                outs[i] = jnp.concatenate([eo[:24] + eo[24:], eo[:24] - eo[24:]], axis=1)
            turned = jnp.swapaxes(outs[...], 0, 1).astype(BF)
            for k in range(24):
                c, r = k // 2, k % 2
                here = pl.ds(pl.multiple_of(r * top + b * half_modes, half_modes), half_modes)
                modes_buf[par, c, here, :] = turned[k]

    for f in range(4):
        local_copy(f).wait()
    for source in reversed(range(shells)):
        for f in range(4):
            relay(f, source, other).wait_recv()

        def both(yy, _, source=source):
            transform(source * groups + yy, low_half[source])
            return 0

        lax.fori_loop(0, groups, both, 0)

    def synth(c, _):
        for par in range(2):
            grid[par, c] = jnp.dot(trig_ref[par], modes_buf[par, c], preferred_element_type=F32)
        return 0

    lax.fori_loop(0, 12, synth, 0)

    piece = 16

    def product_rows(i, _):
        at_rows = pl.ds(pl.multiple_of((i // 2) * piece, piece), piece)
        at_lanes = pl.ds(pl.multiple_of((i % 2) * width, width), width)
        e = [grid[0, c, at_rows, at_lanes] for c in range(12)]
        o = [grid[1, c, at_rows, at_lanes] for c in range(12)]
        sides = []
        for g in ([a + d for a, d in zip(e, o)], [a - d for a, d in zip(e, o)]):
            u, b, w, j = g[0:3], g[3:6], g[6:9], g[9:12]
            lamb, lorentz, induced = cross(u, w), cross(j, b), cross(u, b)
            sides.append([lamb[n] + lorentz[n] for n in range(3)] + induced)
        for c in range(6):
            prod[0, c, at_rows, at_lanes] = (sides[0][c] + sides[1][c]).astype(BF)
            prod[1, c, at_rows, at_lanes] = (sides[0][c] - sides[1][c]).astype(BF)
        return 0

    lax.fori_loop(0, points // 2 // piece * 2, product_rows, 0)

    def analyse(c, _):
        for par in range(2):
            a = jnp.dot(back_ref[par], prod[par, c], preferred_element_type=F32)
            a = a * w_ref[y, 0:1, :]
            plus, minus = a[:, :width] + a[:, width:], a[:, :width] - a[:, width:]
            for r in range(2):
                cut = slice(r * top, (r + 1) * top)
                asc[par, 2 * c + r] = plus[cut]
                asc[par, 16 + 2 * c + r] = minus[cut]
        return 0

    lax.fori_loop(0, 6, analyse, 0)

    out_lane = lax.broadcasted_iota(jnp.int32, (16, degrees), 1) % 2

    def spectrum(b, low):
        cut = slice(0, degrees) if low else slice(top, degrees)
        for par in range(2):
            here = pl.ds(pl.multiple_of(b * half_modes, half_modes), half_modes)
            turned = jnp.swapaxes(asc[par, :, here, :], 0, 1).astype(BF)
            for i in range(half_modes):
                m = b * modes + 2 * i + par
                both = lax.dot_general(
                    turned[i], tab[m, cut, :], (((1,), (1,)), ((), ())), preferred_element_type=F32)
                souts[2 * i + par, :, cut] = jnp.where(out_lane[:, cut] == par, both[:16], both[16:])
        return jnp.swapaxes(souts[:, :, cut], 0, 1)[:12]

    def ycopy(target):
        low = low_half[target]
        return pltpu.make_async_remote_copy(
            src_ref=ysend.at[target, :, :, lanes(low)], dst_ref=yrecv.at[target, :, :, lanes(low)],
            send_sem=yss.at[target], recv_sem=yrs.at[target],
            device_id=at(z, other), device_id_type=MESH,
        )

    def bcopy(target, shell, low):
        return pltpu.make_async_remote_copy(
            src_ref=zsend.at[target, :, :, lanes(low)], dst_ref=land.at[shell, :, :, lanes(low)],
            send_sem=bss.at[target], recv_sem=brs.at[shell],
            device_id=at(target, y), device_id_type=MESH,
        )

    @pl.when(z * block >= top)
    def _():
        land[:, :, :, 0:top] = jnp.zeros((shells, 12, modes, top), BF)

    for target in range(shells):
        low = low_half[target]
        cut = slice(0, degrees) if low else slice(top, degrees)
        ysend[target, :, :, cut] = spectrum(target * groups + other, low).astype(BF)
        ycopy(target).start()
        own[target, :, :, cut] = spectrum(target * groups + y, low)

    for target in range(shells):
        low = low_half[target]
        cut = slice(0, degrees) if low else slice(top, degrees)
        ycopy(target).wait_recv()
        total = (own[target, :, :, cut] + yrecv[target, :, :, cut].astype(F32)).astype(BF)

        @pl.when(z == target)
        def _():
            land[target, :, :, cut] = total

        @pl.when(z != target)
        def _():
            zsend[target, :, :, cut] = total
            bcopy(target, z, low).start()

    def arrived(shell):
        for low in (True, False):
            @pl.when(jnp.logical_and(z != shell, (z * block < top) == low))
            def _(low=low):
                bcopy(shell, shell, low).wait_recv()

    def hcopy(side):
        shell = shells - 1 if side == 0 else 0
        return pltpu.make_async_remote_copy(
            src_ref=land.at[shell, pl.ds(6, 6)], dst_ref=halo.at[side],
            send_sem=hss.at[side], recv_sem=hrs.at[side],
            device_id=rad_up if side == 0 else rad_down, device_id_type=MESH,
        )

    arrived(shells - 1)
    hcopy(0).start()
    arrived(0)
    hcopy(1).start()
    for shell in range(1, shells - 1):
        arrived(shell)
    for step in range(1, harm):
        energy_copy(step).wait_recv()
    energy_out[...] = jnp.sum(energy_all[...], axis=0)
    for shell in range(shells):
        for k in range(6):
            adv_ref[k // 2, shell, k % 2] = land[shell, k]
    hcopy(0).wait_recv()
    hcopy(1).wait_recv()
    for shell in range(shells):
        for k in range(6):
            if shell > 0:
                before = land[shell - 1, 6 + k].astype(F32)
            else:
                before = jnp.where(rad > 0, halo[0, k].astype(F32), 0.0)
            if shell < shells - 1:
                after = land[shell + 1, 6 + k].astype(F32)
            else:
                after = jnp.where(rad < rads - 1, halo[1, k].astype(F32), 0.0)
            grad_ref[k // 2, shell, k % 2] = ((after - before) * 0.5).astype(BF)

    hcopy(0).wait_send()
    hcopy(1).wait_send()
    for step in range(1, harm):
        energy_copy(step).wait_send()
    for low in (True, False):
        @pl.when((z * block < top) == low)
        def _(low=low):
            for j in range(shells - 1):
                for f in range(4):
                    zcopy(f, dest_of(j), low, z).wait_send()
    for source in range(shells):
        for f in range(4):
            relay(f, source, y).wait_send()
        ycopy(source).wait_send()

        @pl.when(z != source)
        def _(source=source):
            bcopy(source, z, low_half[source]).wait_send()


def energy_parts(velocity, magnetic, own, degrees):
    energy_weight = energy_weights(own, degrees)
    return jnp.stack([
        jnp.sum(field.astype(F32) ** 2 * energy_weight[None, None], axis=(0, 2, 3))
        for field in (velocity, magnetic)
    ])


def local_relay(velocity, magnetic, vorticity, current):
    harm, rads = lax.axis_size("harm"), lax.axis_size("rad")
    me = lax.axis_index("harm")
    _, shells, _, modes, degrees = velocity.shape
    thetas, points = 3 * degrees // 2, 3 * degrees
    groups = harm // shells
    x, sect, unscale, w, synthesis, analysis = relay_tables(degrees, thetas, points, groups)
    width = x.shape[2]
    block = groups * modes
    own = me * modes + jnp.arange(modes, dtype=jnp.int32)
    energy = energy_parts(velocity, magnetic, own, degrees)
    vmem = pl.BlockSpec(memory_space=pltpu.VMEM)
    hbm = pl.BlockSpec(memory_space=pl.ANY)
    dims = (rads, harm, shells, groups, modes, degrees, thetas, points)
    result = jax.ShapeDtypeStruct(velocity.shape, BF)
    dma = pltpu.SemaphoreType.DMA
    return pl.pallas_call(
        functools.partial(relay_kernel, dims),
        name="dynamo",
        out_shape=(result, result, jax.ShapeDtypeStruct((2, shells, degrees), F32)),
        in_specs=[hbm] * 4 + [vmem] * 7,
        out_specs=(vmem, vmem, vmem),
        scratch_shapes=[
            pltpu.VMEM((degrees, degrees, width), BF),
            pltpu.VMEM((16, block, width), F32),
            pltpu.VMEM((harm, 4, 3, 2, modes, degrees), BF),
            pltpu.VMEM((modes, 24, degrees), F32),
            pltpu.VMEM((modes // 2, 24, 2 * width), F32),
            pltpu.VMEM((2, 12, degrees, 2 * width), BF),
            pltpu.VMEM((2, 12, points // 2, 2 * width), F32),
            pltpu.VMEM((2, 6, points // 2, 2 * width), BF),
            pltpu.VMEM((2, 32, degrees // 2, width), F32),
            pltpu.VMEM((modes, 16, degrees), F32),
            pltpu.VMEM((shells, 12, modes, degrees), F32),
            pltpu.VMEM((shells, 12, modes, degrees), BF),
            pltpu.VMEM((shells, 12, modes, degrees), BF),
            pltpu.VMEM((shells, 12, modes, degrees), BF),
            pltpu.VMEM((shells, 12, modes, degrees), BF),
            pltpu.VMEM((2, 6, modes, degrees), BF),
            pltpu.VMEM((harm, 2, shells, degrees), F32),
            dma((4,)), dma((shells, 4)), dma((shells, 4)), dma((shells, 4)), dma((shells, 4)),
            dma((shells,)), dma((shells,)), dma((shells,)), dma((shells,)),
            dma((2,)), dma((2,)), dma((harm,)), dma((harm,)),
        ],
        compiler_params=pltpu.CompilerParams(
            collective_id=0, has_side_effects=True, vmem_limit_bytes=62 * 1024 * 1024
        ),
    )(velocity, magnetic, vorticity, current, jnp.asarray(x), jnp.asarray(sect), jnp.asarray(unscale),
      jnp.asarray(w), jnp.asarray(synthesis), jnp.asarray(analysis), energy)


def relay_fits(mesh, args):
    _, total, _, degrees, _ = args[0].shape
    rads, harm = mesh.shape["rad"], mesh.shape["harm"]
    shells, modes = total // rads, degrees // harm
    return harm == 2 * shells and rads > 2 and modes % 32 == 0 and degrees % (2 * LANES) == 0


def solution(mesh):
    spec = P(None, "rad", None, "harm", None)

    def run(*args):
        body = local_relay if relay_fits(mesh, args) else local
        return jax.shard_map(
            body,
            mesh=mesh,
            in_specs=(spec,) * 4,
            out_specs=(spec, spec, P(None, "rad", None)),
            check_vma=False,
        )(*args)

    return run
```

```python
import functools

import jax
import jax.numpy as jnp
import numpy as np
from jax import lax
from jax.experimental import pallas as pl
from jax.experimental.pallas import tpu as pltpu
from jax.sharding import PartitionSpec as P

MESH = pl.DeviceIdType.MESH
PASSES = 2
BF = jnp.bfloat16
F32 = jnp.float32


def tables(degrees, thetas, points, harm_count):
    half = thetas // 2
    angles = np.pi * (np.arange(half) + 0.5) / thetas
    cosine = np.concatenate([np.cos(angles), -np.cos(angles)[::-1]])
    sine = np.concatenate([np.sin(angles), np.sin(angles)[::-1]])
    orders = np.arange(degrees)
    steps = np.arange(1, degrees)
    terms = 0.5 * np.log((2.0 * steps + 1.0) / (2.0 * steps))
    start = 0.5 * np.log(0.5) + np.concatenate([[0.0], np.cumsum(terms)])
    log_sector = start[:, None] + orders[:, None] * np.log(sine)[None, :]
    sectoral = np.exp(np.maximum(log_sector, -60.0)).astype(np.float32)
    unscale = np.exp(np.minimum(log_sector + 60.0, 0.0)).astype(np.float32)
    wave = np.arange(1, half + 1)
    series = np.cos(2.0 * wave[None, :] * angles[:, None]) / (4.0 * wave[None, :] ** 2 - 1.0)
    north = 2.0 / thetas * (1.0 - 2.0 * series.sum(axis=1))
    weights = np.concatenate([north, north[::-1]])
    weights = (weights * degrees / points).astype(np.float32)
    phase = 2.0 * np.pi * ((orders[:, None] * np.arange(points)[None, :]) % points) / points
    trig = np.stack([np.cos(phase), np.sin(phase)])
    trig = trig.reshape(2, harm_count, degrees // harm_count, points)
    trig = trig.transpose(1, 0, 2, 3).reshape(2 * degrees, points).astype(jnp.bfloat16)
    doubled = np.where(orders == 0, 1.0, 2.0).reshape(harm_count, 1, -1)
    doubled = np.broadcast_to(doubled, (harm_count, 2, degrees // harm_count)).reshape(-1, 1)
    analysis = (trig.astype(np.float32) * doubled).astype(jnp.bfloat16)
    return cosine.astype(np.float32), sectoral, unscale, weights, trig.T.copy(), analysis


def wide(column, width):
    return jnp.concatenate([column] * (width // column.shape[1]), axis=1)


def kernel(
    dims,
    cm_ref, x_ref, sect_ref, unscale_ref, w_ref, trig_ref, back_ref, energy_ref,
    out_ref, energy_out,
    tab, rows, outs, send, recv, grid, prod, send2, recv2, folded, spread, energy_all,
    ssem, rsem, ssem2, rsem2, esend, erecv,
):
    harm, shells, groups, modes, degrees, thetas, points, span = dims
    me = lax.axis_index("harm")
    pair_width = 2 * span
    block = min(16, modes)
    q_pairs = 6 // PASSES
    q_rows = 12 // PASSES * shells * 2

    barrier = pltpu.get_barrier_semaphore()
    for step in range(1, harm):
        peer = lax.rem(me + step, harm)
        pl.semaphore_signal(barrier, inc=1, device_id={"harm": peer}, device_id_type=MESH)

    order = (me * modes + lax.broadcasted_iota(jnp.int32, (modes, 128), 0)).astype(F32)
    order_square = order * order
    own = pl.ds(pl.multiple_of(me * modes, modes), modes)
    energy_all[me] = energy_ref[...]

    def table_block(step, carry):
        latest, before, inverse = carry
        for inner in range(16):
            degree = step * 16 + inner
            lf = jnp.full((modes, 128), degree, jnp.int32).astype(F32)
            dd = jnp.maximum(lf * lf - order_square, 1.0) / (4.0 * lf * lf - 1.0)
            guess = lax.rsqrt(dd)
            guess = guess * (1.5 - 0.5 * dd * guess * guess)
            live = lf > order
            alpha = jnp.where(live, guess, 0.0)
            starts = jnp.where(lf == order, 1.0, 0.0)
            new = wide(alpha, thetas) * (x_ref[...] * latest - wide(inverse, thetas) * before)
            new = new + wide(starts, thetas) * sect_ref[own, :]
            rows[inner] = new * unscale_ref[own, :]
            before, latest = latest, new
            inverse = jnp.where(live, dd * guess, 0.0)
        tab[:, pl.ds(pl.multiple_of(step * 16, 16), 16), :] = jnp.swapaxes(rows[...], 0, 1).astype(BF)
        return latest, before, inverse

    zero = jnp.zeros((modes, thetas), F32)
    lax.fori_loop(0, degrees // 16, table_block, (zero, zero, jnp.zeros((modes, 128), F32)))

    pl.semaphore_wait(barrier, harm - 1)

    def energy_copy(step):
        peer = lax.rem(me + step, harm)
        return pltpu.make_async_remote_copy(
            src_ref=energy_all.at[me], dst_ref=energy_all.at[me],
            send_sem=esend.at[step], recv_sem=erecv.at[step],
            device_id={"harm": peer}, device_id_type=MESH,
        )

    def forward(q, step):
        peer = lax.rem(me + step, harm)
        return pltpu.make_async_remote_copy(
            src_ref=send.at[peer, pl.ds(q * q_pairs, q_pairs)],
            dst_ref=recv.at[me, pl.ds(q * q_pairs, q_pairs)],
            send_sem=ssem.at[q, step], recv_sem=rsem.at[q, step],
            device_id={"harm": peer}, device_id_type=MESH,
        )

    def backward(pair, step):
        peer = lax.rem(me + step, harm)
        return pltpu.make_async_remote_copy(
            src_ref=send2.at[peer, pair], dst_ref=recv2.at[me, pair],
            send_sem=ssem2.at[pair, step], recv_sem=rsem2.at[pair, step],
            device_id={"harm": peer}, device_id_type=MESH,
        )

    for q in range(PASSES):
        def mode_block(mb, _, q=q):
            def one(i, _):
                m = mb * block + i
                outs[i] = jnp.dot(cm_ref[q, m], tab[m], preferred_element_type=F32) * (1.0 / degrees)
                return 0

            lax.fori_loop(0, block, one, 0, unroll=4)
            turned = jnp.swapaxes(outs[...], 0, 1)
            for s in range(shells):
                for pair in range(q_pairs):
                    for r in range(2):
                        k = (pair * 2 * shells + s) * 2 + r
                        first, second = turned[k], turned[k + 2 * shells]
                        for g in range(groups):
                            cut = slice(g * span, (g + 1) * span)
                            piece = jnp.concatenate([first[:, cut], second[:, cut]], axis=1).astype(BF)
                            at = pl.multiple_of(r * modes + mb * block, block)
                            send[s * groups + g, q * q_pairs + pair, pl.ds(at, block), :] = piece
            return 0

        lax.fori_loop(0, modes // block, mode_block, 0)
        for step in range(1, harm):
            forward(q, step).start()
        recv[me, pl.ds(q * q_pairs, q_pairs)] = send[me, pl.ds(q * q_pairs, q_pairs)]
    for step in range(1, harm):
        energy_copy(step).start()

    chunk = points // 3
    for q in range(PASSES):
        for step in range(1, harm):
            forward(q, step).wait_recv()
        for pair in range(q * q_pairs, (q + 1) * q_pairs):
            arrived = recv[:, pair].reshape(2 * degrees, pair_width)
            for part in range(3):
                cut = pl.ds(part * chunk, chunk)
                grid[pair, cut, :] = jnp.dot(trig_ref[cut, :], arrived, preferred_element_type=F32)

    piece_rows = 32

    def product_rows(i, _):
        at = pl.ds(pl.multiple_of(i * piece_rows, piece_rows), piece_rows)
        both = [grid[pair, at, :] for pair in range(6)]
        c = []
        for pair in range(6):
            c += [both[pair][:, :span], both[pair][:, span:]]
        u, b, w, j = c[0:3], c[3:6], c[6:9], c[9:12]

        def cross(a, d):
            return [a[1] * d[2] - a[2] * d[1], a[2] * d[0] - a[0] * d[2], a[0] * d[1] - a[1] * d[0]]

        lamb, lorentz, induced = cross(u, w), cross(j, b), cross(u, b)
        six = [lamb[n] + lorentz[n] for n in range(3)] + induced
        for pair in range(3):
            prod[pair, at, :] = jnp.concatenate([six[2 * pair], six[2 * pair + 1]], axis=1).astype(BF)
        return 0

    lax.fori_loop(0, points // piece_rows, product_rows, 0)

    per = 2 * modes
    for pair in range(3):
        analysed = jnp.dot(back_ref[...], prod[pair], preferred_element_type=F32)
        analysed = (analysed * w_ref[lax.rem(me, groups)]).astype(BF)
        send2[:, pair] = analysed.reshape(harm, per, pair_width)
        for step in range(1, harm):
            backward(pair, step).start()
        recv2[me, pair] = send2[me, pair]

    for pair in range(3):
        for step in range(1, harm):
            backward(pair, step).wait_recv()

        def fold_block(mb, _, pair=pair):
            for s in range(shells):
                for r in range(2):
                    at = pl.ds(pl.multiple_of(r * modes + mb * block, block), block)
                    got = [recv2[s * groups + g, pair, at, :].astype(F32) for g in range(groups)]
                    for c in range(2):
                        cut = slice(c * span, (c + 1) * span)
                        spread[(c * shells + s) * 2 + r] = jnp.concatenate([v[:, cut] for v in got], axis=1)
            here = pl.ds(pl.multiple_of(mb * block, block), block)
            folded[here, pl.ds(pair * 4 * shells, 4 * shells), :] = jnp.swapaxes(spread[...], 0, 1).astype(BF)
            return 0

        lax.fori_loop(0, modes // block, fold_block, 0)

    def spectrum(m, _):
        out_ref[m] = lax.dot_general(
            folded[m], tab[m], (((1,), (1,)), ((), ())), preferred_element_type=F32
        ).astype(BF)
        return 0

    lax.fori_loop(0, modes, spectrum, 0, unroll=4)

    for step in range(1, harm):
        energy_copy(step).wait_recv()
    energy_out[...] = jnp.sum(energy_all[...], axis=0)
    for step in range(1, harm):
        energy_copy(step).wait_send()
        for q in range(PASSES):
            forward(q, step).wait_send()
        for pair in range(3):
            backward(pair, step).wait_send()


def with_halo(block, axis):
    count = lax.axis_size(axis)
    up = [(i, i + 1) for i in range(count - 1)]
    down = [(b, a) for a, b in up]
    low = lax.ppermute(block[:, -1:], axis, up)
    high = lax.ppermute(block[:, :1], axis, down)
    return jnp.concatenate([low, block, high], axis=1)


def energy_weights(order_ints, degree_count):
    degrees = jnp.arange(degree_count, dtype=jnp.int32)
    order_col = order_ints[:, None]
    live_part = (degrees[None, :] >= order_col).astype(F32)
    inverse_modes = 1.0 / (2.0 * degrees.astype(F32) + 1.0)
    cosine_weight = jnp.where(order_col == 0, 0.5, 1.0)
    sine_weight = jnp.where(order_col == 0, 0.0, 1.0)
    scaled = live_part * inverse_modes[None, :]
    return jnp.stack([cosine_weight * scaled, sine_weight * scaled])


def local(velocity, magnetic, vorticity, current):
    harm = lax.axis_size("harm")
    me = lax.axis_index("harm")
    _, shells, _, modes, degrees = velocity.shape
    thetas, points = 3 * degrees // 2, 3 * degrees
    groups = harm // shells
    span = thetas // groups
    cosine, sectoral, unscale, weights, synthesis, analysis = tables(degrees, thetas, points, harm)

    own = me * modes + jnp.arange(modes, dtype=jnp.int32)
    energy_weight = energy_weights(own, degrees)
    energy = jnp.stack([
        jnp.sum(field.astype(F32) ** 2 * energy_weight[None, None], axis=(0, 2, 3))
        for field in (velocity, magnetic)
    ])

    fields = jnp.concatenate([velocity, magnetic, vorticity, current], axis=0)
    q_rows = 12 // PASSES * shells * 2
    cm = fields.reshape(PASSES, q_rows, modes, degrees).transpose(0, 2, 1, 3)
    x = jnp.asarray(np.broadcast_to(cosine[None, :], (modes, thetas)).copy())
    cut_weights = weights.reshape(groups, 1, span)
    w = jnp.asarray(np.concatenate([cut_weights, cut_weights], axis=2))

    block = min(16, modes)
    vmem = pl.BlockSpec(memory_space=pltpu.VMEM)
    dims = (harm, shells, groups, modes, degrees, thetas, points, span)
    spectra, total = pl.pallas_call(
        functools.partial(kernel, dims),
        name="dynamo",
        out_shape=(
            jax.ShapeDtypeStruct((modes, 12 * shells, degrees), BF),
            jax.ShapeDtypeStruct((2, shells, degrees), F32),
        ),
        in_specs=[vmem] * 8,
        out_specs=(vmem, vmem),
        scratch_shapes=[
            pltpu.VMEM((modes, degrees, thetas), BF),
            pltpu.VMEM((16, modes, thetas), F32),
            pltpu.VMEM((block, q_rows, thetas), F32),
            pltpu.VMEM((harm, 6, 2 * modes, 2 * span), BF),
            pltpu.VMEM((harm, 6, 2 * modes, 2 * span), BF),
            pltpu.VMEM((6, points, 2 * span), F32),
            pltpu.VMEM((3, points, 2 * span), BF),
            pltpu.VMEM((harm, 3, 2 * modes, 2 * span), BF),
            pltpu.VMEM((harm, 3, 2 * modes, 2 * span), BF),
            pltpu.VMEM((modes, 12 * shells, thetas), BF),
            pltpu.VMEM((4 * shells, block, thetas), F32),
            pltpu.VMEM((harm, 2, shells, degrees), F32),
            pltpu.SemaphoreType.DMA((PASSES, harm)),
            pltpu.SemaphoreType.DMA((PASSES, harm)),
            pltpu.SemaphoreType.DMA((3, harm)),
            pltpu.SemaphoreType.DMA((3, harm)),
            pltpu.SemaphoreType.DMA((harm,)),
            pltpu.SemaphoreType.DMA((harm,)),
        ],
        compiler_params=pltpu.CompilerParams(
            collective_id=0, has_side_effects=True, vmem_limit_bytes=60 * 1024 * 1024
        ),
    )(cm, x, jnp.asarray(sectoral), jnp.asarray(unscale), w, jnp.asarray(synthesis), jnp.asarray(analysis), energy)

    spectra = spectra.transpose(1, 0, 2).reshape(6, shells, 2, modes, degrees)
    rimmed = with_halo(spectra[3:], "rad").astype(F32)
    gradient = ((rimmed[:, 2:] - rimmed[:, :-2]) * 0.5).astype(BF)
    return spectra[:3], gradient, total


LANES = 128


def relay_tables(degrees, thetas, points, groups):
    half = thetas // 2
    rows = half // groups
    wide_rows = -(-rows // LANES) * LANES
    cosine, sectoral, unscale, weights, _, _ = tables(degrees, thetas, points, groups)

    def cut(array):
        parts = array[:, :half].reshape(-1, groups, rows).transpose(1, 0, 2)
        return np.pad(parts, ((0, 0), (0, 0), (0, wide_rows - rows)))

    x = cut(np.broadcast_to(cosine[None, :], (8, thetas)))
    w = np.tile(cut(np.broadcast_to(weights[None, :], (8, thetas))), (1, 1, 2))
    orders = np.arange(degrees)
    phase = 2.0 * np.pi * ((orders[:, None] * np.arange(points // 2)[None, :]) % points) / points
    trig = np.stack([np.cos(phase), np.sin(phase)]).astype(jnp.bfloat16).astype(np.float32)
    trig = trig.reshape(2, degrees // 2, 2, points // 2).transpose(2, 0, 1, 3)
    trig = trig.reshape(2, degrees, points // 2)
    doubled = np.where(orders == 0, 1.0, 2.0).reshape(degrees // 2, 2).T
    doubled = np.concatenate([doubled, doubled], axis=1)[:, :, None]
    synthesis = (trig.transpose(0, 2, 1) / degrees).astype(jnp.bfloat16)
    analysis = (trig * doubled).astype(jnp.bfloat16)
    return x, cut(sectoral), cut(unscale), w, synthesis, analysis


def cross(a, d):
    return [a[1] * d[2] - a[2] * d[1], a[2] * d[0] - a[0] * d[2], a[0] * d[1] - a[1] * d[0]]


def relay_kernel(
    dims,
    vel_ref, mag_ref, vor_ref, cur_ref, x_ref, sect_ref, unscale_ref, w_ref, trig_ref, back_ref,
    adv_ref, grad_ref, energy_out,
    tab, rows, rx, cs, outs, modes_buf, grid, prod, asc, souts, own, ysend, yrecv, zsend, land, halo, energy_all, held,
    lsem, vsem, zss, zrs, rss, rrs, yss, yrs, bss, brs, hss, hrs, esend, erecv,
):
    rads, harm, shells, groups, modes, degrees, thetas, points = dims
    me = lax.axis_index("harm")
    rad = lax.axis_index("rad")
    z, y = me // groups, me % groups
    base, core = rad // groups * groups, rad % groups
    other = 1 - core
    straight = core == y
    block = groups * modes
    top = degrees // 2
    fields = (vel_ref, mag_ref, vor_ref, cur_ref)
    low_half = [src * block < top for src in range(shells)]

    def mate(shell):
        return {"rad": base + y, "harm": shell * groups + core}

    partner = {"rad": base + other}

    rad_up = {"rad": lax.rem(rad + 1, rads)}
    rad_down = {"rad": lax.rem(rad + rads - 1, rads)}

    barrier = pltpu.get_barrier_semaphore()
    for step in range(1, harm):
        pl.semaphore_signal(barrier, inc=1, device_id={"harm": lax.rem(me + step, harm)}, device_id_type=MESH)
    for target in (rad_up, rad_down):
        pl.semaphore_signal(barrier, inc=1, device_id=target, device_id_type=MESH)

    @pl.when(jnp.logical_not(straight))
    def _():
        for shell in range(shells):
            pl.semaphore_signal(barrier, inc=1, device_id=mate(shell), device_id_type=MESH)

    def lanes(low):
        return pl.ds(0, degrees) if low else pl.ds(top, degrees - top)

    def zcopy(f, dest, low, source):
        return pltpu.make_async_remote_copy(
            src_ref=fields[f].at[:, dest, :, :, lanes(low)],
            dst_ref=rx.at[me, f, :, :, :, lanes(low)],
            send_sem=zss.at[dest, f], recv_sem=zrs.at[source, f],
            device_id=mate(dest), device_id_type=MESH,
        )

    def relay(f, source, yy):
        slot = rx.at[source * groups + yy, f, :, :, :, lanes(low_half[source])]
        return pltpu.make_async_remote_copy(
            src_ref=slot, dst_ref=slot,
            send_sem=rss.at[source, f], recv_sem=rrs.at[source, f],
            device_id=partner, device_id_type=MESH,
        )

    def local_copy(f):
        return pltpu.make_async_copy(fields[f].at[:, z], rx.at[me, f], lsem.at[f])

    def held_copy(f):
        return pltpu.make_async_copy(fields[f], held.at[f], vsem.at[f])

    for f in range(2):
        held_copy(f).start()

    @pl.when(straight)
    def _():
        for f in range(4):
            local_copy(f).start()

    pl.semaphore_wait(barrier, harm - 1 + 2 + shells * jnp.where(straight, 0, 1))

    def dest_of(j):
        mark = shells - 1 - j
        return mark - jnp.where(mark <= z, 1, 0)

    for low in (True, False):
        @pl.when((z * block < top) == low)
        def _(low=low):
            for j in range(shells - 1):
                for f in range(4):
                    zcopy(f, dest_of(j), low, z).start()

            @pl.when(jnp.logical_not(straight))
            def _():
                for f in range(4):
                    zcopy(f, z, low, z).start()

    def energy_copy(step):
        peer = lax.rem(me + step, harm)
        return pltpu.make_async_remote_copy(
            src_ref=energy_all.at[me], dst_ref=energy_all.at[me],
            send_sem=esend.at[step], recv_sem=erecv.at[step],
            device_id={"harm": peer}, device_id_type=MESH,
        )

    def pass_on(source):
        for f in range(4):
            @pl.when(jnp.logical_and(straight, z == source))
            def _(f=f):
                local_copy(f).wait()

            @pl.when(jnp.logical_not(jnp.logical_and(straight, z == source)))
            def _(f=f):
                zcopy(f, source, low_half[source], source).wait_recv()

            relay(f, source, core).start()

    x = x_ref[core, 0:1, :]
    width = x.shape[1]
    per = 16

    def table_block(source, starting, step, carry):
        first = source * block
        order = (first + lax.broadcasted_iota(jnp.int32, (block, width), 0)).astype(F32)
        square = order * order
        latest, before, inverse = carry
        for inner in range(per):
            degree = step * per + inner
            lf = jnp.full((1, width), degree, jnp.int32).astype(F32)
            scale = 1.0 / (4.0 * lf * lf - 1.0)
            gap = lf * lf - square
            if starting:
                gap = jnp.maximum(gap, 1.0)
            dd = gap * scale
            guess = lax.rsqrt(dd)
            guess = guess * (1.5 - 0.5 * dd * guess * guess)
            root = dd * guess
            if starting:
                live = lf > order
                guess = jnp.where(live, guess, 0.0)
                root = jnp.where(live, root, 0.0)
            new = guess * (x * latest - inverse * before)
            if starting:
                new = new + jnp.where(lf == order, sect_ref[core, pl.ds(first, block), :], 0.0)
            rows[inner] = new * unscale_ref[core, pl.ds(first, block), :]
            before, latest = latest, new
            inverse = root
        here = pl.ds(pl.multiple_of(step * per, per), per)
        tab[pl.ds(first, block), here, :] = jnp.swapaxes(rows[...], 0, 1).astype(BF)
        return latest, before, inverse

    def table_start(source):
        first = source * block
        floor = 0 if low_half[source] else top
        if first > floor:
            tab[pl.ds(first, block), pl.ds(floor, first - floor), :] = jnp.zeros((block, first - floor, width), BF)
        zero = jnp.zeros((block, width), F32)
        return lax.fori_loop(
            first // per, (first + block) // per, functools.partial(table_block, source, True), (zero, zero, zero))

    def table_rest(source, carry, low, high):
        return lax.fori_loop(low, high, functools.partial(table_block, source, False), carry)

    steps = degrees // per
    for source in reversed(range(shells)):
        carry = table_start(source)
        lax.fori_loop((source + 1) * block // per, steps, functools.partial(table_block, source, False), carry)

    for f in range(2):
        held_copy(f).wait()
    own_order = me * modes + lax.broadcasted_iota(jnp.int32, (modes, degrees), 0)
    degree = lax.broadcasted_iota(jnp.int32, (modes, degrees), 1)
    share = jnp.where(degree >= own_order, 1.0 / (2.0 * degree.astype(F32) + 1.0), 0.0)
    parts = (share * jnp.where(own_order == 0, 0.5, 1.0), share * jnp.where(own_order == 0, 0.0, 1.0))

    def shell_energy(shell, _):
        for f in range(2):
            total = jnp.zeros((modes, degrees), F32)
            for r in range(2):
                square = jnp.zeros((modes, degrees), F32)
                for c in range(3):
                    value = held[f, c, shell, r].astype(F32)
                    square = square + value * value
                total = total + square * parts[r]
            energy_all[me, f, pl.ds(shell, 1), :] = jnp.sum(total, axis=0, keepdims=True)
        return 0

    lax.fori_loop(0, shells, shell_energy, 0)
    for step in range(1, harm):
        energy_copy(step).start()

    lane = lax.broadcasted_iota(jnp.int32, (24, degrees), 1) % 2
    half_modes = modes // 2

    def transform(b, low):
        cut = slice(0, degrees) if low else slice(top, degrees)
        cs[:, :, cut] = jnp.swapaxes(
            rx[b].reshape(24, modes, degrees)[:, :, cut].astype(F32), 0, 1)
        for par in range(2):
            for i in range(half_modes):
                c = cs[2 * i + par, :, cut]
                even = lane[:, cut] == par
                left = jnp.concatenate([jnp.where(even, c, 0.0), jnp.where(even, 0.0, c)], axis=0).astype(BF)
                m = b * modes + 2 * i + par
                eo = jnp.dot(left, tab[m, cut, :], preferred_element_type=F32)
                outs[i] = jnp.concatenate([eo[:24] + eo[24:], eo[:24] - eo[24:]], axis=1)
            turned = jnp.swapaxes(outs[...], 0, 1).astype(BF)
            for k in range(24):
                c, r = k // 2, k % 2
                here = pl.ds(pl.multiple_of(r * top + b * half_modes, half_modes), half_modes)
                modes_buf[par, c, here, :] = turned[k]

    def partner_block(source):
        for f in range(4):
            relay(f, source, other).wait_recv()
        transform(source * groups + other, low_half[source])

    for source in reversed(range(shells)):
        pass_on(source)
        if source + 1 < shells:
            partner_block(source + 1)
        transform(source * groups + core, low_half[source])
    partner_block(0)

    def synth(c, _):
        for par in range(2):
            grid[par, c] = jnp.dot(trig_ref[par], modes_buf[par, c], preferred_element_type=F32)
        return 0

    lax.fori_loop(0, 12, synth, 0)

    piece = 16

    def product_rows(i, _):
        at_rows = pl.ds(pl.multiple_of((i // 2) * piece, piece), piece)
        at_lanes = pl.ds(pl.multiple_of((i % 2) * width, width), width)
        e = [grid[0, c, at_rows, at_lanes] for c in range(12)]
        o = [grid[1, c, at_rows, at_lanes] for c in range(12)]
        sides = []
        for g in ([a + d for a, d in zip(e, o)], [a - d for a, d in zip(e, o)]):
            u, b, w, j = g[0:3], g[3:6], g[6:9], g[9:12]
            lamb, lorentz, induced = cross(u, w), cross(j, b), cross(u, b)
            sides.append([lamb[n] + lorentz[n] for n in range(3)] + induced)
        for c in range(6):
            prod[0, c, at_rows, at_lanes] = (sides[0][c] + sides[1][c]).astype(BF)
            prod[1, c, at_rows, at_lanes] = (sides[0][c] - sides[1][c]).astype(BF)
        return 0

    lax.fori_loop(0, points // 2 // piece * 2, product_rows, 0)

    def analyse(c, _):
        for par in range(2):
            a = jnp.dot(back_ref[par], prod[par, c], preferred_element_type=F32)
            a = a * w_ref[core, 0:1, :]
            plus, minus = a[:, :width] + a[:, width:], a[:, :width] - a[:, width:]
            for r in range(2):
                cut = slice(r * top, (r + 1) * top)
                asc[par, 2 * c + r] = plus[cut]
                asc[par, 16 + 2 * c + r] = minus[cut]
        return 0

    lax.fori_loop(0, 6, analyse, 0)

    out_lane = lax.broadcasted_iota(jnp.int32, (16, degrees), 1) % 2

    def spectrum(b, low):
        cut = slice(0, degrees) if low else slice(top, degrees)
        for par in range(2):
            here = pl.ds(pl.multiple_of(b * half_modes, half_modes), half_modes)
            turned = jnp.swapaxes(asc[par, :, here, :], 0, 1).astype(BF)
            for i in range(half_modes):
                m = b * modes + 2 * i + par
                both = lax.dot_general(
                    turned[i], tab[m, cut, :], (((1,), (1,)), ((), ())), preferred_element_type=F32)
                souts[2 * i + par, :, cut] = jnp.where(out_lane[:, cut] == par, both[:16], both[16:])
        return jnp.swapaxes(souts[:, :, cut], 0, 1)[:12]

    def ycopy(target):
        low = low_half[target]
        return pltpu.make_async_remote_copy(
            src_ref=ysend.at[target, :, :, lanes(low)], dst_ref=yrecv.at[target, :, :, lanes(low)],
            send_sem=yss.at[target], recv_sem=yrs.at[target],
            device_id=partner, device_id_type=MESH,
        )

    def bcopy(target, shell, low):
        return pltpu.make_async_remote_copy(
            src_ref=zsend.at[target, :, :, lanes(low)], dst_ref=land.at[shell, :, :, lanes(low)],
            send_sem=bss.at[target], recv_sem=brs.at[shell],
            device_id=mate(target), device_id_type=MESH,
        )

    @pl.when(z * block >= top)
    def _():
        land[:, :, :, 0:top] = jnp.zeros((shells, 12, modes, top), BF)

    for target in range(shells):
        low = low_half[target]
        cut = slice(0, degrees) if low else slice(top, degrees)
        ysend[target, :, :, cut] = spectrum(target * groups + other, low).astype(BF)
        ycopy(target).start()
        own[target, :, :, cut] = spectrum(target * groups + core, low)

    for target in range(shells):
        low = low_half[target]
        cut = slice(0, degrees) if low else slice(top, degrees)
        ycopy(target).wait_recv()
        total = (own[target, :, :, cut] + yrecv[target, :, :, cut].astype(F32)).astype(BF)

        stays = jnp.logical_and(straight, z == target)

        @pl.when(stays)
        def _():
            land[target, :, :, cut] = total

        @pl.when(jnp.logical_not(stays))
        def _():
            zsend[target, :, :, cut] = total
            bcopy(target, z, low).start()

    def arrived(shell):
        for low in (True, False):
            @pl.when(jnp.logical_and(jnp.logical_not(jnp.logical_and(straight, z == shell)), (z * block < top) == low))
            def _(low=low):
                bcopy(shell, shell, low).wait_recv()

    def hcopy(side):
        shell = shells - 1 if side == 0 else 0
        return pltpu.make_async_remote_copy(
            src_ref=land.at[shell, pl.ds(6, 6)], dst_ref=halo.at[side],
            send_sem=hss.at[side], recv_sem=hrs.at[side],
            device_id=rad_up if side == 0 else rad_down, device_id_type=MESH,
        )

    arrived(shells - 1)
    hcopy(0).start()
    arrived(0)
    hcopy(1).start()
    for shell in range(1, shells - 1):
        arrived(shell)
    for step in range(1, harm):
        energy_copy(step).wait_recv()
    energy_out[...] = jnp.sum(energy_all[...], axis=0)
    for shell in range(shells):
        for k in range(6):
            adv_ref[k // 2, shell, k % 2] = land[shell, k]
    hcopy(0).wait_recv()
    hcopy(1).wait_recv()
    for shell in range(shells):
        for k in range(6):
            if shell > 0:
                before = land[shell - 1, 6 + k].astype(F32)
            else:
                before = jnp.where(rad > 0, halo[0, k].astype(F32), 0.0)
            if shell < shells - 1:
                after = land[shell + 1, 6 + k].astype(F32)
            else:
                after = jnp.where(rad < rads - 1, halo[1, k].astype(F32), 0.0)
            grad_ref[k // 2, shell, k % 2] = ((after - before) * 0.5).astype(BF)

    hcopy(0).wait_send()
    hcopy(1).wait_send()
    for step in range(1, harm):
        energy_copy(step).wait_send()
    for low in (True, False):
        @pl.when((z * block < top) == low)
        def _(low=low):
            for j in range(shells - 1):
                for f in range(4):
                    zcopy(f, dest_of(j), low, z).wait_send()

            @pl.when(jnp.logical_not(straight))
            def _():
                for f in range(4):
                    zcopy(f, z, low, z).wait_send()

    for source in range(shells):
        for f in range(4):
            relay(f, source, core).wait_send()
        ycopy(source).wait_send()

        @pl.when(jnp.logical_not(jnp.logical_and(straight, z == source)))
        def _(source=source):
            bcopy(source, z, low_half[source]).wait_send()


def local_relay(velocity, magnetic, vorticity, current):
    harm, rads = lax.axis_size("harm"), lax.axis_size("rad")
    _, shells, _, modes, degrees = velocity.shape
    thetas, points = 3 * degrees // 2, 3 * degrees
    groups = harm // shells
    x, sect, unscale, w, synthesis, analysis = relay_tables(degrees, thetas, points, groups)
    width = x.shape[2]
    block = groups * modes
    vmem = pl.BlockSpec(memory_space=pltpu.VMEM)
    hbm = pl.BlockSpec(memory_space=pl.ANY)
    dims = (rads, harm, shells, groups, modes, degrees, thetas, points)
    result = jax.ShapeDtypeStruct(velocity.shape, BF)
    dma = pltpu.SemaphoreType.DMA
    return pl.pallas_call(
        functools.partial(relay_kernel, dims),
        name="dynamo",
        out_shape=(result, result, jax.ShapeDtypeStruct((2, shells, degrees), F32)),
        in_specs=[hbm] * 4 + [vmem] * 6,
        out_specs=(vmem, vmem, vmem),
        scratch_shapes=[
            pltpu.VMEM((degrees, degrees, width), BF),
            pltpu.VMEM((16, block, width), F32),
            pltpu.VMEM((harm, 4, 3, 2, modes, degrees), BF),
            pltpu.VMEM((modes, 24, degrees), F32),
            pltpu.VMEM((modes // 2, 24, 2 * width), F32),
            pltpu.VMEM((2, 12, degrees, 2 * width), BF),
            pltpu.VMEM((2, 12, points // 2, 2 * width), F32),
            pltpu.VMEM((2, 6, points // 2, 2 * width), BF),
            pltpu.VMEM((2, 32, degrees // 2, width), F32),
            pltpu.VMEM((modes, 16, degrees), F32),
            pltpu.VMEM((shells, 12, modes, degrees), F32),
            pltpu.VMEM((shells, 12, modes, degrees), BF),
            pltpu.VMEM((shells, 12, modes, degrees), BF),
            pltpu.VMEM((shells, 12, modes, degrees), BF),
            pltpu.VMEM((shells, 12, modes, degrees), BF),
            pltpu.VMEM((2, 6, modes, degrees), BF),
            pltpu.VMEM((harm, 2, shells, degrees), F32),
            pltpu.VMEM((2,) + velocity.shape, BF),
            dma((4,)), dma((2,)), dma((shells, 4)), dma((shells, 4)), dma((shells, 4)), dma((shells, 4)),
            dma((shells,)), dma((shells,)), dma((shells,)), dma((shells,)),
            dma((2,)), dma((2,)), dma((harm,)), dma((harm,)),
        ],
        compiler_params=pltpu.CompilerParams(
            collective_id=0, has_side_effects=True, vmem_limit_bytes=62 * 1024 * 1024
        ),
    )(velocity, magnetic, vorticity, current, jnp.asarray(x), jnp.asarray(sect), jnp.asarray(unscale),
      jnp.asarray(w), jnp.asarray(synthesis), jnp.asarray(analysis))


def relay_fits(mesh, args):
    _, total, _, degrees, _ = args[0].shape
    rads, harm = mesh.shape["rad"], mesh.shape["harm"]
    shells, modes = total // rads, degrees // harm
    return harm == 2 * shells and rads > 2 and rads % 2 == 0 and modes % 32 == 0 and degrees % (2 * LANES) == 0


def solution(mesh):
    spec = P(None, "rad", None, "harm", None)

    def run(*args):
        body = local_relay if relay_fits(mesh, args) else local
        return jax.shard_map(
            body,
            mesh=mesh,
            in_specs=(spec,) * 4,
            out_specs=(spec, spec, P(None, "rad", None)),
            check_vma=False,
        )(*args)

    return run
```

```python
import functools

import jax
import jax.numpy as jnp
import numpy as np
from jax import lax
from jax.experimental import pallas as pl
from jax.experimental.pallas import tpu as pltpu
from jax.sharding import PartitionSpec as P

MESH = pl.DeviceIdType.MESH
PASSES = 2
BF = jnp.bfloat16
F32 = jnp.float32


def tables(degrees, thetas, points, harm_count):
    half = thetas // 2
    angles = np.pi * (np.arange(half) + 0.5) / thetas
    cosine = np.concatenate([np.cos(angles), -np.cos(angles)[::-1]])
    sine = np.concatenate([np.sin(angles), np.sin(angles)[::-1]])
    orders = np.arange(degrees)
    steps = np.arange(1, degrees)
    terms = 0.5 * np.log((2.0 * steps + 1.0) / (2.0 * steps))
    start = 0.5 * np.log(0.5) + np.concatenate([[0.0], np.cumsum(terms)])
    log_sector = start[:, None] + orders[:, None] * np.log(sine)[None, :]
    sectoral = np.exp(np.maximum(log_sector, -60.0)).astype(np.float32)
    unscale = np.exp(np.minimum(log_sector + 60.0, 0.0)).astype(np.float32)
    wave = np.arange(1, half + 1)
    series = np.cos(2.0 * wave[None, :] * angles[:, None]) / (4.0 * wave[None, :] ** 2 - 1.0)
    north = 2.0 / thetas * (1.0 - 2.0 * series.sum(axis=1))
    weights = np.concatenate([north, north[::-1]])
    weights = (weights * degrees / points).astype(np.float32)
    phase = 2.0 * np.pi * ((orders[:, None] * np.arange(points)[None, :]) % points) / points
    trig = np.stack([np.cos(phase), np.sin(phase)])
    trig = trig.reshape(2, harm_count, degrees // harm_count, points)
    trig = trig.transpose(1, 0, 2, 3).reshape(2 * degrees, points).astype(jnp.bfloat16)
    doubled = np.where(orders == 0, 1.0, 2.0).reshape(harm_count, 1, -1)
    doubled = np.broadcast_to(doubled, (harm_count, 2, degrees // harm_count)).reshape(-1, 1)
    analysis = (trig.astype(np.float32) * doubled).astype(jnp.bfloat16)
    return cosine.astype(np.float32), sectoral, unscale, weights, trig.T.copy(), analysis


def wide(column, width):
    return jnp.concatenate([column] * (width // column.shape[1]), axis=1)


def kernel(
    dims,
    cm_ref, x_ref, sect_ref, unscale_ref, w_ref, trig_ref, back_ref, energy_ref,
    out_ref, energy_out,
    tab, rows, outs, send, recv, grid, prod, send2, recv2, folded, spread, energy_all,
    ssem, rsem, ssem2, rsem2, esend, erecv,
):
    harm, shells, groups, modes, degrees, thetas, points, span = dims
    me = lax.axis_index("harm")
    pair_width = 2 * span
    block = min(16, modes)
    q_pairs = 6 // PASSES
    q_rows = 12 // PASSES * shells * 2

    barrier = pltpu.get_barrier_semaphore()
    for step in range(1, harm):
        peer = lax.rem(me + step, harm)
        pl.semaphore_signal(barrier, inc=1, device_id={"harm": peer}, device_id_type=MESH)

    order = (me * modes + lax.broadcasted_iota(jnp.int32, (modes, 128), 0)).astype(F32)
    order_square = order * order
    own = pl.ds(pl.multiple_of(me * modes, modes), modes)
    energy_all[me] = energy_ref[...]

    def table_block(step, carry):
        latest, before, inverse = carry
        for inner in range(16):
            degree = step * 16 + inner
            lf = jnp.full((modes, 128), degree, jnp.int32).astype(F32)
            dd = jnp.maximum(lf * lf - order_square, 1.0) / (4.0 * lf * lf - 1.0)
            guess = lax.rsqrt(dd)
            guess = guess * (1.5 - 0.5 * dd * guess * guess)
            live = lf > order
            alpha = jnp.where(live, guess, 0.0)
            starts = jnp.where(lf == order, 1.0, 0.0)
            new = wide(alpha, thetas) * (x_ref[...] * latest - wide(inverse, thetas) * before)
            new = new + wide(starts, thetas) * sect_ref[own, :]
            rows[inner] = new * unscale_ref[own, :]
            before, latest = latest, new
            inverse = jnp.where(live, dd * guess, 0.0)
        tab[:, pl.ds(pl.multiple_of(step * 16, 16), 16), :] = jnp.swapaxes(rows[...], 0, 1).astype(BF)
        return latest, before, inverse

    zero = jnp.zeros((modes, thetas), F32)
    lax.fori_loop(0, degrees // 16, table_block, (zero, zero, jnp.zeros((modes, 128), F32)))

    pl.semaphore_wait(barrier, harm - 1)

    def energy_copy(step):
        peer = lax.rem(me + step, harm)
        return pltpu.make_async_remote_copy(
            src_ref=energy_all.at[me], dst_ref=energy_all.at[me],
            send_sem=esend.at[step], recv_sem=erecv.at[step],
            device_id={"harm": peer}, device_id_type=MESH,
        )

    def forward(q, step):
        peer = lax.rem(me + step, harm)
        return pltpu.make_async_remote_copy(
            src_ref=send.at[peer, pl.ds(q * q_pairs, q_pairs)],
            dst_ref=recv.at[me, pl.ds(q * q_pairs, q_pairs)],
            send_sem=ssem.at[q, step], recv_sem=rsem.at[q, step],
            device_id={"harm": peer}, device_id_type=MESH,
        )

    def backward(pair, step):
        peer = lax.rem(me + step, harm)
        return pltpu.make_async_remote_copy(
            src_ref=send2.at[peer, pair], dst_ref=recv2.at[me, pair],
            send_sem=ssem2.at[pair, step], recv_sem=rsem2.at[pair, step],
            device_id={"harm": peer}, device_id_type=MESH,
        )

    for q in range(PASSES):
        def mode_block(mb, _, q=q):
            def one(i, _):
                m = mb * block + i
                outs[i] = jnp.dot(cm_ref[q, m], tab[m], preferred_element_type=F32) * (1.0 / degrees)
                return 0

            lax.fori_loop(0, block, one, 0, unroll=4)
            turned = jnp.swapaxes(outs[...], 0, 1)
            for s in range(shells):
                for pair in range(q_pairs):
                    for r in range(2):
                        k = (pair * 2 * shells + s) * 2 + r
                        first, second = turned[k], turned[k + 2 * shells]
                        for g in range(groups):
                            cut = slice(g * span, (g + 1) * span)
                            piece = jnp.concatenate([first[:, cut], second[:, cut]], axis=1).astype(BF)
                            at = pl.multiple_of(r * modes + mb * block, block)
                            send[s * groups + g, q * q_pairs + pair, pl.ds(at, block), :] = piece
            return 0

        lax.fori_loop(0, modes // block, mode_block, 0)
        for step in range(1, harm):
            forward(q, step).start()
        recv[me, pl.ds(q * q_pairs, q_pairs)] = send[me, pl.ds(q * q_pairs, q_pairs)]
    for step in range(1, harm):
        energy_copy(step).start()

    chunk = points // 3
    for q in range(PASSES):
        for step in range(1, harm):
            forward(q, step).wait_recv()
        for pair in range(q * q_pairs, (q + 1) * q_pairs):
            arrived = recv[:, pair].reshape(2 * degrees, pair_width)
            for part in range(3):
                cut = pl.ds(part * chunk, chunk)
                grid[pair, cut, :] = jnp.dot(trig_ref[cut, :], arrived, preferred_element_type=F32)

    piece_rows = 32

    def product_rows(i, _):
        at = pl.ds(pl.multiple_of(i * piece_rows, piece_rows), piece_rows)
        both = [grid[pair, at, :] for pair in range(6)]
        c = []
        for pair in range(6):
            c += [both[pair][:, :span], both[pair][:, span:]]
        u, b, w, j = c[0:3], c[3:6], c[6:9], c[9:12]

        def cross(a, d):
            return [a[1] * d[2] - a[2] * d[1], a[2] * d[0] - a[0] * d[2], a[0] * d[1] - a[1] * d[0]]

        lamb, lorentz, induced = cross(u, w), cross(j, b), cross(u, b)
        six = [lamb[n] + lorentz[n] for n in range(3)] + induced
        for pair in range(3):
            prod[pair, at, :] = jnp.concatenate([six[2 * pair], six[2 * pair + 1]], axis=1).astype(BF)
        return 0

    lax.fori_loop(0, points // piece_rows, product_rows, 0)

    per = 2 * modes
    for pair in range(3):
        analysed = jnp.dot(back_ref[...], prod[pair], preferred_element_type=F32)
        analysed = (analysed * w_ref[lax.rem(me, groups)]).astype(BF)
        send2[:, pair] = analysed.reshape(harm, per, pair_width)
        for step in range(1, harm):
            backward(pair, step).start()
        recv2[me, pair] = send2[me, pair]

    for pair in range(3):
        for step in range(1, harm):
            backward(pair, step).wait_recv()

        def fold_block(mb, _, pair=pair):
            for s in range(shells):
                for r in range(2):
                    at = pl.ds(pl.multiple_of(r * modes + mb * block, block), block)
                    got = [recv2[s * groups + g, pair, at, :].astype(F32) for g in range(groups)]
                    for c in range(2):
                        cut = slice(c * span, (c + 1) * span)
                        spread[(c * shells + s) * 2 + r] = jnp.concatenate([v[:, cut] for v in got], axis=1)
            here = pl.ds(pl.multiple_of(mb * block, block), block)
            folded[here, pl.ds(pair * 4 * shells, 4 * shells), :] = jnp.swapaxes(spread[...], 0, 1).astype(BF)
            return 0

        lax.fori_loop(0, modes // block, fold_block, 0)

    def spectrum(m, _):
        out_ref[m] = lax.dot_general(
            folded[m], tab[m], (((1,), (1,)), ((), ())), preferred_element_type=F32
        ).astype(BF)
        return 0

    lax.fori_loop(0, modes, spectrum, 0, unroll=4)

    for step in range(1, harm):
        energy_copy(step).wait_recv()
    energy_out[...] = jnp.sum(energy_all[...], axis=0)
    for step in range(1, harm):
        energy_copy(step).wait_send()
        for q in range(PASSES):
            forward(q, step).wait_send()
        for pair in range(3):
            backward(pair, step).wait_send()


def with_halo(block, axis):
    count = lax.axis_size(axis)
    up = [(i, i + 1) for i in range(count - 1)]
    down = [(b, a) for a, b in up]
    low = lax.ppermute(block[:, -1:], axis, up)
    high = lax.ppermute(block[:, :1], axis, down)
    return jnp.concatenate([low, block, high], axis=1)


def energy_weights(order_ints, degree_count):
    degrees = jnp.arange(degree_count, dtype=jnp.int32)
    order_col = order_ints[:, None]
    live_part = (degrees[None, :] >= order_col).astype(F32)
    inverse_modes = 1.0 / (2.0 * degrees.astype(F32) + 1.0)
    cosine_weight = jnp.where(order_col == 0, 0.5, 1.0)
    sine_weight = jnp.where(order_col == 0, 0.0, 1.0)
    scaled = live_part * inverse_modes[None, :]
    return jnp.stack([cosine_weight * scaled, sine_weight * scaled])


def local(velocity, magnetic, vorticity, current):
    harm = lax.axis_size("harm")
    me = lax.axis_index("harm")
    _, shells, _, modes, degrees = velocity.shape
    thetas, points = 3 * degrees // 2, 3 * degrees
    groups = harm // shells
    span = thetas // groups
    cosine, sectoral, unscale, weights, synthesis, analysis = tables(degrees, thetas, points, harm)

    own = me * modes + jnp.arange(modes, dtype=jnp.int32)
    energy_weight = energy_weights(own, degrees)
    energy = jnp.stack([
        jnp.sum(field.astype(F32) ** 2 * energy_weight[None, None], axis=(0, 2, 3))
        for field in (velocity, magnetic)
    ])

    fields = jnp.concatenate([velocity, magnetic, vorticity, current], axis=0)
    q_rows = 12 // PASSES * shells * 2
    cm = fields.reshape(PASSES, q_rows, modes, degrees).transpose(0, 2, 1, 3)
    x = jnp.asarray(np.broadcast_to(cosine[None, :], (modes, thetas)).copy())
    cut_weights = weights.reshape(groups, 1, span)
    w = jnp.asarray(np.concatenate([cut_weights, cut_weights], axis=2))

    block = min(16, modes)
    vmem = pl.BlockSpec(memory_space=pltpu.VMEM)
    dims = (harm, shells, groups, modes, degrees, thetas, points, span)
    spectra, total = pl.pallas_call(
        functools.partial(kernel, dims),
        name="dynamo",
        out_shape=(
            jax.ShapeDtypeStruct((modes, 12 * shells, degrees), BF),
            jax.ShapeDtypeStruct((2, shells, degrees), F32),
        ),
        in_specs=[vmem] * 8,
        out_specs=(vmem, vmem),
        scratch_shapes=[
            pltpu.VMEM((modes, degrees, thetas), BF),
            pltpu.VMEM((16, modes, thetas), F32),
            pltpu.VMEM((block, q_rows, thetas), F32),
            pltpu.VMEM((harm, 6, 2 * modes, 2 * span), BF),
            pltpu.VMEM((harm, 6, 2 * modes, 2 * span), BF),
            pltpu.VMEM((6, points, 2 * span), F32),
            pltpu.VMEM((3, points, 2 * span), BF),
            pltpu.VMEM((harm, 3, 2 * modes, 2 * span), BF),
            pltpu.VMEM((harm, 3, 2 * modes, 2 * span), BF),
            pltpu.VMEM((modes, 12 * shells, thetas), BF),
            pltpu.VMEM((4 * shells, block, thetas), F32),
            pltpu.VMEM((harm, 2, shells, degrees), F32),
            pltpu.SemaphoreType.DMA((PASSES, harm)),
            pltpu.SemaphoreType.DMA((PASSES, harm)),
            pltpu.SemaphoreType.DMA((3, harm)),
            pltpu.SemaphoreType.DMA((3, harm)),
            pltpu.SemaphoreType.DMA((harm,)),
            pltpu.SemaphoreType.DMA((harm,)),
        ],
        compiler_params=pltpu.CompilerParams(
            collective_id=0, has_side_effects=True, vmem_limit_bytes=60 * 1024 * 1024
        ),
    )(cm, x, jnp.asarray(sectoral), jnp.asarray(unscale), w, jnp.asarray(synthesis), jnp.asarray(analysis), energy)

    spectra = spectra.transpose(1, 0, 2).reshape(6, shells, 2, modes, degrees)
    rimmed = with_halo(spectra[3:], "rad").astype(F32)
    gradient = ((rimmed[:, 2:] - rimmed[:, :-2]) * 0.5).astype(BF)
    return spectra[:3], gradient, total


LANES = 128


def relay_tables(degrees, thetas, points, groups):
    half = thetas // 2
    rows = half // groups
    wide_rows = -(-rows // LANES) * LANES
    cosine, sectoral, unscale, weights, _, _ = tables(degrees, thetas, points, groups)

    def cut(array):
        parts = array[:, :half].reshape(-1, groups, rows).transpose(1, 0, 2)
        return np.pad(parts, ((0, 0), (0, 0), (0, wide_rows - rows)))

    x = cut(np.broadcast_to(cosine[None, :], (8, thetas)))
    w = np.tile(cut(np.broadcast_to(weights[None, :], (8, thetas))), (1, 1, 2))
    orders = np.arange(degrees)
    phase = 2.0 * np.pi * ((orders[:, None] * np.arange(points // 2)[None, :]) % points) / points
    trig = np.stack([np.cos(phase), np.sin(phase)]).astype(jnp.bfloat16).astype(np.float32)
    trig = trig.reshape(2, degrees // 2, 2, points // 2).transpose(2, 0, 1, 3)
    trig = trig.reshape(2, degrees, points // 2)
    doubled = np.where(orders == 0, 1.0, 2.0).reshape(degrees // 2, 2).T
    doubled = np.concatenate([doubled, doubled], axis=1)[:, :, None]
    synthesis = (trig.transpose(0, 2, 1) / degrees).astype(jnp.bfloat16)
    analysis = (trig * doubled).astype(jnp.bfloat16)
    return x, cut(sectoral), cut(unscale), w, synthesis, analysis


def cross(a, d):
    return [a[1] * d[2] - a[2] * d[1], a[2] * d[0] - a[0] * d[2], a[0] * d[1] - a[1] * d[0]]


def relay_kernel(
    dims,
    vel_ref, mag_ref, vor_ref, cur_ref, x_hbm, sect_hbm, unscale_hbm, w_hbm, trig_hbm, back_hbm,
    land_out, halo_out, energy_out,
    x_ref, sect_ref, unscale_ref, w_ref, trig_ref, back_ref, tab, rows, rx, cs, outs, modes_buf, grid, prod, asc, souts, own, ysend, yrecv, zsend, land, halo, energy_all, held,
    csem, osem, lsem, vsem, zss, zrs, rss, rrs, yss, yrs, bss, brs, hss, hrs, esend, erecv,
):
    rads, harm, shells, groups, modes, degrees, thetas, points = dims
    me = lax.axis_index("harm")
    rad = lax.axis_index("rad")
    z, y = me // groups, me % groups
    base, core = rad // groups * groups, rad % groups
    other = 1 - core
    straight = core == y
    block = groups * modes
    top = degrees // 2
    fields = (vel_ref, mag_ref, vor_ref, cur_ref)
    low_half = [src * block < top for src in range(shells)]

    def mate(shell):
        return {"rad": base + y, "harm": shell * groups + core}

    partner = {"rad": base + other}

    rad_up = {"rad": lax.rem(rad + 1, rads)}
    rad_down = {"rad": lax.rem(rad + rads - 1, rads)}

    barrier = pltpu.get_barrier_semaphore()
    for step in range(1, harm):
        pl.semaphore_signal(barrier, inc=1, device_id={"harm": lax.rem(me + step, harm)}, device_id_type=MESH)
    for target in (rad_up, rad_down):
        pl.semaphore_signal(barrier, inc=1, device_id=target, device_id_type=MESH)

    @pl.when(jnp.logical_not(straight))
    def _():
        for shell in range(shells):
            pl.semaphore_signal(barrier, inc=1, device_id=mate(shell), device_id_type=MESH)

    def lanes(low):
        return pl.ds(0, degrees) if low else pl.ds(top, degrees - top)

    def zcopy(f, dest, low, source):
        return pltpu.make_async_remote_copy(
            src_ref=fields[f].at[:, dest, :, :, lanes(low)],
            dst_ref=rx.at[me, f, :, :, :, lanes(low)],
            send_sem=zss.at[dest, f], recv_sem=zrs.at[source, f],
            device_id=mate(dest), device_id_type=MESH,
        )

    def relay(f, source, yy):
        slot = rx.at[source * groups + yy, f, :, :, :, lanes(low_half[source])]
        return pltpu.make_async_remote_copy(
            src_ref=slot, dst_ref=slot,
            send_sem=rss.at[source, f], recv_sem=rrs.at[source, f],
            device_id=partner, device_id_type=MESH,
        )

    def local_copy(f):
        return pltpu.make_async_copy(fields[f].at[:, z], rx.at[me, f], lsem.at[f])

    def held_copy(f):
        return pltpu.make_async_copy(fields[f], held.at[f], vsem.at[f])

    consts = [
        pltpu.make_async_copy(src, dst, csem.at[i]) for i, (src, dst) in enumerate((
            (x_hbm.at[core], x_ref), (sect_hbm.at[core], sect_ref), (unscale_hbm.at[core], unscale_ref),
            (w_hbm.at[core], w_ref), (trig_hbm, trig_ref), (back_hbm, back_ref)))
    ]
    for copy in consts:
        copy.start()
    for f in range(2):
        held_copy(f).start()

    @pl.when(straight)
    def _():
        for f in range(4):
            local_copy(f).start()

    pl.semaphore_wait(barrier, harm - 1 + 2 + shells * jnp.where(straight, 0, 1))

    def dest_of(j):
        mark = shells - 1 - j
        return mark - jnp.where(mark <= z, 1, 0)

    for low in (True, False):
        @pl.when((z * block < top) == low)
        def _(low=low):
            for j in range(shells - 1):
                for f in range(4):
                    zcopy(f, dest_of(j), low, z).start()

            @pl.when(jnp.logical_not(straight))
            def _():
                for f in range(4):
                    zcopy(f, z, low, z).start()

    def energy_copy(step):
        peer = lax.rem(me + step, harm)
        return pltpu.make_async_remote_copy(
            src_ref=energy_all.at[me], dst_ref=energy_all.at[me],
            send_sem=esend.at[step], recv_sem=erecv.at[step],
            device_id={"harm": peer}, device_id_type=MESH,
        )

    def pass_on(source):
        for f in range(4):
            @pl.when(jnp.logical_and(straight, z == source))
            def _(f=f):
                local_copy(f).wait()

            @pl.when(jnp.logical_not(jnp.logical_and(straight, z == source)))
            def _(f=f):
                zcopy(f, source, low_half[source], source).wait_recv()

            relay(f, source, core).start()

    for copy in consts[:3]:
        copy.wait()
    x = x_ref[0:1, :]
    width = x.shape[1]
    per = 16

    def table_block(source, starting, step, carry):
        first = source * block
        order = (first + lax.broadcasted_iota(jnp.int32, (block, width), 0)).astype(F32)
        square = order * order
        latest, before, inverse = carry
        for inner in range(per):
            degree = step * per + inner
            lf = jnp.full((1, width), degree, jnp.int32).astype(F32)
            scale = 1.0 / (4.0 * lf * lf - 1.0)
            gap = lf * lf - square
            if starting:
                gap = jnp.maximum(gap, 1.0)
            dd = gap * scale
            guess = lax.rsqrt(dd)
            guess = guess * (1.5 - 0.5 * dd * guess * guess)
            root = dd * guess
            if starting:
                live = lf > order
                guess = jnp.where(live, guess, 0.0)
                root = jnp.where(live, root, 0.0)
            new = guess * (x * latest - inverse * before)
            if starting:
                new = new + jnp.where(lf == order, sect_ref[pl.ds(first, block), :], 0.0)
            rows[inner] = new * unscale_ref[pl.ds(first, block), :]
            before, latest = latest, new
            inverse = root
        here = pl.ds(pl.multiple_of(step * per, per), per)
        tab[pl.ds(first, block), here, :] = jnp.swapaxes(rows[...], 0, 1).astype(BF)
        return latest, before, inverse

    def table_start(source):
        first = source * block
        floor = 0 if low_half[source] else top
        if first > floor:
            tab[pl.ds(first, block), pl.ds(floor, first - floor), :] = jnp.zeros((block, first - floor, width), BF)
        zero = jnp.zeros((block, width), F32)
        return lax.fori_loop(
            first // per, (first + block) // per, functools.partial(table_block, source, True), (zero, zero, zero))

    def table_rest(source, carry, low, high):
        return lax.fori_loop(low, high, functools.partial(table_block, source, False), carry)

    steps = degrees // per
    for source in reversed(range(shells)):
        carry = table_start(source)
        lax.fori_loop((source + 1) * block // per, steps, functools.partial(table_block, source, False), carry)

    for f in range(2):
        held_copy(f).wait()
    own_order = me * modes + lax.broadcasted_iota(jnp.int32, (modes, degrees), 0)
    degree = lax.broadcasted_iota(jnp.int32, (modes, degrees), 1)
    share = jnp.where(degree >= own_order, 1.0 / (2.0 * degree.astype(F32) + 1.0), 0.0)
    parts = (share * jnp.where(own_order == 0, 0.5, 1.0), share * jnp.where(own_order == 0, 0.0, 1.0))

    def shell_energy(shell, _):
        for f in range(2):
            total = jnp.zeros((modes, degrees), F32)
            for r in range(2):
                square = jnp.zeros((modes, degrees), F32)
                for c in range(3):
                    value = held[f, c, shell, r].astype(F32)
                    square = square + value * value
                total = total + square * parts[r]
            energy_all[me, f, pl.ds(shell, 1), :] = jnp.sum(total, axis=0, keepdims=True)
        return 0

    lax.fori_loop(0, shells, shell_energy, 0)
    for step in range(1, harm):
        energy_copy(step).start()

    lane = lax.broadcasted_iota(jnp.int32, (24, degrees), 1) % 2
    half_modes = modes // 2

    def transform(b, low):
        cut = slice(0, degrees) if low else slice(top, degrees)
        cs[:, :, cut] = jnp.swapaxes(
            rx[b].reshape(24, modes, degrees)[:, :, cut].astype(F32), 0, 1)
        for par in range(2):
            for i in range(half_modes):
                c = cs[2 * i + par, :, cut]
                even = lane[:, cut] == par
                left = jnp.concatenate([jnp.where(even, c, 0.0), jnp.where(even, 0.0, c)], axis=0).astype(BF)
                m = b * modes + 2 * i + par
                eo = jnp.dot(left, tab[m, cut, :], preferred_element_type=F32)
                outs[i] = jnp.concatenate([eo[:24] + eo[24:], eo[:24] - eo[24:]], axis=1)
            turned = jnp.swapaxes(outs[...], 0, 1).astype(BF)
            for k in range(24):
                c, r = k // 2, k % 2
                here = pl.ds(pl.multiple_of(r * top + b * half_modes, half_modes), half_modes)
                modes_buf[par, c, here, :] = turned[k]

    def partner_block(source):
        for f in range(4):
            relay(f, source, other).wait_recv()
        transform(source * groups + other, low_half[source])

    def own_block(source):
        transform(source * groups + core, low_half[source])

    for source in reversed(range(shells)):
        pass_on(source)
        if source + 1 < shells and (source < shells // 2 - 1 or source >= shells // 2):
            partner_block(source + 1)
        own_block(source)
        if source == shells // 2:
            partner_block(source)
    partner_block(0)

    for copy in consts[3:]:
        copy.wait()

    def synth(c, _):
        for par in range(2):
            grid[par, c] = jnp.dot(trig_ref[par], modes_buf[par, c], preferred_element_type=F32)
        return 0

    lax.fori_loop(0, 12, synth, 0, unroll=True)

    piece = 16

    def product_rows(i, _):
        at_rows = pl.ds(pl.multiple_of((i // 2) * piece, piece), piece)
        at_lanes = pl.ds(pl.multiple_of((i % 2) * width, width), width)
        e = [grid[0, c, at_rows, at_lanes] for c in range(12)]
        o = [grid[1, c, at_rows, at_lanes] for c in range(12)]
        sides = []
        for g in ([a + d for a, d in zip(e, o)], [a - d for a, d in zip(e, o)]):
            u, b, w, j = g[0:3], g[3:6], g[6:9], g[9:12]
            lamb, lorentz, induced = cross(u, w), cross(j, b), cross(u, b)
            sides.append([lamb[n] + lorentz[n] for n in range(3)] + induced)
        for c in range(6):
            prod[0, c, at_rows, at_lanes] = (sides[0][c] + sides[1][c]).astype(BF)
            prod[1, c, at_rows, at_lanes] = (sides[0][c] - sides[1][c]).astype(BF)
        return 0

    lax.fori_loop(0, points // 2 // piece * 2, product_rows, 0)

    def analyse(c, _):
        for par in range(2):
            a = jnp.dot(back_ref[par], prod[par, c], preferred_element_type=F32)
            a = a * w_ref[0:1, :]
            plus, minus = a[:, :width] + a[:, width:], a[:, :width] - a[:, width:]
            for r in range(2):
                cut = slice(r * top, (r + 1) * top)
                asc[par, 2 * c + r] = plus[cut]
                asc[par, 16 + 2 * c + r] = minus[cut]
        return 0

    lax.fori_loop(0, 6, analyse, 0, unroll=True)

    out_lane = lax.broadcasted_iota(jnp.int32, (16, degrees), 1) % 2

    def spectrum(b, low):
        cut = slice(0, degrees) if low else slice(top, degrees)
        for par in range(2):
            here = pl.ds(pl.multiple_of(b * half_modes, half_modes), half_modes)
            turned = jnp.swapaxes(asc[par, :, here, :], 0, 1).astype(BF)
            for i in range(half_modes):
                m = b * modes + 2 * i + par
                both = lax.dot_general(
                    turned[i], tab[m, cut, :], (((1,), (1,)), ((), ())), preferred_element_type=F32)
                souts[2 * i + par, :, cut] = jnp.where(out_lane[:, cut] == par, both[:16], both[16:])
        return jnp.swapaxes(souts[:, :, cut], 0, 1)[:12]

    def ycopy(target):
        low = low_half[target]
        return pltpu.make_async_remote_copy(
            src_ref=ysend.at[target, :, :, lanes(low)], dst_ref=yrecv.at[target, :, :, lanes(low)],
            send_sem=yss.at[target], recv_sem=yrs.at[target],
            device_id=partner, device_id_type=MESH,
        )

    def bcopy(target, shell, low):
        return pltpu.make_async_remote_copy(
            src_ref=zsend.at[target, :, :, lanes(low)], dst_ref=land.at[shell, :, :, lanes(low)],
            send_sem=bss.at[target], recv_sem=brs.at[shell],
            device_id=mate(target), device_id_type=MESH,
        )

    @pl.when(z * block >= top)
    def _():
        land[:, :, :, 0:top] = jnp.zeros((shells, 12, modes, top), BF)

    def finish(target):
        low = low_half[target]
        cut = slice(0, degrees) if low else slice(top, degrees)
        ycopy(target).wait_recv()
        total = (own[target, :, :, cut] + yrecv[target, :, :, cut].astype(F32)).astype(BF)
        stays = jnp.logical_and(straight, z == target)

        @pl.when(stays)
        def _():
            land[target, :, :, cut] = total

        @pl.when(jnp.logical_not(stays))
        def _():
            zsend[target, :, :, cut] = total
            bcopy(target, z, low).start()

    for target in range(shells):
        low = low_half[target]
        cut = slice(0, degrees) if low else slice(top, degrees)
        ysend[target, :, :, cut] = spectrum(target * groups + other, low).astype(BF)
        ycopy(target).start()
        if target > 0:
            finish(target - 1)
        own[target, :, :, cut] = spectrum(target * groups + core, low)
    finish(shells - 1)

    def arrived(shell):
        for low in (True, False):
            @pl.when(jnp.logical_and(jnp.logical_not(jnp.logical_and(straight, z == shell)), (z * block < top) == low))
            def _(low=low):
                bcopy(shell, shell, low).wait_recv()

    def hcopy(side):
        shell = shells - 1 if side == 0 else 0
        return pltpu.make_async_remote_copy(
            src_ref=land.at[shell, pl.ds(6, 6)], dst_ref=halo.at[side],
            send_sem=hss.at[side], recv_sem=hrs.at[side],
            device_id=rad_up if side == 0 else rad_down, device_id_type=MESH,
        )

    def out_copy(shell):
        return pltpu.make_async_copy(land.at[shell], land_out.at[shell], osem.at[shell])

    def halo_copy(side):
        return pltpu.make_async_copy(halo.at[side], halo_out.at[side], osem.at[shells + side])

    arrived(shells - 1)
    hcopy(0).start()
    out_copy(shells - 1).start()
    arrived(0)
    hcopy(1).start()
    out_copy(0).start()
    for step in range(1, harm):
        energy_copy(step).wait_recv()
    energy_out[...] = jnp.sum(energy_all[...], axis=0)
    for shell in range(1, shells - 1):
        arrived(shell)
        out_copy(shell).start()
    for side in range(2):
        hcopy(side).wait_recv()
        halo_copy(side).start()
    for shell in range(shells):
        out_copy(shell).wait()
    for side in range(2):
        halo_copy(side).wait()
    hcopy(0).wait_send()
    hcopy(1).wait_send()
    for step in range(1, harm):
        energy_copy(step).wait_send()
    for low in (True, False):
        @pl.when((z * block < top) == low)
        def _(low=low):
            for j in range(shells - 1):
                for f in range(4):
                    zcopy(f, dest_of(j), low, z).wait_send()

            @pl.when(jnp.logical_not(straight))
            def _():
                for f in range(4):
                    zcopy(f, z, low, z).wait_send()

    for source in range(shells):
        for f in range(4):
            relay(f, source, core).wait_send()
        ycopy(source).wait_send()

        @pl.when(jnp.logical_not(jnp.logical_and(straight, z == source)))
        def _(source=source):
            bcopy(source, z, low_half[source]).wait_send()


def local_relay(velocity, magnetic, vorticity, current):
    harm, rads = lax.axis_size("harm"), lax.axis_size("rad")
    _, shells, _, modes, degrees = velocity.shape
    thetas, points = 3 * degrees // 2, 3 * degrees
    groups = harm // shells
    x, sect, unscale, w, synthesis, analysis = relay_tables(degrees, thetas, points, groups)
    width = x.shape[2]
    block = groups * modes
    vmem = pl.BlockSpec(memory_space=pltpu.VMEM)
    hbm = pl.BlockSpec(memory_space=pl.ANY)
    dims = (rads, harm, shells, groups, modes, degrees, thetas, points)
    dma = pltpu.SemaphoreType.DMA
    consts = (x, sect, unscale, w, synthesis, analysis)
    landed, halo, energy = pl.pallas_call(
        functools.partial(relay_kernel, dims),
        name="dynamo",
        out_shape=(
            jax.ShapeDtypeStruct((shells, 12, modes, degrees), BF),
            jax.ShapeDtypeStruct((2, 6, modes, degrees), BF),
            jax.ShapeDtypeStruct((2, shells, degrees), F32),
        ),
        in_specs=[hbm] * 10,
        out_specs=(hbm, hbm, vmem),
        scratch_shapes=[
            *(pltpu.VMEM(c.shape[1:], c.dtype) for c in consts[:4]),
            *(pltpu.VMEM(c.shape, c.dtype) for c in consts[4:]),
            pltpu.VMEM((degrees, degrees, width), BF),
            pltpu.VMEM((16, block, width), F32),
            pltpu.VMEM((harm, 4, 3, 2, modes, degrees), BF),
            pltpu.VMEM((modes, 24, degrees), F32),
            pltpu.VMEM((modes // 2, 24, 2 * width), F32),
            pltpu.VMEM((2, 12, degrees, 2 * width), BF),
            pltpu.VMEM((2, 12, points // 2, 2 * width), F32),
            pltpu.VMEM((2, 6, points // 2, 2 * width), BF),
            pltpu.VMEM((2, 32, degrees // 2, width), F32),
            pltpu.VMEM((modes, 16, degrees), F32),
            pltpu.VMEM((shells, 12, modes, degrees), F32),
            pltpu.VMEM((shells, 12, modes, degrees), BF),
            pltpu.VMEM((shells, 12, modes, degrees), BF),
            pltpu.VMEM((shells, 12, modes, degrees), BF),
            pltpu.VMEM((shells, 12, modes, degrees), BF),
            pltpu.VMEM((2, 6, modes, degrees), BF),
            pltpu.VMEM((harm, 2, shells, degrees), F32),
            pltpu.VMEM((2,) + velocity.shape, BF),
            dma((6,)), dma((shells + 2,)), dma((4,)), dma((2,)), dma((shells, 4)), dma((shells, 4)), dma((shells, 4)), dma((shells, 4)),
            dma((shells,)), dma((shells,)), dma((shells,)), dma((shells,)),
            dma((2,)), dma((2,)), dma((harm,)), dma((harm,)),
        ],
        compiler_params=pltpu.CompilerParams(
            collective_id=0, has_side_effects=True, vmem_limit_bytes=62 * 1024 * 1024
        ),
    )(velocity, magnetic, vorticity, current, *(jnp.asarray(c) for c in consts))

    spectra = landed.reshape(shells, 6, 2, modes, degrees).transpose(1, 0, 2, 3, 4)
    rad = lax.axis_index("rad")
    below = jnp.where(rad > 0, halo[0].astype(F32), 0.0).reshape(3, 1, 2, modes, degrees)
    above = jnp.where(rad < rads - 1, halo[1].astype(F32), 0.0).reshape(3, 1, 2, modes, degrees)
    rimmed = jnp.concatenate([below, spectra[3:].astype(F32), above], axis=1)
    gradient = ((rimmed[:, 2:] - rimmed[:, :-2]) * 0.5).astype(BF)
    return spectra[:3], gradient, energy


def relay_fits(mesh, args):
    _, total, _, degrees, _ = args[0].shape
    rads, harm = mesh.shape["rad"], mesh.shape["harm"]
    shells, modes = total // rads, degrees // harm
    return harm == 2 * shells and rads > 2 and rads % 2 == 0 and modes % 32 == 0 and degrees % (2 * LANES) == 0


def solution(mesh):
    spec = P(None, "rad", None, "harm", None)

    def run(*args):
        body = local_relay if relay_fits(mesh, args) else local
        return jax.shard_map(
            body,
            mesh=mesh,
            in_specs=(spec,) * 4,
            out_specs=(spec, spec, P(None, "rad", None)),
            check_vma=False,
        )(*args)

    return run
```

```python
import functools

import jax
import jax.numpy as jnp
import numpy as np
from jax import lax
from jax.experimental import pallas as pl
from jax.experimental.pallas import tpu as pltpu
from jax.sharding import PartitionSpec as P

MESH = pl.DeviceIdType.MESH
PASSES = 2
BF = jnp.bfloat16
F32 = jnp.float32


def tables(degrees, thetas, points, harm_count):
    half = thetas // 2
    angles = np.pi * (np.arange(half) + 0.5) / thetas
    cosine = np.concatenate([np.cos(angles), -np.cos(angles)[::-1]])
    sine = np.concatenate([np.sin(angles), np.sin(angles)[::-1]])
    orders = np.arange(degrees)
    steps = np.arange(1, degrees)
    terms = 0.5 * np.log((2.0 * steps + 1.0) / (2.0 * steps))
    start = 0.5 * np.log(0.5) + np.concatenate([[0.0], np.cumsum(terms)])
    log_sector = start[:, None] + orders[:, None] * np.log(sine)[None, :]
    sectoral = np.exp(np.maximum(log_sector, -60.0)).astype(np.float32)
    unscale = np.exp(np.minimum(log_sector + 60.0, 0.0)).astype(np.float32)
    wave = np.arange(1, half + 1)
    series = np.cos(2.0 * wave[None, :] * angles[:, None]) / (4.0 * wave[None, :] ** 2 - 1.0)
    north = 2.0 / thetas * (1.0 - 2.0 * series.sum(axis=1))
    weights = np.concatenate([north, north[::-1]])
    weights = (weights * degrees / points).astype(np.float32)
    phase = 2.0 * np.pi * ((orders[:, None] * np.arange(points)[None, :]) % points) / points
    trig = np.stack([np.cos(phase), np.sin(phase)])
    trig = trig.reshape(2, harm_count, degrees // harm_count, points)
    trig = trig.transpose(1, 0, 2, 3).reshape(2 * degrees, points).astype(jnp.bfloat16)
    doubled = np.where(orders == 0, 1.0, 2.0).reshape(harm_count, 1, -1)
    doubled = np.broadcast_to(doubled, (harm_count, 2, degrees // harm_count)).reshape(-1, 1)
    analysis = (trig.astype(np.float32) * doubled).astype(jnp.bfloat16)
    return cosine.astype(np.float32), sectoral, unscale, weights, trig.T.copy(), analysis


def wide(column, width):
    return jnp.concatenate([column] * (width // column.shape[1]), axis=1)


def kernel(
    dims,
    cm_ref, x_ref, sect_ref, unscale_ref, w_ref, trig_ref, back_ref, energy_ref,
    out_ref, energy_out,
    tab, rows, outs, send, recv, grid, prod, send2, recv2, folded, spread, energy_all,
    ssem, rsem, ssem2, rsem2, esend, erecv,
):
    harm, shells, groups, modes, degrees, thetas, points, span = dims
    me = lax.axis_index("harm")
    pair_width = 2 * span
    block = min(16, modes)
    q_pairs = 6 // PASSES
    q_rows = 12 // PASSES * shells * 2

    barrier = pltpu.get_barrier_semaphore()
    for step in range(1, harm):
        peer = lax.rem(me + step, harm)
        pl.semaphore_signal(barrier, inc=1, device_id={"harm": peer}, device_id_type=MESH)

    order = (me * modes + lax.broadcasted_iota(jnp.int32, (modes, 128), 0)).astype(F32)
    order_square = order * order
    own = pl.ds(pl.multiple_of(me * modes, modes), modes)
    energy_all[me] = energy_ref[...]

    def table_block(step, carry):
        latest, before, inverse = carry
        for inner in range(16):
            degree = step * 16 + inner
            lf = jnp.full((modes, 128), degree, jnp.int32).astype(F32)
            dd = jnp.maximum(lf * lf - order_square, 1.0) / (4.0 * lf * lf - 1.0)
            guess = lax.rsqrt(dd)
            guess = guess * (1.5 - 0.5 * dd * guess * guess)
            live = lf > order
            alpha = jnp.where(live, guess, 0.0)
            starts = jnp.where(lf == order, 1.0, 0.0)
            new = wide(alpha, thetas) * (x_ref[...] * latest - wide(inverse, thetas) * before)
            new = new + wide(starts, thetas) * sect_ref[own, :]
            rows[inner] = new * unscale_ref[own, :]
            before, latest = latest, new
            inverse = jnp.where(live, dd * guess, 0.0)
        tab[:, pl.ds(pl.multiple_of(step * 16, 16), 16), :] = jnp.swapaxes(rows[...], 0, 1).astype(BF)
        return latest, before, inverse

    zero = jnp.zeros((modes, thetas), F32)
    lax.fori_loop(0, degrees // 16, table_block, (zero, zero, jnp.zeros((modes, 128), F32)))

    pl.semaphore_wait(barrier, harm - 1)

    def energy_copy(step):
        peer = lax.rem(me + step, harm)
        return pltpu.make_async_remote_copy(
            src_ref=energy_all.at[me], dst_ref=energy_all.at[me],
            send_sem=esend.at[step], recv_sem=erecv.at[step],
            device_id={"harm": peer}, device_id_type=MESH,
        )

    def forward(q, step):
        peer = lax.rem(me + step, harm)
        return pltpu.make_async_remote_copy(
            src_ref=send.at[peer, pl.ds(q * q_pairs, q_pairs)],
            dst_ref=recv.at[me, pl.ds(q * q_pairs, q_pairs)],
            send_sem=ssem.at[q, step], recv_sem=rsem.at[q, step],
            device_id={"harm": peer}, device_id_type=MESH,
        )

    def backward(pair, step):
        peer = lax.rem(me + step, harm)
        return pltpu.make_async_remote_copy(
            src_ref=send2.at[peer, pair], dst_ref=recv2.at[me, pair],
            send_sem=ssem2.at[pair, step], recv_sem=rsem2.at[pair, step],
            device_id={"harm": peer}, device_id_type=MESH,
        )

    for q in range(PASSES):
        def mode_block(mb, _, q=q):
            def one(i, _):
                m = mb * block + i
                outs[i] = jnp.dot(cm_ref[q, m], tab[m], preferred_element_type=F32) * (1.0 / degrees)
                return 0

            lax.fori_loop(0, block, one, 0, unroll=4)
            turned = jnp.swapaxes(outs[...], 0, 1)
            for s in range(shells):
                for pair in range(q_pairs):
                    for r in range(2):
                        k = (pair * 2 * shells + s) * 2 + r
                        first, second = turned[k], turned[k + 2 * shells]
                        for g in range(groups):
                            cut = slice(g * span, (g + 1) * span)
                            piece = jnp.concatenate([first[:, cut], second[:, cut]], axis=1).astype(BF)
                            at = pl.multiple_of(r * modes + mb * block, block)
                            send[s * groups + g, q * q_pairs + pair, pl.ds(at, block), :] = piece
            return 0

        lax.fori_loop(0, modes // block, mode_block, 0)
        for step in range(1, harm):
            forward(q, step).start()
        recv[me, pl.ds(q * q_pairs, q_pairs)] = send[me, pl.ds(q * q_pairs, q_pairs)]
    for step in range(1, harm):
        energy_copy(step).start()

    chunk = points // 3
    for q in range(PASSES):
        for step in range(1, harm):
            forward(q, step).wait_recv()
        for pair in range(q * q_pairs, (q + 1) * q_pairs):
            arrived = recv[:, pair].reshape(2 * degrees, pair_width)
            for part in range(3):
                cut = pl.ds(part * chunk, chunk)
                grid[pair, cut, :] = jnp.dot(trig_ref[cut, :], arrived, preferred_element_type=F32)

    piece_rows = 32

    def product_rows(i, _):
        at = pl.ds(pl.multiple_of(i * piece_rows, piece_rows), piece_rows)
        both = [grid[pair, at, :] for pair in range(6)]
        c = []
        for pair in range(6):
            c += [both[pair][:, :span], both[pair][:, span:]]
        u, b, w, j = c[0:3], c[3:6], c[6:9], c[9:12]

        def cross(a, d):
            return [a[1] * d[2] - a[2] * d[1], a[2] * d[0] - a[0] * d[2], a[0] * d[1] - a[1] * d[0]]

        lamb, lorentz, induced = cross(u, w), cross(j, b), cross(u, b)
        six = [lamb[n] + lorentz[n] for n in range(3)] + induced
        for pair in range(3):
            prod[pair, at, :] = jnp.concatenate([six[2 * pair], six[2 * pair + 1]], axis=1).astype(BF)
        return 0

    lax.fori_loop(0, points // piece_rows, product_rows, 0)

    per = 2 * modes
    for pair in range(3):
        analysed = jnp.dot(back_ref[...], prod[pair], preferred_element_type=F32)
        analysed = (analysed * w_ref[lax.rem(me, groups)]).astype(BF)
        send2[:, pair] = analysed.reshape(harm, per, pair_width)
        for step in range(1, harm):
            backward(pair, step).start()
        recv2[me, pair] = send2[me, pair]

    for pair in range(3):
        for step in range(1, harm):
            backward(pair, step).wait_recv()

        def fold_block(mb, _, pair=pair):
            for s in range(shells):
                for r in range(2):
                    at = pl.ds(pl.multiple_of(r * modes + mb * block, block), block)
                    got = [recv2[s * groups + g, pair, at, :].astype(F32) for g in range(groups)]
                    for c in range(2):
                        cut = slice(c * span, (c + 1) * span)
                        spread[(c * shells + s) * 2 + r] = jnp.concatenate([v[:, cut] for v in got], axis=1)
            here = pl.ds(pl.multiple_of(mb * block, block), block)
            folded[here, pl.ds(pair * 4 * shells, 4 * shells), :] = jnp.swapaxes(spread[...], 0, 1).astype(BF)
            return 0

        lax.fori_loop(0, modes // block, fold_block, 0)

    def spectrum(m, _):
        out_ref[m] = lax.dot_general(
            folded[m], tab[m], (((1,), (1,)), ((), ())), preferred_element_type=F32
        ).astype(BF)
        return 0

    lax.fori_loop(0, modes, spectrum, 0, unroll=4)

    for step in range(1, harm):
        energy_copy(step).wait_recv()
    energy_out[...] = jnp.sum(energy_all[...], axis=0)
    for step in range(1, harm):
        energy_copy(step).wait_send()
        for q in range(PASSES):
            forward(q, step).wait_send()
        for pair in range(3):
            backward(pair, step).wait_send()


def with_halo(block, axis):
    count = lax.axis_size(axis)
    up = [(i, i + 1) for i in range(count - 1)]
    down = [(b, a) for a, b in up]
    low = lax.ppermute(block[:, -1:], axis, up)
    high = lax.ppermute(block[:, :1], axis, down)
    return jnp.concatenate([low, block, high], axis=1)


def energy_weights(order_ints, degree_count):
    degrees = jnp.arange(degree_count, dtype=jnp.int32)
    order_col = order_ints[:, None]
    live_part = (degrees[None, :] >= order_col).astype(F32)
    inverse_modes = 1.0 / (2.0 * degrees.astype(F32) + 1.0)
    cosine_weight = jnp.where(order_col == 0, 0.5, 1.0)
    sine_weight = jnp.where(order_col == 0, 0.0, 1.0)
    scaled = live_part * inverse_modes[None, :]
    return jnp.stack([cosine_weight * scaled, sine_weight * scaled])


def local(velocity, magnetic, vorticity, current):
    harm = lax.axis_size("harm")
    me = lax.axis_index("harm")
    _, shells, _, modes, degrees = velocity.shape
    thetas, points = 3 * degrees // 2, 3 * degrees
    groups = harm // shells
    span = thetas // groups
    cosine, sectoral, unscale, weights, synthesis, analysis = tables(degrees, thetas, points, harm)

    own = me * modes + jnp.arange(modes, dtype=jnp.int32)
    energy_weight = energy_weights(own, degrees)
    energy = jnp.stack([
        jnp.sum(field.astype(F32) ** 2 * energy_weight[None, None], axis=(0, 2, 3))
        for field in (velocity, magnetic)
    ])

    fields = jnp.concatenate([velocity, magnetic, vorticity, current], axis=0)
    q_rows = 12 // PASSES * shells * 2
    cm = fields.reshape(PASSES, q_rows, modes, degrees).transpose(0, 2, 1, 3)
    x = jnp.asarray(np.broadcast_to(cosine[None, :], (modes, thetas)).copy())
    cut_weights = weights.reshape(groups, 1, span)
    w = jnp.asarray(np.concatenate([cut_weights, cut_weights], axis=2))

    block = min(16, modes)
    vmem = pl.BlockSpec(memory_space=pltpu.VMEM)
    dims = (harm, shells, groups, modes, degrees, thetas, points, span)
    spectra, total = pl.pallas_call(
        functools.partial(kernel, dims),
        name="dynamo",
        out_shape=(
            jax.ShapeDtypeStruct((modes, 12 * shells, degrees), BF),
            jax.ShapeDtypeStruct((2, shells, degrees), F32),
        ),
        in_specs=[vmem] * 8,
        out_specs=(vmem, vmem),
        scratch_shapes=[
            pltpu.VMEM((modes, degrees, thetas), BF),
            pltpu.VMEM((16, modes, thetas), F32),
            pltpu.VMEM((block, q_rows, thetas), F32),
            pltpu.VMEM((harm, 6, 2 * modes, 2 * span), BF),
            pltpu.VMEM((harm, 6, 2 * modes, 2 * span), BF),
            pltpu.VMEM((6, points, 2 * span), F32),
            pltpu.VMEM((3, points, 2 * span), BF),
            pltpu.VMEM((harm, 3, 2 * modes, 2 * span), BF),
            pltpu.VMEM((harm, 3, 2 * modes, 2 * span), BF),
            pltpu.VMEM((modes, 12 * shells, thetas), BF),
            pltpu.VMEM((4 * shells, block, thetas), F32),
            pltpu.VMEM((harm, 2, shells, degrees), F32),
            pltpu.SemaphoreType.DMA((PASSES, harm)),
            pltpu.SemaphoreType.DMA((PASSES, harm)),
            pltpu.SemaphoreType.DMA((3, harm)),
            pltpu.SemaphoreType.DMA((3, harm)),
            pltpu.SemaphoreType.DMA((harm,)),
            pltpu.SemaphoreType.DMA((harm,)),
        ],
        compiler_params=pltpu.CompilerParams(
            collective_id=0, has_side_effects=True, vmem_limit_bytes=60 * 1024 * 1024
        ),
    )(cm, x, jnp.asarray(sectoral), jnp.asarray(unscale), w, jnp.asarray(synthesis), jnp.asarray(analysis), energy)

    spectra = spectra.transpose(1, 0, 2).reshape(6, shells, 2, modes, degrees)
    rimmed = with_halo(spectra[3:], "rad").astype(F32)
    gradient = ((rimmed[:, 2:] - rimmed[:, :-2]) * 0.5).astype(BF)
    return spectra[:3], gradient, total


LANES = 128


def relay_tables(degrees, thetas, points, groups):
    half = thetas // 2
    rows = half // groups
    wide_rows = -(-rows // LANES) * LANES
    cosine, sectoral, unscale, weights, _, _ = tables(degrees, thetas, points, groups)

    def cut(array):
        parts = array[:, :half].reshape(-1, groups, rows).transpose(1, 0, 2)
        return np.pad(parts, ((0, 0), (0, 0), (0, wide_rows - rows)))

    x = cut(np.broadcast_to(cosine[None, :], (8, thetas)))
    w = np.tile(cut(np.broadcast_to(weights[None, :], (8, thetas))), (1, 1, 2))
    orders = np.arange(degrees)
    phase = 2.0 * np.pi * ((orders[:, None] * np.arange(points // 2)[None, :]) % points) / points
    trig = np.stack([np.cos(phase), np.sin(phase)]).astype(jnp.bfloat16).astype(np.float32)
    trig = trig.reshape(2, degrees // 2, 2, points // 2).transpose(2, 0, 1, 3)
    trig = trig.reshape(2, degrees, points // 2)
    doubled = np.where(orders == 0, 1.0, 2.0).reshape(degrees // 2, 2).T
    doubled = np.concatenate([doubled, doubled], axis=1)[:, :, None]
    synthesis = (trig.transpose(0, 2, 1) / degrees).astype(jnp.bfloat16)
    analysis = (trig * doubled).astype(jnp.bfloat16)
    return x, cut(sectoral), cut(unscale), w, synthesis, analysis


def cross(a, d):
    return [a[1] * d[2] - a[2] * d[1], a[2] * d[0] - a[0] * d[2], a[0] * d[1] - a[1] * d[0]]


def relay_kernel(
    dims,
    vel_ref, mag_ref, vor_ref, cur_ref, x_hbm, sect_hbm, unscale_hbm, w_hbm, trig_hbm, back_hbm,
    land_out, halo_out, energy_hbm,
    x_ref, sect_ref, unscale_ref, w_ref, trig_ref, back_ref, tab, rows, rx, cs, outs, modes_buf, grid, prod, asc, souts, own, ysend, yrecv, zsend, land, halo, energy_all, held,
    pack, rxp, zpack, landp, energy_out, csem, osem, lsem, vsem, zss, zrs, rss, rrs, yss, yrs, bss, brs, hss, hrs, esend, erecv, pss, prs, qss, qrs, bps, bpr,
):
    rads, harm, shells, groups, modes, degrees, thetas, points = dims
    me = lax.axis_index("harm")
    rad = lax.axis_index("rad")
    z, y = me // groups, me % groups
    base, core = rad // groups * groups, rad % groups
    other = 1 - core
    straight = core == y
    block = groups * modes
    top = degrees // 2
    fields = (vel_ref, mag_ref, vor_ref, cur_ref)
    low_half = [src * block < top for src in range(shells)]
    packed = [2 * src * block == top for src in range(shells)]
    whole = [low and not half for low, half in zip(low_half, packed)]
    mid = top // 2
    packs = 2 * z * block == top

    def mate(shell):
        return {"rad": base + y, "harm": shell * groups + core}

    partner = {"rad": base + other}

    rad_up = {"rad": lax.rem(rad + 1, rads)}
    rad_down = {"rad": lax.rem(rad + rads - 1, rads)}

    barrier = pltpu.get_barrier_semaphore()
    for step in range(1, harm):
        pl.semaphore_signal(barrier, inc=1, device_id={"harm": lax.rem(me + step, harm)}, device_id_type=MESH)
    for target in (rad_up, rad_down):
        pl.semaphore_signal(barrier, inc=1, device_id=target, device_id_type=MESH)

    @pl.when(jnp.logical_not(straight))
    def _():
        for shell in range(shells):
            pl.semaphore_signal(barrier, inc=1, device_id=mate(shell), device_id_type=MESH)

    def lanes(low):
        return pl.ds(0, degrees) if low else pl.ds(top, degrees - top)

    def zcopy(f, dest, low, source):
        return pltpu.make_async_remote_copy(
            src_ref=fields[f].at[:, dest, :, :, lanes(low)],
            dst_ref=rx.at[me, f, :, :, :, lanes(low)],
            send_sem=zss.at[dest, f], recv_sem=zrs.at[source, f],
            device_id=mate(dest), device_id_type=MESH,
        )

    def relay(f, source, yy):
        slot = rx.at[source * groups + yy, f, :, :, :, lanes(whole[source])]
        return pltpu.make_async_remote_copy(
            src_ref=slot, dst_ref=slot,
            send_sem=rss.at[source, f], recv_sem=rrs.at[source, f],
            device_id=partner, device_id_type=MESH,
        )

    def pcopy(f, dest, source):
        return pltpu.make_async_remote_copy(
            src_ref=pack.at[f, :, dest], dst_ref=rxp.at[y, f],
            send_sem=pss.at[dest, f], recv_sem=prs.at[f],
            device_id=mate(dest), device_id_type=MESH,
        )

    def relay_packed(f, yy):
        return pltpu.make_async_remote_copy(
            src_ref=rxp.at[yy, f], dst_ref=rxp.at[yy, f],
            send_sem=qss.at[f], recv_sem=qrs.at[f],
            device_id=partner, device_id_type=MESH,
        )

    def local_copy(f):
        return pltpu.make_async_copy(fields[f].at[:, z], rx.at[me, f], lsem.at[f])

    def held_copy(f):
        return pltpu.make_async_copy(fields[f], held.at[f], vsem.at[f])

    consts = [
        pltpu.make_async_copy(src, dst, csem.at[i]) for i, (src, dst) in enumerate((
            (x_hbm.at[core], x_ref), (sect_hbm.at[core], sect_ref), (unscale_hbm.at[core], unscale_ref),
            (w_hbm.at[core], w_ref), (trig_hbm, trig_ref), (back_hbm, back_ref)))
    ]
    for copy in consts:
        copy.start()
    for f in range(2):
        held_copy(f).start()

    @pl.when(straight)
    def _():
        for f in range(4):
            local_copy(f).start()

    pl.semaphore_wait(barrier, harm - 1 + 2 + shells * jnp.where(straight, 0, 1))

    def dest_of(j):
        mark = shells - 1 - j
        return mark - jnp.where(mark <= z, 1, 0)

    is_whole = jnp.logical_and(z * block < top, jnp.logical_not(packs))

    def routed(phase, send):
        for j in range(shells - 1):
            if j == 0:
                if phase == 0:
                    send(dest_of(j))
            else:
                crossing = jnp.logical_and(z * block < top, dest_of(j) * block >= top)

                @pl.when(crossing == (phase == 1))
                def _(j=j):
                    send(dest_of(j))
        if phase == 0:
            @pl.when(jnp.logical_not(straight))
            def _():
                send(z)

    def plain_sends(phase, act, early=None):
        for low in (True, False):
            if early is not None and early == low:
                continue

            @pl.when(is_whole == low)
            def _(low=low):
                routed(phase, lambda dest: [act(zcopy(f, dest, low, z)) for f in range(4)])

    def packed_sends(phase, act):
        @pl.when(packs)
        def _():
            routed(phase, lambda dest: [act(pcopy(f, dest, z)) for f in range(4)])

    def begin(copy):
        copy.start()

    plain_sends(0, begin)

    @pl.when(packs)
    def _():
        for f in range(2, 4):
            held_copy(f).start()
        for f in range(4):
            held_copy(f).wait()
            for c in range(3):
                for shell in range(shells):
                    first, second = held[f, c, shell, 0, :, 0:top], held[f, c, shell, 1, :, 0:top]
                    pack[f, c, shell] = jnp.concatenate([second[:, mid:], first[:, mid:]], axis=1)

        @pl.when(straight)
        def _():
            for f in range(4):
                rxp[core, f] = pack[f, :, z]

    packed_sends(0, begin)

    def energy_copy(step):
        peer = lax.rem(me + step, harm)
        return pltpu.make_async_remote_copy(
            src_ref=energy_all.at[me], dst_ref=energy_all.at[me],
            send_sem=esend.at[step], recv_sem=erecv.at[step],
            device_id={"harm": peer}, device_id_type=MESH,
        )

    def pass_on(source):
        for f in range(4):
            @pl.when(jnp.logical_and(straight, z == source))
            def _(f=f):
                local_copy(f).wait()

            @pl.when(jnp.logical_not(jnp.logical_and(straight, z == source)))
            def _(f=f):
                zcopy(f, source, whole[source], source).wait_recv()
                if packed[source]:
                    pcopy(f, source, source).wait_recv()

            relay(f, source, core).start()
            if packed[source]:
                relay_packed(f, core).start()

    for copy in consts[:3]:
        copy.wait()
    x = x_ref[0:1, :]
    width = x.shape[1]
    per = 16

    def table_block(source, starting, step, carry):
        first = source * block
        order = (first + lax.broadcasted_iota(jnp.int32, (block, width), 0)).astype(F32)
        square = order * order
        latest, before, inverse = carry
        for inner in range(per):
            degree = step * per + inner
            lf = jnp.full((1, width), degree, jnp.int32).astype(F32)
            scale = 1.0 / (4.0 * lf * lf - 1.0)
            gap = lf * lf - square
            if starting:
                gap = jnp.maximum(gap, 1.0)
            dd = gap * scale
            guess = lax.rsqrt(dd)
            guess = guess * (1.5 - 0.5 * dd * guess * guess)
            root = dd * guess
            if starting:
                live = lf > order
                guess = jnp.where(live, guess, 0.0)
                root = jnp.where(live, root, 0.0)
            new = guess * (x * latest - inverse * before)
            if starting:
                new = new + jnp.where(lf == order, sect_ref[pl.ds(first, block), :], 0.0)
            rows[inner] = new * unscale_ref[pl.ds(first, block), :]
            before, latest = latest, new
            inverse = root
        here = pl.ds(pl.multiple_of(step * per, per), per)
        tab[pl.ds(first, block), here, :] = jnp.swapaxes(rows[...], 0, 1).astype(BF)
        return latest, before, inverse

    def table_start(source):
        first = source * block
        floor = 0 if low_half[source] else top
        if first > floor:
            tab[pl.ds(first, block), pl.ds(floor, first - floor), :] = jnp.zeros((block, first - floor, width), BF)
        zero = jnp.zeros((block, width), F32)
        return lax.fori_loop(
            first // per, (first + block) // per, functools.partial(table_block, source, True), (zero, zero, zero))

    def table_rest(source, carry, low, high):
        return lax.fori_loop(low, high, functools.partial(table_block, source, False), carry)

    steps = degrees // per
    for source in reversed(range(shells)):
        carry = table_start(source)
        first = (source + 1) * block // per
        turn = first + (steps - first) // 4 if source == 0 else steps
        carry = lax.fori_loop(first, turn, functools.partial(table_block, source, False), carry)
        if source == 1:
            plain_sends(1, begin, early=True)
            packed_sends(1, begin)
        if source == 0:
            plain_sends(1, begin, early=False)
            lax.fori_loop(turn, steps, functools.partial(table_block, source, False), carry)

    @pl.when(jnp.logical_not(packs))
    def _():
        for f in range(2):
            held_copy(f).wait()

    own_order = me * modes + lax.broadcasted_iota(jnp.int32, (modes, degrees), 0)
    degree = lax.broadcasted_iota(jnp.int32, (modes, degrees), 1)
    share = jnp.where(degree >= own_order, 1.0 / (2.0 * degree.astype(F32) + 1.0), 0.0)
    parts = (share * jnp.where(own_order == 0, 0.5, 1.0), share * jnp.where(own_order == 0, 0.0, 1.0))

    def shell_energy(shell, _):
        for f in range(2):
            total = jnp.zeros((modes, degrees), F32)
            for r in range(2):
                square = jnp.zeros((modes, degrees), F32)
                for c in range(3):
                    value = held[f, c, shell, r].astype(F32)
                    square = square + value * value
                total = total + square * parts[r]
            energy_all[me, f, pl.ds(shell, 1), :] = jnp.sum(total, axis=0, keepdims=True)
        return 0

    lax.fori_loop(0, shells, shell_energy, 0)
    for step in range(1, harm):
        energy_copy(step).start()

    lane = lax.broadcasted_iota(jnp.int32, (24, degrees), 1) % 2
    half_modes = modes // 2

    def transform(source, yy):
        b = source * groups + yy
        cut = slice(0, degrees) if low_half[source] else slice(top, degrees)
        direct = slice(0, degrees) if whole[source] else slice(top, degrees)
        cs[:, :, direct] = jnp.swapaxes(
            rx[b].reshape(24, modes, degrees)[:, :, direct].astype(F32), 0, 1)
        if packed[source]:
            first = rxp[yy].reshape(12, 1, modes, top).astype(F32)
            second = jnp.concatenate([first[..., mid:], first[..., :mid]], axis=3)
            both = jnp.concatenate([first, second], axis=1).reshape(24, modes, top)
            cs[:, :, 0:top] = jnp.swapaxes(both, 0, 1)
        for par in range(2):
            for i in range(half_modes):
                c = cs[2 * i + par, :, cut]
                even = lane[:, cut] == par
                left = jnp.concatenate([jnp.where(even, c, 0.0), jnp.where(even, 0.0, c)], axis=0).astype(BF)
                m = b * modes + 2 * i + par
                eo = jnp.dot(left, tab[m, cut, :], preferred_element_type=F32)
                outs[i] = jnp.concatenate([eo[:24] + eo[24:], eo[:24] - eo[24:]], axis=1)
            turned = jnp.swapaxes(outs[...], 0, 1).astype(BF)
            for k in range(24):
                c, r = k // 2, k % 2
                here = pl.ds(pl.multiple_of(r * top + b * half_modes, half_modes), half_modes)
                modes_buf[par, c, here, :] = turned[k]

    def partner_block(source):
        for f in range(4):
            relay(f, source, other).wait_recv()
            if packed[source]:
                relay_packed(f, other).wait_recv()
        transform(source, other)

    def own_block(source):
        transform(source, core)

    near = list(reversed(range(shells // 2, shells)))
    far = list(range(shells // 2))
    for i, source in enumerate(near):
        pass_on(source)
        if i > 0:
            partner_block(near[i - 1])
        own_block(source)
    partner_block(near[-1])
    for source in far:
        pass_on(source)
        own_block(source)
        partner_block(source)

    for copy in consts[3:]:
        copy.wait()

    def synth(c, _):
        for par in range(2):
            grid[par, c] = jnp.dot(trig_ref[par], modes_buf[par, c], preferred_element_type=F32)
        return 0

    lax.fori_loop(0, 12, synth, 0, unroll=True)

    piece = 16

    def product_rows(i, _):
        at_rows = pl.ds(pl.multiple_of((i // 2) * piece, piece), piece)
        at_lanes = pl.ds(pl.multiple_of((i % 2) * width, width), width)
        e = [grid[0, c, at_rows, at_lanes] for c in range(12)]
        o = [grid[1, c, at_rows, at_lanes] for c in range(12)]
        sides = []
        for g in ([a + d for a, d in zip(e, o)], [a - d for a, d in zip(e, o)]):
            u, b, w, j = g[0:3], g[3:6], g[6:9], g[9:12]
            lamb, lorentz, induced = cross(u, w), cross(j, b), cross(u, b)
            sides.append([lamb[n] + lorentz[n] for n in range(3)] + induced)
        for c in range(6):
            prod[0, c, at_rows, at_lanes] = (sides[0][c] + sides[1][c]).astype(BF)
            prod[1, c, at_rows, at_lanes] = (sides[0][c] - sides[1][c]).astype(BF)
        return 0

    lax.fori_loop(0, points // 2 // piece * 2, product_rows, 0)

    def analyse(c, _):
        for par in range(2):
            a = jnp.dot(back_ref[par], prod[par, c], preferred_element_type=F32)
            a = a * w_ref[0:1, :]
            plus, minus = a[:, :width] + a[:, width:], a[:, :width] - a[:, width:]
            for r in range(2):
                cut = slice(r * top, (r + 1) * top)
                asc[par, 2 * c + r] = plus[cut]
                asc[par, 16 + 2 * c + r] = minus[cut]
        return 0

    lax.fori_loop(0, 6, analyse, 0, unroll=True)

    out_lane = lax.broadcasted_iota(jnp.int32, (16, degrees), 1) % 2

    def spectrum(b, low):
        cut = slice(0, degrees) if low else slice(top, degrees)
        for par in range(2):
            here = pl.ds(pl.multiple_of(b * half_modes, half_modes), half_modes)
            turned = jnp.swapaxes(asc[par, :, here, :], 0, 1).astype(BF)
            for i in range(half_modes):
                m = b * modes + 2 * i + par
                both = lax.dot_general(
                    turned[i], tab[m, cut, :], (((1,), (1,)), ((), ())), preferred_element_type=F32)
                souts[2 * i + par, :, cut] = jnp.where(out_lane[:, cut] == par, both[:16], both[16:])
        return jnp.swapaxes(souts[:, :, cut], 0, 1)[:12]

    def ycopy(target):
        low = low_half[target]
        return pltpu.make_async_remote_copy(
            src_ref=ysend.at[target, :, :, lanes(low)], dst_ref=yrecv.at[target, :, :, lanes(low)],
            send_sem=yss.at[target], recv_sem=yrs.at[target],
            device_id=partner, device_id_type=MESH,
        )

    def bcopy(target, shell, low):
        return pltpu.make_async_remote_copy(
            src_ref=zsend.at[target, :, :, :, lanes(low)], dst_ref=land.at[shell, :, :, :, lanes(low)],
            send_sem=bss.at[target], recv_sem=brs.at[shell],
            device_id=mate(target), device_id_type=MESH,
        )

    def bpack(target, shell):
        return pltpu.make_async_remote_copy(
            src_ref=zpack, dst_ref=landp.at[shell],
            send_sem=bps.at[0], recv_sem=bpr.at[shell],
            device_id=mate(target), device_id_type=MESH,
        )

    @pl.when(z * block >= top)
    def _():
        land[:, :, :, :, 0:top] = jnp.zeros((shells, 6, 2, modes, top), BF)

    def finish(target):
        low = low_half[target]
        cut = slice(0, degrees) if low else slice(top, degrees)
        ycopy(target).wait_recv()
        total = (own[target, :, :, cut] + yrecv[target, :, :, cut].astype(F32)).astype(BF)
        total = total.reshape(6, 2, modes, total.shape[-1])
        stays = jnp.logical_and(straight, z == target)

        @pl.when(stays)
        def _():
            land[target, :, :, :, cut] = total

        @pl.when(jnp.logical_not(stays))
        def _():
            zsend[target, :, :, :, cut] = total
            bcopy(target, z, whole[target]).start()
            if packed[target]:
                zpack[...] = jnp.concatenate([total[:, 1, :, mid:top], total[:, 0, :, mid:top]], axis=2)
                bpack(target, z).start()

    for target in range(shells):
        low = low_half[target]
        cut = slice(0, degrees) if low else slice(top, degrees)
        ysend[target, :, :, cut] = spectrum(target * groups + other, low).astype(BF)
        ycopy(target).start()
        if target > 1:
            finish(target - 1)
        own[target, :, :, cut] = spectrum(target * groups + core, low)
        if target == 0:
            finish(0)
    finish(shells - 1)

    upper = lax.broadcasted_iota(jnp.int32, (modes, top), 1) >= mid

    def arrived(shell):
        moved = jnp.logical_not(jnp.logical_and(straight, z == shell))
        for low in (True, False):
            @pl.when(jnp.logical_and(moved, is_whole == low))
            def _(low=low):
                bcopy(shell, shell, low).wait_recv()

        @pl.when(jnp.logical_and(moved, packs))
        def _():
            bpack(shell, shell).wait_recv()
            for k in range(6):
                first = landp[shell, k].astype(F32)
                second = jnp.concatenate([first[:, mid:], first[:, :mid]], axis=1)
                land[shell, k, 0, :, 0:top] = jnp.where(upper, first, 0.0).astype(BF)
                land[shell, k, 1, :, 0:top] = jnp.where(upper, second, 0.0).astype(BF)

    def hcopy(side):
        shell = shells - 1 if side == 0 else 0
        return pltpu.make_async_remote_copy(
            src_ref=land.at[shell, pl.ds(3, 3)], dst_ref=halo.at[side],
            send_sem=hss.at[side], recv_sem=hrs.at[side],
            device_id=rad_up if side == 0 else rad_down, device_id_type=MESH,
        )

    def out_copy(shell):
        return pltpu.make_async_copy(land.at[shell], land_out.at[:, shell], osem.at[shell])

    def halo_copy(side):
        return pltpu.make_async_copy(halo.at[side], halo_out.at[side], osem.at[shells + side])

    arrived(shells - 1)
    hcopy(0).start()
    out_copy(shells - 1).start()
    arrived(0)
    hcopy(1).start()
    out_copy(0).start()
    for step in range(1, harm):
        energy_copy(step).wait_recv()
    energy_out[...] = jnp.sum(energy_all[...], axis=0)
    energy_done = pltpu.make_async_copy(energy_out, energy_hbm, osem.at[shells + 2])
    energy_done.start()
    for shell in range(1, shells - 1):
        arrived(shell)
        out_copy(shell).start()
    for side in range(2):
        hcopy(side).wait_recv()
        halo_copy(side).start()
    for shell in range(shells):
        out_copy(shell).wait()
    for side in range(2):
        halo_copy(side).wait()
    energy_done.wait()
    hcopy(0).wait_send()
    hcopy(1).wait_send()
    for step in range(1, harm):
        energy_copy(step).wait_send()
    def ended(copy):
        copy.wait_send()

    for phase in range(2):
        plain_sends(phase, ended)
        packed_sends(phase, ended)
    for source in range(shells):
        for f in range(4):
            relay(f, source, core).wait_send()
            if packed[source]:
                relay_packed(f, core).wait_send()
        ycopy(source).wait_send()

        @pl.when(jnp.logical_not(jnp.logical_and(straight, z == source)))
        def _(source=source):
            bcopy(source, z, whole[source]).wait_send()
            if packed[source]:
                bpack(source, z).wait_send()


def local_relay(velocity, magnetic, vorticity, current):
    harm, rads = lax.axis_size("harm"), lax.axis_size("rad")
    _, shells, _, modes, degrees = velocity.shape
    thetas, points = 3 * degrees // 2, 3 * degrees
    groups = harm // shells
    x, sect, unscale, w, synthesis, analysis = relay_tables(degrees, thetas, points, groups)
    width = x.shape[2]
    block = groups * modes
    hbm = pl.BlockSpec(memory_space=pl.ANY)
    dims = (rads, harm, shells, groups, modes, degrees, thetas, points)
    dma = pltpu.SemaphoreType.DMA
    consts = (x, sect, unscale, w, synthesis, analysis)
    landed, halo, energy = pl.pallas_call(
        functools.partial(relay_kernel, dims),
        name="dynamo",
        out_shape=(
            jax.ShapeDtypeStruct((6, shells, 2, modes, degrees), BF),
            jax.ShapeDtypeStruct((2, 3, 2, modes, degrees), BF),
            jax.ShapeDtypeStruct((2, shells, degrees), F32),
        ),
        in_specs=[hbm] * 10,
        out_specs=(hbm, hbm, hbm),
        scratch_shapes=[
            *(pltpu.VMEM(c.shape[1:], c.dtype) for c in consts[:4]),
            *(pltpu.VMEM(c.shape, c.dtype) for c in consts[4:]),
            pltpu.VMEM((degrees, degrees, width), BF),
            pltpu.VMEM((16, block, width), F32),
            pltpu.VMEM((harm, 4, 3, 2, modes, degrees), BF),
            pltpu.VMEM((modes, 24, degrees), F32),
            pltpu.VMEM((modes // 2, 24, 2 * width), F32),
            pltpu.VMEM((2, 12, degrees, 2 * width), BF),
            pltpu.VMEM((2, 12, points // 2, 2 * width), F32),
            pltpu.VMEM((2, 6, points // 2, 2 * width), BF),
            pltpu.VMEM((2, 32, degrees // 2, width), F32),
            pltpu.VMEM((modes, 16, degrees), F32),
            pltpu.VMEM((shells, 12, modes, degrees), F32),
            pltpu.VMEM((shells, 12, modes, degrees), BF),
            pltpu.VMEM((shells, 12, modes, degrees), BF),
            pltpu.VMEM((shells, 6, 2, modes, degrees), BF),
            pltpu.VMEM((shells, 6, 2, modes, degrees), BF),
            pltpu.VMEM((2, 3, 2, modes, degrees), BF),
            pltpu.VMEM((harm, 2, shells, degrees), F32),
            pltpu.VMEM((4,) + velocity.shape, BF),
            pltpu.VMEM((4, 3, shells, modes, degrees // 2), BF),
            pltpu.VMEM((groups, 4, 3, modes, degrees // 2), BF),
            pltpu.VMEM((6, modes, degrees // 2), BF),
            pltpu.VMEM((shells, 6, modes, degrees // 2), BF),
            pltpu.VMEM((2, shells, degrees), F32),
            dma((6,)), dma((shells + 3,)), dma((4,)), dma((4,)), dma((shells, 4)), dma((shells, 4)), dma((shells, 4)), dma((shells, 4)),
            dma((shells,)), dma((shells,)), dma((shells,)), dma((shells,)),
            dma((2,)), dma((2,)), dma((harm,)), dma((harm,)),
            dma((shells, 4)), dma((4,)), dma((4,)), dma((4,)), dma((1,)), dma((shells,)),
        ],
        compiler_params=pltpu.CompilerParams(
            collective_id=0, has_side_effects=True, vmem_limit_bytes=62 * 1024 * 1024
        ),
    )(velocity, magnetic, vorticity, current, *(jnp.asarray(c) for c in consts))

    rad = lax.axis_index("rad")
    below = jnp.where(rad > 0, halo[0].astype(F32), 0.0).reshape(3, 1, 2, modes, degrees)
    above = jnp.where(rad < rads - 1, halo[1].astype(F32), 0.0).reshape(3, 1, 2, modes, degrees)
    rimmed = jnp.concatenate([below, landed[3:].astype(F32), above], axis=1)
    gradient = ((rimmed[:, 2:] - rimmed[:, :-2]) * 0.5).astype(BF)
    return landed[:3], gradient, energy


def relay_fits(mesh, args):
    _, total, _, degrees, _ = args[0].shape
    rads, harm = mesh.shape["rad"], mesh.shape["harm"]
    shells, modes = total // rads, degrees // harm
    return harm == 2 * shells and rads > 2 and rads % 2 == 0 and modes % 32 == 0 and degrees % (2 * LANES) == 0


def solution(mesh):
    spec = P(None, "rad", None, "harm", None)

    def run(*args):
        body = local_relay if relay_fits(mesh, args) else local
        return jax.shard_map(
            body,
            mesh=mesh,
            in_specs=(spec,) * 4,
            out_specs=(spec, spec, P(None, "rad", None)),
            check_vma=False,
        )(*args)

    return run
```

```python
import functools

import jax
import jax.numpy as jnp
import numpy as np
from jax import lax
from jax.experimental import pallas as pl
from jax.experimental.pallas import tpu as pltpu
from jax.sharding import PartitionSpec as P

MESH = pl.DeviceIdType.MESH
PASSES = 2
BF = jnp.bfloat16
F32 = jnp.float32


def tables(degrees, thetas, points, harm_count):
    half = thetas // 2
    angles = np.pi * (np.arange(half) + 0.5) / thetas
    cosine = np.concatenate([np.cos(angles), -np.cos(angles)[::-1]])
    sine = np.concatenate([np.sin(angles), np.sin(angles)[::-1]])
    orders = np.arange(degrees)
    steps = np.arange(1, degrees)
    terms = 0.5 * np.log((2.0 * steps + 1.0) / (2.0 * steps))
    start = 0.5 * np.log(0.5) + np.concatenate([[0.0], np.cumsum(terms)])
    log_sector = start[:, None] + orders[:, None] * np.log(sine)[None, :]
    sectoral = np.exp(np.maximum(log_sector, -60.0)).astype(np.float32)
    unscale = np.exp(np.minimum(log_sector + 60.0, 0.0)).astype(np.float32)
    wave = np.arange(1, half + 1)
    series = np.cos(2.0 * wave[None, :] * angles[:, None]) / (4.0 * wave[None, :] ** 2 - 1.0)
    north = 2.0 / thetas * (1.0 - 2.0 * series.sum(axis=1))
    weights = np.concatenate([north, north[::-1]])
    weights = (weights * degrees / points).astype(np.float32)
    phase = 2.0 * np.pi * ((orders[:, None] * np.arange(points)[None, :]) % points) / points
    trig = np.stack([np.cos(phase), np.sin(phase)])
    trig = trig.reshape(2, harm_count, degrees // harm_count, points)
    trig = trig.transpose(1, 0, 2, 3).reshape(2 * degrees, points).astype(jnp.bfloat16)
    doubled = np.where(orders == 0, 1.0, 2.0).reshape(harm_count, 1, -1)
    doubled = np.broadcast_to(doubled, (harm_count, 2, degrees // harm_count)).reshape(-1, 1)
    analysis = (trig.astype(np.float32) * doubled).astype(jnp.bfloat16)
    return cosine.astype(np.float32), sectoral, unscale, weights, trig.T.copy(), analysis


def wide(column, width):
    return jnp.concatenate([column] * (width // column.shape[1]), axis=1)


def kernel(
    dims,
    cm_ref, x_ref, sect_ref, unscale_ref, w_ref, trig_ref, back_ref, energy_ref,
    out_ref, energy_out,
    tab, rows, outs, send, recv, grid, prod, send2, recv2, folded, spread, energy_all,
    ssem, rsem, ssem2, rsem2, esend, erecv,
):
    harm, shells, groups, modes, degrees, thetas, points, span = dims
    me = lax.axis_index("harm")
    pair_width = 2 * span
    block = min(16, modes)
    q_pairs = 6 // PASSES
    q_rows = 12 // PASSES * shells * 2

    barrier = pltpu.get_barrier_semaphore()
    for step in range(1, harm):
        peer = lax.rem(me + step, harm)
        pl.semaphore_signal(barrier, inc=1, device_id={"harm": peer}, device_id_type=MESH)

    order = (me * modes + lax.broadcasted_iota(jnp.int32, (modes, 128), 0)).astype(F32)
    order_square = order * order
    own = pl.ds(pl.multiple_of(me * modes, modes), modes)
    energy_all[me] = energy_ref[...]

    def table_block(step, carry):
        latest, before, inverse = carry
        for inner in range(16):
            degree = step * 16 + inner
            lf = jnp.full((modes, 128), degree, jnp.int32).astype(F32)
            dd = jnp.maximum(lf * lf - order_square, 1.0) / (4.0 * lf * lf - 1.0)
            guess = lax.rsqrt(dd)
            guess = guess * (1.5 - 0.5 * dd * guess * guess)
            live = lf > order
            alpha = jnp.where(live, guess, 0.0)
            starts = jnp.where(lf == order, 1.0, 0.0)
            new = wide(alpha, thetas) * (x_ref[...] * latest - wide(inverse, thetas) * before)
            new = new + wide(starts, thetas) * sect_ref[own, :]
            rows[inner] = new * unscale_ref[own, :]
            before, latest = latest, new
            inverse = jnp.where(live, dd * guess, 0.0)
        tab[:, pl.ds(pl.multiple_of(step * 16, 16), 16), :] = jnp.swapaxes(rows[...], 0, 1).astype(BF)
        return latest, before, inverse

    zero = jnp.zeros((modes, thetas), F32)
    lax.fori_loop(0, degrees // 16, table_block, (zero, zero, jnp.zeros((modes, 128), F32)))

    pl.semaphore_wait(barrier, harm - 1)

    def energy_copy(step):
        peer = lax.rem(me + step, harm)
        return pltpu.make_async_remote_copy(
            src_ref=energy_all.at[me], dst_ref=energy_all.at[me],
            send_sem=esend.at[step], recv_sem=erecv.at[step],
            device_id={"harm": peer}, device_id_type=MESH,
        )

    def forward(q, step):
        peer = lax.rem(me + step, harm)
        return pltpu.make_async_remote_copy(
            src_ref=send.at[peer, pl.ds(q * q_pairs, q_pairs)],
            dst_ref=recv.at[me, pl.ds(q * q_pairs, q_pairs)],
            send_sem=ssem.at[q, step], recv_sem=rsem.at[q, step],
            device_id={"harm": peer}, device_id_type=MESH,
        )

    def backward(pair, step):
        peer = lax.rem(me + step, harm)
        return pltpu.make_async_remote_copy(
            src_ref=send2.at[peer, pair], dst_ref=recv2.at[me, pair],
            send_sem=ssem2.at[pair, step], recv_sem=rsem2.at[pair, step],
            device_id={"harm": peer}, device_id_type=MESH,
        )

    for q in range(PASSES):
        def mode_block(mb, _, q=q):
            def one(i, _):
                m = mb * block + i
                outs[i] = jnp.dot(cm_ref[q, m], tab[m], preferred_element_type=F32) * (1.0 / degrees)
                return 0

            lax.fori_loop(0, block, one, 0, unroll=4)
            turned = jnp.swapaxes(outs[...], 0, 1)
            for s in range(shells):
                for pair in range(q_pairs):
                    for r in range(2):
                        k = (pair * 2 * shells + s) * 2 + r
                        first, second = turned[k], turned[k + 2 * shells]
                        for g in range(groups):
                            cut = slice(g * span, (g + 1) * span)
                            piece = jnp.concatenate([first[:, cut], second[:, cut]], axis=1).astype(BF)
                            at = pl.multiple_of(r * modes + mb * block, block)
                            send[s * groups + g, q * q_pairs + pair, pl.ds(at, block), :] = piece
            return 0

        lax.fori_loop(0, modes // block, mode_block, 0)
        for step in range(1, harm):
            forward(q, step).start()
        recv[me, pl.ds(q * q_pairs, q_pairs)] = send[me, pl.ds(q * q_pairs, q_pairs)]
    for step in range(1, harm):
        energy_copy(step).start()

    chunk = points // 3
    for q in range(PASSES):
        for step in range(1, harm):
            forward(q, step).wait_recv()
        for pair in range(q * q_pairs, (q + 1) * q_pairs):
            arrived = recv[:, pair].reshape(2 * degrees, pair_width)
            for part in range(3):
                cut = pl.ds(part * chunk, chunk)
                grid[pair, cut, :] = jnp.dot(trig_ref[cut, :], arrived, preferred_element_type=F32)

    piece_rows = 32

    def product_rows(i, _):
        at = pl.ds(pl.multiple_of(i * piece_rows, piece_rows), piece_rows)
        both = [grid[pair, at, :] for pair in range(6)]
        c = []
        for pair in range(6):
            c += [both[pair][:, :span], both[pair][:, span:]]
        u, b, w, j = c[0:3], c[3:6], c[6:9], c[9:12]

        def cross(a, d):
            return [a[1] * d[2] - a[2] * d[1], a[2] * d[0] - a[0] * d[2], a[0] * d[1] - a[1] * d[0]]

        lamb, lorentz, induced = cross(u, w), cross(j, b), cross(u, b)
        six = [lamb[n] + lorentz[n] for n in range(3)] + induced
        for pair in range(3):
            prod[pair, at, :] = jnp.concatenate([six[2 * pair], six[2 * pair + 1]], axis=1).astype(BF)
        return 0

    lax.fori_loop(0, points // piece_rows, product_rows, 0)

    per = 2 * modes
    for pair in range(3):
        analysed = jnp.dot(back_ref[...], prod[pair], preferred_element_type=F32)
        analysed = (analysed * w_ref[lax.rem(me, groups)]).astype(BF)
        send2[:, pair] = analysed.reshape(harm, per, pair_width)
        for step in range(1, harm):
            backward(pair, step).start()
        recv2[me, pair] = send2[me, pair]

    for pair in range(3):
        for step in range(1, harm):
            backward(pair, step).wait_recv()

        def fold_block(mb, _, pair=pair):
            for s in range(shells):
                for r in range(2):
                    at = pl.ds(pl.multiple_of(r * modes + mb * block, block), block)
                    got = [recv2[s * groups + g, pair, at, :].astype(F32) for g in range(groups)]
                    for c in range(2):
                        cut = slice(c * span, (c + 1) * span)
                        spread[(c * shells + s) * 2 + r] = jnp.concatenate([v[:, cut] for v in got], axis=1)
            here = pl.ds(pl.multiple_of(mb * block, block), block)
            folded[here, pl.ds(pair * 4 * shells, 4 * shells), :] = jnp.swapaxes(spread[...], 0, 1).astype(BF)
            return 0

        lax.fori_loop(0, modes // block, fold_block, 0)

    def spectrum(m, _):
        out_ref[m] = lax.dot_general(
            folded[m], tab[m], (((1,), (1,)), ((), ())), preferred_element_type=F32
        ).astype(BF)
        return 0

    lax.fori_loop(0, modes, spectrum, 0, unroll=4)

    for step in range(1, harm):
        energy_copy(step).wait_recv()
    energy_out[...] = jnp.sum(energy_all[...], axis=0)
    for step in range(1, harm):
        energy_copy(step).wait_send()
        for q in range(PASSES):
            forward(q, step).wait_send()
        for pair in range(3):
            backward(pair, step).wait_send()


def with_halo(block, axis):
    count = lax.axis_size(axis)
    up = [(i, i + 1) for i in range(count - 1)]
    down = [(b, a) for a, b in up]
    low = lax.ppermute(block[:, -1:], axis, up)
    high = lax.ppermute(block[:, :1], axis, down)
    return jnp.concatenate([low, block, high], axis=1)


def energy_weights(order_ints, degree_count):
    degrees = jnp.arange(degree_count, dtype=jnp.int32)
    order_col = order_ints[:, None]
    live_part = (degrees[None, :] >= order_col).astype(F32)
    inverse_modes = 1.0 / (2.0 * degrees.astype(F32) + 1.0)
    cosine_weight = jnp.where(order_col == 0, 0.5, 1.0)
    sine_weight = jnp.where(order_col == 0, 0.0, 1.0)
    scaled = live_part * inverse_modes[None, :]
    return jnp.stack([cosine_weight * scaled, sine_weight * scaled])


def local(velocity, magnetic, vorticity, current):
    harm = lax.axis_size("harm")
    me = lax.axis_index("harm")
    _, shells, _, modes, degrees = velocity.shape
    thetas, points = 3 * degrees // 2, 3 * degrees
    groups = harm // shells
    span = thetas // groups
    cosine, sectoral, unscale, weights, synthesis, analysis = tables(degrees, thetas, points, harm)

    own = me * modes + jnp.arange(modes, dtype=jnp.int32)
    energy_weight = energy_weights(own, degrees)
    energy = jnp.stack([
        jnp.sum(field.astype(F32) ** 2 * energy_weight[None, None], axis=(0, 2, 3))
        for field in (velocity, magnetic)
    ])

    fields = jnp.concatenate([velocity, magnetic, vorticity, current], axis=0)
    q_rows = 12 // PASSES * shells * 2
    cm = fields.reshape(PASSES, q_rows, modes, degrees).transpose(0, 2, 1, 3)
    x = jnp.asarray(np.broadcast_to(cosine[None, :], (modes, thetas)).copy())
    cut_weights = weights.reshape(groups, 1, span)
    w = jnp.asarray(np.concatenate([cut_weights, cut_weights], axis=2))

    block = min(16, modes)
    vmem = pl.BlockSpec(memory_space=pltpu.VMEM)
    dims = (harm, shells, groups, modes, degrees, thetas, points, span)
    spectra, total = pl.pallas_call(
        functools.partial(kernel, dims),
        name="dynamo",
        out_shape=(
            jax.ShapeDtypeStruct((modes, 12 * shells, degrees), BF),
            jax.ShapeDtypeStruct((2, shells, degrees), F32),
        ),
        in_specs=[vmem] * 8,
        out_specs=(vmem, vmem),
        scratch_shapes=[
            pltpu.VMEM((modes, degrees, thetas), BF),
            pltpu.VMEM((16, modes, thetas), F32),
            pltpu.VMEM((block, q_rows, thetas), F32),
            pltpu.VMEM((harm, 6, 2 * modes, 2 * span), BF),
            pltpu.VMEM((harm, 6, 2 * modes, 2 * span), BF),
            pltpu.VMEM((6, points, 2 * span), F32),
            pltpu.VMEM((3, points, 2 * span), BF),
            pltpu.VMEM((harm, 3, 2 * modes, 2 * span), BF),
            pltpu.VMEM((harm, 3, 2 * modes, 2 * span), BF),
            pltpu.VMEM((modes, 12 * shells, thetas), BF),
            pltpu.VMEM((4 * shells, block, thetas), F32),
            pltpu.VMEM((harm, 2, shells, degrees), F32),
            pltpu.SemaphoreType.DMA((PASSES, harm)),
            pltpu.SemaphoreType.DMA((PASSES, harm)),
            pltpu.SemaphoreType.DMA((3, harm)),
            pltpu.SemaphoreType.DMA((3, harm)),
            pltpu.SemaphoreType.DMA((harm,)),
            pltpu.SemaphoreType.DMA((harm,)),
        ],
        compiler_params=pltpu.CompilerParams(
            collective_id=0, has_side_effects=True, vmem_limit_bytes=60 * 1024 * 1024
        ),
    )(cm, x, jnp.asarray(sectoral), jnp.asarray(unscale), w, jnp.asarray(synthesis), jnp.asarray(analysis), energy)

    spectra = spectra.transpose(1, 0, 2).reshape(6, shells, 2, modes, degrees)
    rimmed = with_halo(spectra[3:], "rad").astype(F32)
    gradient = ((rimmed[:, 2:] - rimmed[:, :-2]) * 0.5).astype(BF)
    return spectra[:3], gradient, total


LANES = 128


def relay_tables(degrees, thetas, points, groups):
    half = thetas // 2
    rows = half // groups
    wide_rows = -(-rows // LANES) * LANES
    cosine, sectoral, unscale, weights, _, _ = tables(degrees, thetas, points, groups)

    def cut(array):
        parts = array[:, :half].reshape(-1, groups, rows).transpose(1, 0, 2)
        return np.pad(parts, ((0, 0), (0, 0), (0, wide_rows - rows)))

    x = cut(np.broadcast_to(cosine[None, :], (8, thetas)))
    w = np.tile(cut(np.broadcast_to(weights[None, :], (8, thetas))), (1, 1, 2))
    orders = np.arange(degrees)
    phase = 2.0 * np.pi * ((orders[:, None] * np.arange(points // 2)[None, :]) % points) / points
    trig = np.stack([np.cos(phase), np.sin(phase)]).astype(jnp.bfloat16).astype(np.float32)
    trig = trig.reshape(2, degrees // 2, 2, points // 2).transpose(2, 0, 1, 3)
    trig = trig.reshape(2, degrees, points // 2)
    doubled = np.where(orders == 0, 1.0, 2.0).reshape(degrees // 2, 2).T
    doubled = np.concatenate([doubled, doubled], axis=1)[:, :, None]
    synthesis = (trig.transpose(0, 2, 1) / degrees).astype(jnp.bfloat16)
    analysis = (trig * doubled).astype(jnp.bfloat16)
    return x, cut(sectoral), cut(unscale), w, synthesis, analysis


def cross(a, d):
    return [a[1] * d[2] - a[2] * d[1], a[2] * d[0] - a[0] * d[2], a[0] * d[1] - a[1] * d[0]]


def relay_kernel(
    dims,
    vel_ref, mag_ref, vor_ref, cur_ref, x_hbm, sect_hbm, unscale_hbm, w_hbm, trig_hbm, back_hbm,
    land_out, halo_out, energy_hbm,
    x_ref, sect_ref, unscale_ref, w_ref, trig_ref, back_ref, tab, rows, rx, cs, outs, modes_buf, grid, prod, asc, souts, own, ysend, yrecv, zsend, land, halo, energy_all, held,
    pack, rxp, zpack, landp, energy_out, csem, osem, lsem, vsem, zss, zrs, rss, rrs, yss, yrs, bss, brs, hss, hrs, esend, erecv, pss, prs, qss, qrs, bps, bpr,
):
    rads, harm, shells, groups, modes, degrees, thetas, points = dims
    me = lax.axis_index("harm")
    rad = lax.axis_index("rad")
    z, y = me // groups, me % groups
    base, core = rad // groups * groups, rad % groups
    other = 1 - core
    straight = core == y
    block = groups * modes
    top = degrees // 2
    fields = (vel_ref, mag_ref, vor_ref, cur_ref)
    low_half = [src * block < top for src in range(shells)]
    packed = [2 * src * block == top for src in range(shells)]
    whole = [low and not half for low, half in zip(low_half, packed)]
    mid = top // 2
    packs = 2 * z * block == top

    def mate(shell):
        return {"rad": base + y, "harm": shell * groups + core}

    partner = {"rad": base + other}

    rad_up = {"rad": lax.rem(rad + 1, rads)}
    rad_down = {"rad": lax.rem(rad + rads - 1, rads)}

    barrier = pltpu.get_barrier_semaphore()
    for step in range(1, harm):
        pl.semaphore_signal(barrier, inc=1, device_id={"harm": lax.rem(me + step, harm)}, device_id_type=MESH)
    for target in (rad_up, rad_down):
        pl.semaphore_signal(barrier, inc=1, device_id=target, device_id_type=MESH)

    @pl.when(jnp.logical_not(straight))
    def _():
        for shell in range(shells):
            pl.semaphore_signal(barrier, inc=1, device_id=mate(shell), device_id_type=MESH)

    def lanes(low):
        return pl.ds(0, degrees) if low else pl.ds(top, degrees - top)

    def zcopy(f, dest, low, source):
        return pltpu.make_async_remote_copy(
            src_ref=fields[f].at[:, dest, :, :, lanes(low)],
            dst_ref=rx.at[me, f, :, :, :, lanes(low)],
            send_sem=zss.at[dest, f], recv_sem=zrs.at[source, f],
            device_id=mate(dest), device_id_type=MESH,
        )

    def relay(f, source, yy):
        slot = rx.at[source * groups + yy, f, :, :, :, lanes(whole[source])]
        return pltpu.make_async_remote_copy(
            src_ref=slot, dst_ref=slot,
            send_sem=rss.at[source, f], recv_sem=rrs.at[source, f],
            device_id=partner, device_id_type=MESH,
        )

    def pcopy(f, dest, source):
        return pltpu.make_async_remote_copy(
            src_ref=pack.at[f, :, dest], dst_ref=rxp.at[y, f],
            send_sem=pss.at[dest, f], recv_sem=prs.at[f],
            device_id=mate(dest), device_id_type=MESH,
        )

    def relay_packed(f, yy):
        return pltpu.make_async_remote_copy(
            src_ref=rxp.at[yy, f], dst_ref=rxp.at[yy, f],
            send_sem=qss.at[f], recv_sem=qrs.at[f],
            device_id=partner, device_id_type=MESH,
        )

    def local_copy(f):
        return pltpu.make_async_copy(fields[f].at[:, z], rx.at[me, f], lsem.at[f])

    def held_copy(f):
        return pltpu.make_async_copy(fields[f], held.at[f], vsem.at[f])

    consts = [
        pltpu.make_async_copy(src, dst, csem.at[i]) for i, (src, dst) in enumerate((
            (x_hbm.at[core], x_ref), (sect_hbm.at[core], sect_ref), (unscale_hbm.at[core], unscale_ref),
            (w_hbm.at[core], w_ref), (trig_hbm, trig_ref), (back_hbm, back_ref)))
    ]
    for copy in consts:
        copy.start()
    for f in range(2):
        held_copy(f).start()

    @pl.when(straight)
    def _():
        for f in range(4):
            local_copy(f).start()

    pl.semaphore_wait(barrier, harm - 1 + 2 + shells * jnp.where(straight, 0, 1))

    def dest_of(j):
        mark = shells - 1 - j
        return mark - jnp.where(mark <= z, 1, 0)

    is_whole = jnp.logical_and(z * block < top, jnp.logical_not(packs))

    def routed(phase, send):
        for j in range(shells - 1):
            if j == 0:
                if phase == 0:
                    send(dest_of(j))
            else:
                crossing = jnp.logical_and(z * block < top, dest_of(j) * block >= top)

                @pl.when(crossing == (phase == 1))
                def _(j=j):
                    send(dest_of(j))
        if phase == 0:
            @pl.when(jnp.logical_not(straight))
            def _():
                send(z)

    def plain_sends(phase, act, early=None):
        for low in (True, False):
            if early is not None and early == low:
                continue

            @pl.when(is_whole == low)
            def _(low=low):
                routed(phase, lambda dest: [act(zcopy(f, dest, low, z)) for f in range(4)])

    def packed_sends(phase, act):
        @pl.when(packs)
        def _():
            routed(phase, lambda dest: [act(pcopy(f, dest, z)) for f in range(4)])

    def begin(copy):
        copy.start()

    plain_sends(0, begin)

    @pl.when(packs)
    def _():
        for f in range(2, 4):
            held_copy(f).start()
        for f in range(4):
            held_copy(f).wait()
            for c in range(3):
                for shell in range(shells):
                    first, second = held[f, c, shell, 0, :, 0:top], held[f, c, shell, 1, :, 0:top]
                    pack[f, c, shell] = jnp.concatenate([second[:, mid:], first[:, mid:]], axis=1)

        @pl.when(straight)
        def _():
            for f in range(4):
                rxp[core, f] = pack[f, :, z]

    packed_sends(0, begin)

    def energy_copy(step):
        peer = lax.rem(me + step, harm)
        return pltpu.make_async_remote_copy(
            src_ref=energy_all.at[me], dst_ref=energy_all.at[me],
            send_sem=esend.at[step], recv_sem=erecv.at[step],
            device_id={"harm": peer}, device_id_type=MESH,
        )

    def pass_on(source):
        for f in range(4):
            @pl.when(jnp.logical_and(straight, z == source))
            def _(f=f):
                local_copy(f).wait()

            @pl.when(jnp.logical_not(jnp.logical_and(straight, z == source)))
            def _(f=f):
                zcopy(f, source, whole[source], source).wait_recv()
                if packed[source]:
                    pcopy(f, source, source).wait_recv()

            relay(f, source, core).start()
            if packed[source]:
                relay_packed(f, core).start()

    for copy in consts[:3]:
        copy.wait()
    x = x_ref[0:1, :]
    width = x.shape[1]
    per = 16

    def table_block(source, starting, step, carry):
        first = source * block
        order = (first + lax.broadcasted_iota(jnp.int32, (block, width), 0)).astype(F32)
        square = order * order
        latest, before, inverse = carry
        for inner in range(per):
            degree = step * per + inner
            lf = jnp.full((1, width), degree, jnp.int32).astype(F32)
            scale = 1.0 / (4.0 * lf * lf - 1.0)
            gap = lf * lf - square
            if starting:
                gap = jnp.maximum(gap, 1.0)
            dd = gap * scale
            guess = lax.rsqrt(dd)
            guess = guess * (1.5 - 0.5 * dd * guess * guess)
            root = dd * guess
            if starting:
                live = lf > order
                guess = jnp.where(live, guess, 0.0)
                root = jnp.where(live, root, 0.0)
            new = guess * (x * latest - inverse * before)
            if starting:
                new = new + jnp.where(lf == order, sect_ref[pl.ds(first, block), :], 0.0)
            rows[inner] = new * unscale_ref[pl.ds(first, block), :]
            before, latest = latest, new
            inverse = root
        here = pl.ds(pl.multiple_of(step * per, per), per)
        tab[pl.ds(first, block), here, :] = jnp.swapaxes(rows[...], 0, 1).astype(BF)
        return latest, before, inverse

    def table_start(source):
        first = source * block
        floor = 0 if low_half[source] else top
        if first > floor:
            tab[pl.ds(first, block), pl.ds(floor, first - floor), :] = jnp.zeros((block, first - floor, width), BF)
        zero = jnp.zeros((block, width), F32)
        return lax.fori_loop(
            first // per, (first + block) // per, functools.partial(table_block, source, True), (zero, zero, zero))

    def table_rest(source, carry, low, high):
        return lax.fori_loop(low, high, functools.partial(table_block, source, False), carry)

    steps = degrees // per
    for source in reversed(range(shells)):
        carry = table_start(source)
        first = (source + 1) * block // per
        turn = first + (steps - first) // 4 if source == 0 else steps
        carry = lax.fori_loop(first, turn, functools.partial(table_block, source, False), carry)
        if source == 1:
            plain_sends(1, begin, early=True)
            packed_sends(1, begin)
        if source == 0:
            plain_sends(1, begin, early=False)
            lax.fori_loop(turn, steps, functools.partial(table_block, source, False), carry)

    @pl.when(jnp.logical_not(packs))
    def _():
        for f in range(2):
            held_copy(f).wait()

    own_order = me * modes + lax.broadcasted_iota(jnp.int32, (modes, degrees), 0)
    degree = lax.broadcasted_iota(jnp.int32, (modes, degrees), 1)
    share = jnp.where(degree >= own_order, 1.0 / (2.0 * degree.astype(F32) + 1.0), 0.0)
    parts = (share * jnp.where(own_order == 0, 0.5, 1.0), share * jnp.where(own_order == 0, 0.0, 1.0))

    def shell_energy(shell, _):
        for f in range(2):
            total = jnp.zeros((modes, degrees), F32)
            for r in range(2):
                square = jnp.zeros((modes, degrees), F32)
                for c in range(3):
                    value = held[f, c, shell, r].astype(F32)
                    square = square + value * value
                total = total + square * parts[r]
            energy_all[me, f, pl.ds(shell, 1), :] = jnp.sum(total, axis=0, keepdims=True)
        return 0

    lax.fori_loop(0, shells, shell_energy, 0)
    for step in range(1, harm):
        energy_copy(step).start()

    lane = lax.broadcasted_iota(jnp.int32, (24, degrees), 1) % 2
    half_modes = modes // 2

    def transform(source, yy):
        b = source * groups + yy
        cut = slice(0, degrees) if low_half[source] else slice(top, degrees)
        direct = slice(0, degrees) if whole[source] else slice(top, degrees)
        cs[:, :, direct] = jnp.swapaxes(
            rx[b].reshape(24, modes, degrees)[:, :, direct].astype(F32), 0, 1)
        if packed[source]:
            first = rxp[yy].reshape(12, 1, modes, top).astype(F32)
            second = jnp.concatenate([first[..., mid:], first[..., :mid]], axis=3)
            both = jnp.concatenate([first, second], axis=1).reshape(24, modes, top)
            cs[:, :, 0:top] = jnp.swapaxes(both, 0, 1)
        for par in range(2):
            for i in range(half_modes):
                c = cs[2 * i + par, :, cut]
                even = lane[:, cut] == par
                left = jnp.concatenate([jnp.where(even, c, 0.0), jnp.where(even, 0.0, c)], axis=0).astype(BF)
                m = b * modes + 2 * i + par
                eo = jnp.dot(left, tab[m, cut, :], preferred_element_type=F32)
                outs[i] = jnp.concatenate([eo[:24] + eo[24:], eo[:24] - eo[24:]], axis=1)
            turned = jnp.swapaxes(outs[...], 0, 1).astype(BF)
            for k in range(24):
                c, r = k // 2, k % 2
                here = pl.ds(pl.multiple_of(r * top + b * half_modes, half_modes), half_modes)
                modes_buf[par, c, here, :] = turned[k]

    def partner_block(source):
        for f in range(4):
            relay(f, source, other).wait_recv()
            if packed[source]:
                relay_packed(f, other).wait_recv()
        transform(source, other)

    def own_block(source):
        transform(source, core)

    near = list(reversed(range(shells // 2, shells)))
    far = list(range(shells // 2))
    for i, source in enumerate(near):
        pass_on(source)
        if i > 0:
            partner_block(near[i - 1])
        own_block(source)
    partner_block(near[-1])
    for source in far:
        pass_on(source)
        own_block(source)
        partner_block(source)

    for copy in consts[3:]:
        copy.wait()

    piece = 16

    def product_rows(i, _):
        at_rows = pl.ds((i // 2) * piece, piece)
        at_lanes = pl.ds((i % 2) * width, width)
        e = [grid[0, c, at_rows, at_lanes] for c in range(12)]
        o = [grid[1, c, at_rows, at_lanes] for c in range(12)]
        sides = []
        for g in ([a + d for a, d in zip(e, o)], [a - d for a, d in zip(e, o)]):
            u, b, w, j = g[0:3], g[3:6], g[6:9], g[9:12]
            lamb, lorentz, induced = cross(u, w), cross(j, b), cross(u, b)
            sides.append([lamb[n] + lorentz[n] for n in range(3)] + induced)
        for c in range(6):
            prod[0, c, at_rows, at_lanes] = (sides[0][c] + sides[1][c]).astype(BF)
            prod[1, c, at_rows, at_lanes] = (sides[0][c] - sides[1][c]).astype(BF)
        return 0


    span = points // 2 // 3
    for part in range(3):
        at_part = slice(part * span, (part + 1) * span)
        for c in range(12):
            for par in range(2):
                grid[par, c, at_part] = jnp.dot(
                    trig_ref[par, at_part], modes_buf[par, c], preferred_element_type=F32)
        if part > 0:
            for i in range((part - 1) * span // piece * 2, part * span // piece * 2):
                product_rows(i, 0)
    for i in range(2 * span // piece * 2, 3 * span // piece * 2):
        product_rows(i, 0)

    def analyse(c, _):
        for par in range(2):
            a = jnp.dot(back_ref[par], prod[par, c], preferred_element_type=F32)
            a = a * w_ref[0:1, :]
            plus, minus = a[:, :width] + a[:, width:], a[:, :width] - a[:, width:]
            for r in range(2):
                cut = slice(r * top, (r + 1) * top)
                asc[par, 2 * c + r] = plus[cut]
                asc[par, 16 + 2 * c + r] = minus[cut]
        return 0

    lax.fori_loop(0, 6, analyse, 0, unroll=True)

    out_lane = lax.broadcasted_iota(jnp.int32, (16, degrees), 1) % 2

    sides = (slice(0, top), slice(top, degrees), slice(0, degrees))

    def spectrum(b, part):
        cut = sides[part]
        for par in range(2):
            here = pl.ds(pl.multiple_of(b * half_modes, half_modes), half_modes)
            turned = jnp.swapaxes(asc[par, :, here, :], 0, 1).astype(BF)
            for i in range(half_modes):
                m = b * modes + 2 * i + par
                both = lax.dot_general(
                    turned[i], tab[m, cut, :], (((1,), (1,)), ((), ())), preferred_element_type=F32)
                souts[2 * i + par, :, cut] = jnp.where(out_lane[:, cut] == par, both[:16], both[16:])
        return jnp.swapaxes(souts[:, :, cut], 0, 1)[:12]

    def ycopy(target, part):
        here = pl.ds(0, degrees) if part == 2 else pl.ds(part * top, top)
        return pltpu.make_async_remote_copy(
            src_ref=ysend.at[target, :, :, here], dst_ref=yrecv.at[target, :, :, here],
            send_sem=yss.at[target, part % 2], recv_sem=yrs.at[target, part % 2],
            device_id=partner, device_id_type=MESH,
        )

    def bcopy(target, shell, part):
        here = pl.ds(part * top, top)
        return pltpu.make_async_remote_copy(
            src_ref=zsend.at[target, :, :, :, here], dst_ref=land.at[shell, :, :, :, here],
            send_sem=bss.at[target, part], recv_sem=brs.at[shell, part],
            device_id=mate(target), device_id_type=MESH,
        )

    def bpack(target, shell):
        return pltpu.make_async_remote_copy(
            src_ref=zpack, dst_ref=landp.at[shell],
            send_sem=bps.at[0], recv_sem=bpr.at[shell],
            device_id=mate(target), device_id_type=MESH,
        )

    @pl.when(z * block >= top)
    def _():
        land[:, :, :, :, 0:top] = jnp.zeros((shells, 6, 2, modes, top), BF)

    def returned(target, part, shell):
        copies = []
        if part != 0:
            copies.append(bcopy(target, shell, 1))
        if part != 1:
            copies.append(bpack(target, shell) if packed[target] else bcopy(target, shell, 0))
        return copies

    def finish(target, part):
        cut = sides[part]
        ycopy(target, part).wait_recv()
        total = (own[target, :, :, cut] + yrecv[target, :, :, cut].astype(F32)).astype(BF)
        total = total.reshape(6, 2, modes, total.shape[-1])
        stays = jnp.logical_and(straight, z == target)

        @pl.when(stays)
        def _():
            land[target, :, :, :, cut] = total

        @pl.when(jnp.logical_not(stays))
        def _():
            zsend[target, :, :, :, cut] = total
            if part != 1 and packed[target]:
                zpack[...] = jnp.concatenate([total[:, 1, :, mid:top], total[:, 0, :, mid:top]], axis=2)
            for copy in returned(target, part, z):
                copy.start()

    upper = lax.broadcasted_iota(jnp.int32, (modes, top), 1) >= mid

    def arrived(shell):
        moved = jnp.logical_not(jnp.logical_and(straight, z == shell))
        @pl.when(moved)
        def _():
            bcopy(shell, shell, 1).wait_recv()

        @pl.when(jnp.logical_and(moved, is_whole))
        def _():
            bcopy(shell, shell, 0).wait_recv()

        @pl.when(jnp.logical_and(moved, packs))
        def _():
            bpack(shell, shell).wait_recv()
            for k in range(6):
                first = landp[shell, k].astype(F32)
                second = jnp.concatenate([first[:, mid:], first[:, :mid]], axis=1)
                land[shell, k, 0, :, 0:top] = jnp.where(upper, first, 0.0).astype(BF)
                land[shell, k, 1, :, 0:top] = jnp.where(upper, second, 0.0).astype(BF)

    def hcopy(side):
        shell = shells - 1 if side == 0 else 0
        return pltpu.make_async_remote_copy(
            src_ref=land.at[shell, pl.ds(3, 3)], dst_ref=halo.at[side],
            send_sem=hss.at[side], recv_sem=hrs.at[side],
            device_id=rad_up if side == 0 else rad_down, device_id_type=MESH,
        )

    def out_copy(shell):
        return pltpu.make_async_copy(land.at[shell], land_out.at[:, shell], osem.at[shell])

    def halo_copy(side):
        return pltpu.make_async_copy(halo.at[side], halo_out.at[side], osem.at[shells + side])

    def edges_out():
        arrived(shells - 1)
        hcopy(0).start()
        out_copy(shells - 1).start()
        arrived(0)
        hcopy(1).start()
        out_copy(0).start()

    late = z == shells // 2
    pieces = [(0, 1), (0, 0)] + [(target, 2 if low_half[target] else 1) for target in range(1, shells)]
    for i, (target, part) in enumerate(pieces):
        ysend[target, :, :, sides[part]] = spectrum(target * groups + other, part).astype(BF)
        ycopy(target, part).start()
        if i > 0:
            finish(*pieces[i - 1])
        own[target, :, :, sides[part]] = spectrum(target * groups + core, part)
        if i == len(pieces) - 2:
            pl.when(late)(edges_out)
    finish(*pieces[-1])
    pl.when(jnp.logical_not(late))(edges_out)

    for step in range(1, harm):
        energy_copy(step).wait_recv()
    energy_out[...] = jnp.sum(energy_all[...], axis=0)
    energy_done = pltpu.make_async_copy(energy_out, energy_hbm, osem.at[shells + 2])
    energy_done.start()
    for shell in range(1, shells - 1):
        arrived(shell)
        out_copy(shell).start()
    for side in range(2):
        hcopy(side).wait_recv()
        halo_copy(side).start()
    for shell in range(shells):
        out_copy(shell).wait()
    for side in range(2):
        halo_copy(side).wait()
    energy_done.wait()
    hcopy(0).wait_send()
    hcopy(1).wait_send()
    for step in range(1, harm):
        energy_copy(step).wait_send()
    def ended(copy):
        copy.wait_send()

    for phase in range(2):
        plain_sends(phase, ended)
        packed_sends(phase, ended)
    for source in range(shells):
        for f in range(4):
            relay(f, source, core).wait_send()
            if packed[source]:
                relay_packed(f, core).wait_send()

    for target, part in pieces:
        ycopy(target, part).wait_send()

        @pl.when(jnp.logical_not(jnp.logical_and(straight, z == target)))
        def _(target=target, part=part):
            for copy in returned(target, part, z):
                copy.wait_send()


def closing_kernel(
    rads, shells, landed, halo, energy, adv_out, grad_out, energy_out, adv, ind, grad, rim, total, isem, osem
):
    rad = lax.axis_index("rad")
    copy = pltpu.make_async_copy
    halos = copy(halo, rim, isem.at[0])
    induced = [copy(landed.at[pl.ds(3, 3), s], ind.at[:, s], isem.at[3 + s]) for s in range(shells)]
    advected = copy(landed.at[pl.ds(0, 3)], adv, isem.at[1])
    energies = copy(energy, total, isem.at[2])
    halos.start()
    for shell in induced:
        shell.start()
    advected.start()
    energies.start()
    outs = [copy(grad.at[:, s], grad_out.at[:, s], osem.at[2 + s]) for s in range(shells)]
    outs += [copy(adv, adv_out, osem.at[0]), copy(total, energy_out, osem.at[1])]
    halos.wait()
    induced[0].wait()
    for s in range(shells):
        if s + 1 < shells:
            induced[s + 1].wait()
            after = ind[:, s + 1].astype(F32)
        else:
            after = jnp.where(rad < rads - 1, rim[1].astype(F32), 0.0)
        before = ind[:, s - 1].astype(F32) if s > 0 else jnp.where(rad > 0, rim[0].astype(F32), 0.0)
        grad[:, s] = ((after - before) * 0.5).astype(BF)
        outs[s].start()
    advected.wait()
    outs[shells].start()
    energies.wait()
    outs[shells + 1].start()
    for out in outs:
        out.wait()


def local_relay(velocity, magnetic, vorticity, current):
    harm, rads = lax.axis_size("harm"), lax.axis_size("rad")
    _, shells, _, modes, degrees = velocity.shape
    thetas, points = 3 * degrees // 2, 3 * degrees
    groups = harm // shells
    x, sect, unscale, w, synthesis, analysis = relay_tables(degrees, thetas, points, groups)
    width = x.shape[2]
    block = groups * modes
    hbm = pl.BlockSpec(memory_space=pl.ANY)
    dims = (rads, harm, shells, groups, modes, degrees, thetas, points)
    dma = pltpu.SemaphoreType.DMA
    consts = (x, sect, unscale, w, synthesis, analysis)
    landed, halo, energy = pl.pallas_call(
        functools.partial(relay_kernel, dims),
        name="dynamo",
        out_shape=(
            jax.ShapeDtypeStruct((6, shells, 2, modes, degrees), BF),
            jax.ShapeDtypeStruct((2, 3, 2, modes, degrees), BF),
            jax.ShapeDtypeStruct((2, shells, degrees), F32),
        ),
        in_specs=[hbm] * 10,
        out_specs=(hbm, hbm, hbm),
        scratch_shapes=[
            *(pltpu.VMEM(c.shape[1:], c.dtype) for c in consts[:4]),
            *(pltpu.VMEM(c.shape, c.dtype) for c in consts[4:]),
            pltpu.VMEM((degrees, degrees, width), BF),
            pltpu.VMEM((16, block, width), F32),
            pltpu.VMEM((harm, 4, 3, 2, modes, degrees), BF),
            pltpu.VMEM((modes, 24, degrees), F32),
            pltpu.VMEM((modes // 2, 24, 2 * width), F32),
            pltpu.VMEM((2, 12, degrees, 2 * width), BF),
            pltpu.VMEM((2, 12, points // 2, 2 * width), F32),
            pltpu.VMEM((2, 6, points // 2, 2 * width), BF),
            pltpu.VMEM((2, 32, degrees // 2, width), F32),
            pltpu.VMEM((modes, 16, degrees), F32),
            pltpu.VMEM((shells, 12, modes, degrees), F32),
            pltpu.VMEM((shells, 12, modes, degrees), BF),
            pltpu.VMEM((shells, 12, modes, degrees), BF),
            pltpu.VMEM((shells, 6, 2, modes, degrees), BF),
            pltpu.VMEM((shells, 6, 2, modes, degrees), BF),
            pltpu.VMEM((2, 3, 2, modes, degrees), BF),
            pltpu.VMEM((harm, 2, shells, degrees), F32),
            pltpu.VMEM((4,) + velocity.shape, BF),
            pltpu.VMEM((4, 3, shells, modes, degrees // 2), BF),
            pltpu.VMEM((groups, 4, 3, modes, degrees // 2), BF),
            pltpu.VMEM((6, modes, degrees // 2), BF),
            pltpu.VMEM((shells, 6, modes, degrees // 2), BF),
            pltpu.VMEM((2, shells, degrees), F32),
            dma((6,)), dma((shells + 3,)), dma((4,)), dma((4,)), dma((shells, 4)), dma((shells, 4)), dma((shells, 4)), dma((shells, 4)),
            dma((shells, 2)), dma((shells, 2)), dma((shells, 2)), dma((shells, 2)),
            dma((2,)), dma((2,)), dma((harm,)), dma((harm,)),
            dma((shells, 4)), dma((4,)), dma((4,)), dma((4,)), dma((1,)), dma((shells,)),
        ],
        compiler_params=pltpu.CompilerParams(
            collective_id=0, has_side_effects=True, vmem_limit_bytes=62 * 1024 * 1024
        ),
    )(velocity, magnetic, vorticity, current, *(jnp.asarray(c) for c in consts))

    half = (3,) + landed.shape[1:]
    return pl.pallas_call(
        functools.partial(closing_kernel, rads, shells),
        name="closing",
        out_shape=(
            jax.ShapeDtypeStruct(half, BF),
            jax.ShapeDtypeStruct(half, BF),
            jax.ShapeDtypeStruct(energy.shape, F32),
        ),
        in_specs=[hbm] * 3,
        out_specs=(hbm, hbm, hbm),
        scratch_shapes=[
            pltpu.VMEM(half, BF), pltpu.VMEM(half, BF), pltpu.VMEM(half, BF),
            pltpu.VMEM(halo.shape, BF), pltpu.VMEM(energy.shape, F32), dma((5 + shells,)), dma((2 + shells,)),
        ],
    )(landed, halo, energy)


def relay_fits(mesh, args):
    _, total, _, degrees, _ = args[0].shape
    rads, harm = mesh.shape["rad"], mesh.shape["harm"]
    shells, modes = total // rads, degrees // harm
    return harm == 2 * shells and rads > 2 and rads % 2 == 0 and modes % 32 == 0 and degrees % (2 * LANES) == 0


def solution(mesh):
    spec = P(None, "rad", None, "harm", None)

    def run(*args):
        body = local_relay if relay_fits(mesh, args) else local
        return jax.shard_map(
            body,
            mesh=mesh,
            in_specs=(spec,) * 4,
            out_specs=(spec, spec, P(None, "rad", None)),
            check_vma=False,
        )(*args)

    return run
```

```python
import functools

import jax
import jax.numpy as jnp
import numpy as np
from jax import lax
from jax.experimental import pallas as pl
from jax.experimental.pallas import tpu as pltpu
from jax.sharding import PartitionSpec as P

MESH = pl.DeviceIdType.MESH
PASSES = 2
BF = jnp.bfloat16
F32 = jnp.float32


def tables(degrees, thetas, points, harm_count):
    half = thetas // 2
    angles = np.pi * (np.arange(half) + 0.5) / thetas
    cosine = np.concatenate([np.cos(angles), -np.cos(angles)[::-1]])
    sine = np.concatenate([np.sin(angles), np.sin(angles)[::-1]])
    orders = np.arange(degrees)
    steps = np.arange(1, degrees)
    terms = 0.5 * np.log((2.0 * steps + 1.0) / (2.0 * steps))
    start = 0.5 * np.log(0.5) + np.concatenate([[0.0], np.cumsum(terms)])
    log_sector = start[:, None] + orders[:, None] * np.log(sine)[None, :]
    sectoral = np.exp(np.maximum(log_sector, -60.0)).astype(np.float32)
    unscale = np.exp(np.minimum(log_sector + 60.0, 0.0)).astype(np.float32)
    wave = np.arange(1, half + 1)
    series = np.cos(2.0 * wave[None, :] * angles[:, None]) / (4.0 * wave[None, :] ** 2 - 1.0)
    north = 2.0 / thetas * (1.0 - 2.0 * series.sum(axis=1))
    weights = np.concatenate([north, north[::-1]])
    weights = (weights * degrees / points).astype(np.float32)
    phase = 2.0 * np.pi * ((orders[:, None] * np.arange(points)[None, :]) % points) / points
    trig = np.stack([np.cos(phase), np.sin(phase)])
    trig = trig.reshape(2, harm_count, degrees // harm_count, points)
    trig = trig.transpose(1, 0, 2, 3).reshape(2 * degrees, points).astype(jnp.bfloat16)
    doubled = np.where(orders == 0, 1.0, 2.0).reshape(harm_count, 1, -1)
    doubled = np.broadcast_to(doubled, (harm_count, 2, degrees // harm_count)).reshape(-1, 1)
    analysis = (trig.astype(np.float32) * doubled).astype(jnp.bfloat16)
    return cosine.astype(np.float32), sectoral, unscale, weights, trig.T.copy(), analysis


def wide(column, width):
    return jnp.concatenate([column] * (width // column.shape[1]), axis=1)


def kernel(
    dims,
    cm_ref, x_ref, sect_ref, unscale_ref, w_ref, trig_ref, back_ref, energy_ref,
    out_ref, energy_out,
    tab, rows, outs, send, recv, grid, prod, send2, recv2, folded, spread, energy_all,
    ssem, rsem, ssem2, rsem2, esend, erecv,
):
    harm, shells, groups, modes, degrees, thetas, points, span = dims
    me = lax.axis_index("harm")
    pair_width = 2 * span
    block = min(16, modes)
    q_pairs = 6 // PASSES
    q_rows = 12 // PASSES * shells * 2

    barrier = pltpu.get_barrier_semaphore()
    for step in range(1, harm):
        peer = lax.rem(me + step, harm)
        pl.semaphore_signal(barrier, inc=1, device_id={"harm": peer}, device_id_type=MESH)

    order = (me * modes + lax.broadcasted_iota(jnp.int32, (modes, 128), 0)).astype(F32)
    order_square = order * order
    own = pl.ds(pl.multiple_of(me * modes, modes), modes)
    energy_all[me] = energy_ref[...]

    def table_block(step, carry):
        latest, before, inverse = carry
        for inner in range(16):
            degree = step * 16 + inner
            lf = jnp.full((modes, 128), degree, jnp.int32).astype(F32)
            dd = jnp.maximum(lf * lf - order_square, 1.0) / (4.0 * lf * lf - 1.0)
            guess = lax.rsqrt(dd)
            guess = guess * (1.5 - 0.5 * dd * guess * guess)
            live = lf > order
            alpha = jnp.where(live, guess, 0.0)
            starts = jnp.where(lf == order, 1.0, 0.0)
            new = wide(alpha, thetas) * (x_ref[...] * latest - wide(inverse, thetas) * before)
            new = new + wide(starts, thetas) * sect_ref[own, :]
            rows[inner] = new * unscale_ref[own, :]
            before, latest = latest, new
            inverse = jnp.where(live, dd * guess, 0.0)
        tab[:, pl.ds(pl.multiple_of(step * 16, 16), 16), :] = jnp.swapaxes(rows[...], 0, 1).astype(BF)
        return latest, before, inverse

    zero = jnp.zeros((modes, thetas), F32)
    lax.fori_loop(0, degrees // 16, table_block, (zero, zero, jnp.zeros((modes, 128), F32)))

    pl.semaphore_wait(barrier, harm - 1)

    def energy_copy(step):
        peer = lax.rem(me + step, harm)
        return pltpu.make_async_remote_copy(
            src_ref=energy_all.at[me], dst_ref=energy_all.at[me],
            send_sem=esend.at[step], recv_sem=erecv.at[step],
            device_id={"harm": peer}, device_id_type=MESH,
        )

    def forward(q, step):
        peer = lax.rem(me + step, harm)
        return pltpu.make_async_remote_copy(
            src_ref=send.at[peer, pl.ds(q * q_pairs, q_pairs)],
            dst_ref=recv.at[me, pl.ds(q * q_pairs, q_pairs)],
            send_sem=ssem.at[q, step], recv_sem=rsem.at[q, step],
            device_id={"harm": peer}, device_id_type=MESH,
        )

    def backward(pair, step):
        peer = lax.rem(me + step, harm)
        return pltpu.make_async_remote_copy(
            src_ref=send2.at[peer, pair], dst_ref=recv2.at[me, pair],
            send_sem=ssem2.at[pair, step], recv_sem=rsem2.at[pair, step],
            device_id={"harm": peer}, device_id_type=MESH,
        )

    for q in range(PASSES):
        def mode_block(mb, _, q=q):
            def one(i, _):
                m = mb * block + i
                outs[i] = jnp.dot(cm_ref[q, m], tab[m], preferred_element_type=F32) * (1.0 / degrees)
                return 0

            lax.fori_loop(0, block, one, 0, unroll=4)
            turned = jnp.swapaxes(outs[...], 0, 1)
            for s in range(shells):
                for pair in range(q_pairs):
                    for r in range(2):
                        k = (pair * 2 * shells + s) * 2 + r
                        first, second = turned[k], turned[k + 2 * shells]
                        for g in range(groups):
                            cut = slice(g * span, (g + 1) * span)
                            piece = jnp.concatenate([first[:, cut], second[:, cut]], axis=1).astype(BF)
                            at = pl.multiple_of(r * modes + mb * block, block)
                            send[s * groups + g, q * q_pairs + pair, pl.ds(at, block), :] = piece
            return 0

        lax.fori_loop(0, modes // block, mode_block, 0)
        for step in range(1, harm):
            forward(q, step).start()
        recv[me, pl.ds(q * q_pairs, q_pairs)] = send[me, pl.ds(q * q_pairs, q_pairs)]
    for step in range(1, harm):
        energy_copy(step).start()

    chunk = points // 3
    for q in range(PASSES):
        for step in range(1, harm):
            forward(q, step).wait_recv()
        for pair in range(q * q_pairs, (q + 1) * q_pairs):
            arrived = recv[:, pair].reshape(2 * degrees, pair_width)
            for part in range(3):
                cut = pl.ds(part * chunk, chunk)
                grid[pair, cut, :] = jnp.dot(trig_ref[cut, :], arrived, preferred_element_type=F32)

    piece_rows = 32

    def product_rows(i, _):
        at = pl.ds(pl.multiple_of(i * piece_rows, piece_rows), piece_rows)
        both = [grid[pair, at, :] for pair in range(6)]
        c = []
        for pair in range(6):
            c += [both[pair][:, :span], both[pair][:, span:]]
        u, b, w, j = c[0:3], c[3:6], c[6:9], c[9:12]

        def cross(a, d):
            return [a[1] * d[2] - a[2] * d[1], a[2] * d[0] - a[0] * d[2], a[0] * d[1] - a[1] * d[0]]

        lamb, lorentz, induced = cross(u, w), cross(j, b), cross(u, b)
        six = [lamb[n] + lorentz[n] for n in range(3)] + induced
        for pair in range(3):
            prod[pair, at, :] = jnp.concatenate([six[2 * pair], six[2 * pair + 1]], axis=1).astype(BF)
        return 0

    lax.fori_loop(0, points // piece_rows, product_rows, 0)

    per = 2 * modes
    for pair in range(3):
        analysed = jnp.dot(back_ref[...], prod[pair], preferred_element_type=F32)
        analysed = (analysed * w_ref[lax.rem(me, groups)]).astype(BF)
        send2[:, pair] = analysed.reshape(harm, per, pair_width)
        for step in range(1, harm):
            backward(pair, step).start()
        recv2[me, pair] = send2[me, pair]

    for pair in range(3):
        for step in range(1, harm):
            backward(pair, step).wait_recv()

        def fold_block(mb, _, pair=pair):
            for s in range(shells):
                for r in range(2):
                    at = pl.ds(pl.multiple_of(r * modes + mb * block, block), block)
                    got = [recv2[s * groups + g, pair, at, :].astype(F32) for g in range(groups)]
                    for c in range(2):
                        cut = slice(c * span, (c + 1) * span)
                        spread[(c * shells + s) * 2 + r] = jnp.concatenate([v[:, cut] for v in got], axis=1)
            here = pl.ds(pl.multiple_of(mb * block, block), block)
            folded[here, pl.ds(pair * 4 * shells, 4 * shells), :] = jnp.swapaxes(spread[...], 0, 1).astype(BF)
            return 0

        lax.fori_loop(0, modes // block, fold_block, 0)

    def spectrum(m, _):
        out_ref[m] = lax.dot_general(
            folded[m], tab[m], (((1,), (1,)), ((), ())), preferred_element_type=F32
        ).astype(BF)
        return 0

    lax.fori_loop(0, modes, spectrum, 0, unroll=4)

    for step in range(1, harm):
        energy_copy(step).wait_recv()
    energy_out[...] = jnp.sum(energy_all[...], axis=0)
    for step in range(1, harm):
        energy_copy(step).wait_send()
        for q in range(PASSES):
            forward(q, step).wait_send()
        for pair in range(3):
            backward(pair, step).wait_send()


def with_halo(block, axis):
    count = lax.axis_size(axis)
    up = [(i, i + 1) for i in range(count - 1)]
    down = [(b, a) for a, b in up]
    low = lax.ppermute(block[:, -1:], axis, up)
    high = lax.ppermute(block[:, :1], axis, down)
    return jnp.concatenate([low, block, high], axis=1)


def energy_weights(order_ints, degree_count):
    degrees = jnp.arange(degree_count, dtype=jnp.int32)
    order_col = order_ints[:, None]
    live_part = (degrees[None, :] >= order_col).astype(F32)
    inverse_modes = 1.0 / (2.0 * degrees.astype(F32) + 1.0)
    cosine_weight = jnp.where(order_col == 0, 0.5, 1.0)
    sine_weight = jnp.where(order_col == 0, 0.0, 1.0)
    scaled = live_part * inverse_modes[None, :]
    return jnp.stack([cosine_weight * scaled, sine_weight * scaled])


def local(velocity, magnetic, vorticity, current):
    harm = lax.axis_size("harm")
    me = lax.axis_index("harm")
    _, shells, _, modes, degrees = velocity.shape
    thetas, points = 3 * degrees // 2, 3 * degrees
    groups = harm // shells
    span = thetas // groups
    cosine, sectoral, unscale, weights, synthesis, analysis = tables(degrees, thetas, points, harm)

    own = me * modes + jnp.arange(modes, dtype=jnp.int32)
    energy_weight = energy_weights(own, degrees)
    energy = jnp.stack([
        jnp.sum(field.astype(F32) ** 2 * energy_weight[None, None], axis=(0, 2, 3))
        for field in (velocity, magnetic)
    ])

    fields = jnp.concatenate([velocity, magnetic, vorticity, current], axis=0)
    q_rows = 12 // PASSES * shells * 2
    cm = fields.reshape(PASSES, q_rows, modes, degrees).transpose(0, 2, 1, 3)
    x = jnp.asarray(np.broadcast_to(cosine[None, :], (modes, thetas)).copy())
    cut_weights = weights.reshape(groups, 1, span)
    w = jnp.asarray(np.concatenate([cut_weights, cut_weights], axis=2))

    block = min(16, modes)
    vmem = pl.BlockSpec(memory_space=pltpu.VMEM)
    dims = (harm, shells, groups, modes, degrees, thetas, points, span)
    spectra, total = pl.pallas_call(
        functools.partial(kernel, dims),
        name="dynamo",
        out_shape=(
            jax.ShapeDtypeStruct((modes, 12 * shells, degrees), BF),
            jax.ShapeDtypeStruct((2, shells, degrees), F32),
        ),
        in_specs=[vmem] * 8,
        out_specs=(vmem, vmem),
        scratch_shapes=[
            pltpu.VMEM((modes, degrees, thetas), BF),
            pltpu.VMEM((16, modes, thetas), F32),
            pltpu.VMEM((block, q_rows, thetas), F32),
            pltpu.VMEM((harm, 6, 2 * modes, 2 * span), BF),
            pltpu.VMEM((harm, 6, 2 * modes, 2 * span), BF),
            pltpu.VMEM((6, points, 2 * span), F32),
            pltpu.VMEM((3, points, 2 * span), BF),
            pltpu.VMEM((harm, 3, 2 * modes, 2 * span), BF),
            pltpu.VMEM((harm, 3, 2 * modes, 2 * span), BF),
            pltpu.VMEM((modes, 12 * shells, thetas), BF),
            pltpu.VMEM((4 * shells, block, thetas), F32),
            pltpu.VMEM((harm, 2, shells, degrees), F32),
            pltpu.SemaphoreType.DMA((PASSES, harm)),
            pltpu.SemaphoreType.DMA((PASSES, harm)),
            pltpu.SemaphoreType.DMA((3, harm)),
            pltpu.SemaphoreType.DMA((3, harm)),
            pltpu.SemaphoreType.DMA((harm,)),
            pltpu.SemaphoreType.DMA((harm,)),
        ],
        compiler_params=pltpu.CompilerParams(
            collective_id=0, has_side_effects=True, vmem_limit_bytes=60 * 1024 * 1024
        ),
    )(cm, x, jnp.asarray(sectoral), jnp.asarray(unscale), w, jnp.asarray(synthesis), jnp.asarray(analysis), energy)

    spectra = spectra.transpose(1, 0, 2).reshape(6, shells, 2, modes, degrees)
    rimmed = with_halo(spectra[3:], "rad").astype(F32)
    gradient = ((rimmed[:, 2:] - rimmed[:, :-2]) * 0.5).astype(BF)
    return spectra[:3], gradient, total


LANES = 128


def relay_tables(degrees, thetas, points, groups):
    half = thetas // 2
    rows = half // groups
    wide_rows = -(-rows // LANES) * LANES
    cosine, sectoral, unscale, weights, _, _ = tables(degrees, thetas, points, groups)

    def cut(array):
        parts = array[:, :half].reshape(-1, groups, rows).transpose(1, 0, 2)
        return np.pad(parts, ((0, 0), (0, 0), (0, wide_rows - rows)))

    x = cut(np.broadcast_to(cosine[None, :], (8, thetas)))
    w = np.tile(cut(np.broadcast_to(weights[None, :], (8, thetas))), (1, 1, 2))
    orders = np.arange(degrees)
    phase = 2.0 * np.pi * ((orders[:, None] * np.arange(points // 2)[None, :]) % points) / points
    trig = np.stack([np.cos(phase), np.sin(phase)]).astype(jnp.bfloat16).astype(np.float32)
    trig = trig.reshape(2, degrees // 2, 2, points // 2).transpose(2, 0, 1, 3)
    trig = trig.reshape(2, degrees, points // 2)
    doubled = np.where(orders == 0, 1.0, 2.0).reshape(degrees // 2, 2).T
    doubled = np.concatenate([doubled, doubled], axis=1)[:, :, None]
    synthesis = (trig.transpose(0, 2, 1) / degrees).astype(jnp.bfloat16)
    analysis = (trig * doubled).astype(jnp.bfloat16)
    return x, cut(sectoral), cut(unscale), w, synthesis, analysis


def cross(a, d):
    return [a[1] * d[2] - a[2] * d[1], a[2] * d[0] - a[0] * d[2], a[0] * d[1] - a[1] * d[0]]


def relay_kernel(
    dims,
    vel_ref, mag_ref, vor_ref, cur_ref, x_hbm, sect_hbm, unscale_hbm, w_hbm, trig_hbm, back_hbm,
    land_out, halo_out, energy_hbm,
    x_ref, sect_ref, unscale_ref, w_ref, trig_ref, back_ref, tab, rows, rx, cs, outs, modes_buf, grid, prod, asc, souts, own, ysend, yrecv, zsend, land, halo, energy_all, held,
    pack, rxp, zpack, landp, energy_out, csem, osem, lsem, vsem, zss, zrs, rss, rrs, yss, yrs, bss, brs, hss, hrs, esend, erecv, pss, prs, qss, qrs, bps, bpr,
):
    rads, harm, shells, groups, modes, degrees, thetas, points = dims
    me = lax.axis_index("harm")
    rad = lax.axis_index("rad")
    z, y = me // groups, me % groups
    base, core = rad // groups * groups, rad % groups
    other = 1 - core
    straight = core == y
    block = groups * modes
    top = degrees // 2
    fields = (vel_ref, mag_ref, vor_ref, cur_ref)
    low_half = [src * block < top for src in range(shells)]
    packed = [2 * src * block == top for src in range(shells)]
    whole = [low and not half for low, half in zip(low_half, packed)]
    mid = top // 2
    packs = 2 * z * block == top

    def mate(shell):
        return {"rad": base + y, "harm": shell * groups + core}

    partner = {"rad": base + other}

    rad_up = {"rad": lax.rem(rad + 1, rads)}
    rad_down = {"rad": lax.rem(rad + rads - 1, rads)}

    barrier = pltpu.get_barrier_semaphore()
    for step in range(1, harm):
        pl.semaphore_signal(barrier, inc=1, device_id={"harm": lax.rem(me + step, harm)}, device_id_type=MESH)
    for target in (rad_up, rad_down):
        pl.semaphore_signal(barrier, inc=1, device_id=target, device_id_type=MESH)

    @pl.when(jnp.logical_not(straight))
    def _():
        for shell in range(shells):
            pl.semaphore_signal(barrier, inc=1, device_id=mate(shell), device_id_type=MESH)

    def lanes(low):
        return pl.ds(0, degrees) if low else pl.ds(top, degrees - top)

    def zcopy(f, dest, low, source):
        return pltpu.make_async_remote_copy(
            src_ref=fields[f].at[:, dest, :, :, lanes(low)],
            dst_ref=rx.at[me, f, :, :, :, lanes(low)],
            send_sem=zss.at[dest, f], recv_sem=zrs.at[source, f],
            device_id=mate(dest), device_id_type=MESH,
        )

    def relay(f, source, yy):
        slot = rx.at[source * groups + yy, f, :, :, :, lanes(whole[source])]
        return pltpu.make_async_remote_copy(
            src_ref=slot, dst_ref=slot,
            send_sem=rss.at[source, f], recv_sem=rrs.at[source, f],
            device_id=partner, device_id_type=MESH,
        )

    def pcopy(f, dest, source):
        return pltpu.make_async_remote_copy(
            src_ref=pack.at[f, :, dest], dst_ref=rxp.at[y, f],
            send_sem=pss.at[dest, f], recv_sem=prs.at[f],
            device_id=mate(dest), device_id_type=MESH,
        )

    def relay_packed(f, yy):
        return pltpu.make_async_remote_copy(
            src_ref=rxp.at[yy, f], dst_ref=rxp.at[yy, f],
            send_sem=qss.at[f], recv_sem=qrs.at[f],
            device_id=partner, device_id_type=MESH,
        )

    def local_copy(f):
        return pltpu.make_async_copy(fields[f].at[:, z], rx.at[me, f], lsem.at[f])

    def held_copy(f):
        return pltpu.make_async_copy(fields[f], held.at[f], vsem.at[f])

    consts = [
        pltpu.make_async_copy(src, dst, csem.at[i]) for i, (src, dst) in enumerate((
            (x_hbm.at[core], x_ref), (sect_hbm.at[core], sect_ref), (unscale_hbm.at[core], unscale_ref),
            (w_hbm.at[core], w_ref), (trig_hbm, trig_ref), (back_hbm, back_ref)))
    ]
    for copy in consts:
        copy.start()
    for f in range(2):
        held_copy(f).start()

    @pl.when(straight)
    def _():
        for f in range(4):
            local_copy(f).start()

    pl.semaphore_wait(barrier, harm - 1 + 2 + shells * jnp.where(straight, 0, 1))

    def dest_of(j):
        mark = shells - 1 - j
        return mark - jnp.where(mark <= z, 1, 0)

    is_whole = jnp.logical_and(z * block < top, jnp.logical_not(packs))

    def routed(phase, send):
        for j in range(shells - 1):
            if j == 0:
                if phase == 0:
                    send(dest_of(j))
            else:
                crossing = jnp.logical_and(z * block < top, dest_of(j) * block >= top)

                @pl.when(crossing == (phase == 1))
                def _(j=j):
                    send(dest_of(j))
        if phase == 0:
            @pl.when(jnp.logical_not(straight))
            def _():
                send(z)

    def plain_sends(phase, act, early=None):
        for low in (True, False):
            if early is not None and early == low:
                continue

            @pl.when(is_whole == low)
            def _(low=low):
                routed(phase, lambda dest: [act(zcopy(f, dest, low, z)) for f in range(4)])

    def packed_sends(phase, act):
        @pl.when(packs)
        def _():
            routed(phase, lambda dest: [act(pcopy(f, dest, z)) for f in range(4)])

    def begin(copy):
        copy.start()

    plain_sends(0, begin)

    @pl.when(packs)
    def _():
        for f in range(2, 4):
            held_copy(f).start()
        for f in range(4):
            held_copy(f).wait()
            for c in range(3):
                for shell in range(shells):
                    first, second = held[f, c, shell, 0, :, 0:top], held[f, c, shell, 1, :, 0:top]
                    pack[f, c, shell] = jnp.concatenate([second[:, mid:], first[:, mid:]], axis=1)

        @pl.when(straight)
        def _():
            for f in range(4):
                rxp[core, f] = pack[f, :, z]

    packed_sends(0, begin)

    def energy_copy(step):
        peer = lax.rem(me + step, harm)
        return pltpu.make_async_remote_copy(
            src_ref=energy_all.at[me], dst_ref=energy_all.at[me],
            send_sem=esend.at[step], recv_sem=erecv.at[step],
            device_id={"harm": peer}, device_id_type=MESH,
        )

    def pass_on(source):
        for f in range(4):
            @pl.when(jnp.logical_and(straight, z == source))
            def _(f=f):
                local_copy(f).wait()

            @pl.when(jnp.logical_not(jnp.logical_and(straight, z == source)))
            def _(f=f):
                zcopy(f, source, whole[source], source).wait_recv()
                if packed[source]:
                    pcopy(f, source, source).wait_recv()

            relay(f, source, core).start()
            if packed[source]:
                relay_packed(f, core).start()

    for copy in consts[:3]:
        copy.wait()
    x = x_ref[0:1, :]
    width = x.shape[1]
    per = 16

    def table_block(source, starting, step, carry):
        first = source * block
        order = (first + lax.broadcasted_iota(jnp.int32, (block, width), 0)).astype(F32)
        square = order * order
        latest, before, inverse = carry
        for inner in range(per):
            degree = step * per + inner
            lf = jnp.full((1, width), degree, jnp.int32).astype(F32)
            scale = 1.0 / (4.0 * lf * lf - 1.0)
            gap = lf * lf - square
            if starting:
                gap = jnp.maximum(gap, 1.0)
            dd = gap * scale
            guess = lax.rsqrt(dd)
            guess = guess * (1.5 - 0.5 * dd * guess * guess)
            root = dd * guess
            if starting:
                live = lf > order
                guess = jnp.where(live, guess, 0.0)
                root = jnp.where(live, root, 0.0)
            new = guess * (x * latest - inverse * before)
            if starting:
                new = new + jnp.where(lf == order, sect_ref[pl.ds(first, block), :], 0.0)
            rows[inner] = new * unscale_ref[pl.ds(first, block), :]
            before, latest = latest, new
            inverse = root
        here = pl.ds(pl.multiple_of(step * per, per), per)
        tab[pl.ds(first, block), here, :] = jnp.swapaxes(rows[...], 0, 1).astype(BF)
        return latest, before, inverse

    def table_start(source):
        first = source * block
        floor = 0 if low_half[source] else top
        if first > floor:
            tab[pl.ds(first, block), pl.ds(floor, first - floor), :] = jnp.zeros((block, first - floor, width), BF)
        zero = jnp.zeros((block, width), F32)
        return lax.fori_loop(
            first // per, (first + block) // per, functools.partial(table_block, source, True), (zero, zero, zero))

    def table_rest(source, carry, low, high):
        return lax.fori_loop(low, high, functools.partial(table_block, source, False), carry)

    steps = degrees // per
    for source in reversed(range(shells)):
        carry = table_start(source)
        first = (source + 1) * block // per
        turn = first + (steps - first) // 4 if source == 0 else steps
        carry = lax.fori_loop(first, turn, functools.partial(table_block, source, False), carry)
        if source == 1:
            plain_sends(1, begin, early=True)
            packed_sends(1, begin)
        if source == 0:
            plain_sends(1, begin, early=False)
            lax.fori_loop(turn, steps, functools.partial(table_block, source, False), carry)

    @pl.when(jnp.logical_not(packs))
    def _():
        for f in range(2):
            held_copy(f).wait()

    own_order = me * modes + lax.broadcasted_iota(jnp.int32, (modes, degrees), 0)
    degree = lax.broadcasted_iota(jnp.int32, (modes, degrees), 1)
    share = jnp.where(degree >= own_order, 1.0 / (2.0 * degree.astype(F32) + 1.0), 0.0)
    parts = (share * jnp.where(own_order == 0, 0.5, 1.0), share * jnp.where(own_order == 0, 0.0, 1.0))

    def shell_energy(shell, _):
        for f in range(2):
            total = jnp.zeros((modes, degrees), F32)
            for r in range(2):
                square = jnp.zeros((modes, degrees), F32)
                for c in range(3):
                    value = held[f, c, shell, r].astype(F32)
                    square = square + value * value
                total = total + square * parts[r]
            energy_all[me, f, pl.ds(shell, 1), :] = jnp.sum(total, axis=0, keepdims=True)
        return 0

    lax.fori_loop(0, shells, shell_energy, 0)
    for step in range(1, harm):
        energy_copy(step).start()

    lane = lax.broadcasted_iota(jnp.int32, (24, degrees), 1) % 2
    half_modes = modes // 2

    def transform(source, yy):
        b = source * groups + yy
        cut = slice(0, degrees) if low_half[source] else slice(top, degrees)
        direct = slice(0, degrees) if whole[source] else slice(top, degrees)
        cs[:, :, direct] = jnp.swapaxes(
            rx[b].reshape(24, modes, degrees)[:, :, direct].astype(F32), 0, 1)
        if packed[source]:
            first = rxp[yy].reshape(12, 1, modes, top).astype(F32)
            second = jnp.concatenate([first[..., mid:], first[..., :mid]], axis=3)
            both = jnp.concatenate([first, second], axis=1).reshape(24, modes, top)
            cs[:, :, 0:top] = jnp.swapaxes(both, 0, 1)
        for par in range(2):
            for i in range(half_modes):
                c = cs[2 * i + par, :, cut]
                even = lane[:, cut] == par
                left = jnp.concatenate([jnp.where(even, c, 0.0), jnp.where(even, 0.0, c)], axis=0).astype(BF)
                m = b * modes + 2 * i + par
                eo = jnp.dot(left, tab[m, cut, :], preferred_element_type=F32)
                outs[i] = jnp.concatenate([eo[:24] + eo[24:], eo[:24] - eo[24:]], axis=1)
            turned = jnp.swapaxes(outs[...], 0, 1).astype(BF)
            for k in range(24):
                c, r = k // 2, k % 2
                here = pl.ds(pl.multiple_of(r * top + b * half_modes, half_modes), half_modes)
                modes_buf[par, c, here, :] = turned[k]

    def partner_block(source):
        for f in range(4):
            relay(f, source, other).wait_recv()
            if packed[source]:
                relay_packed(f, other).wait_recv()
        transform(source, other)

    def own_block(source):
        transform(source, core)

    near = list(reversed(range(shells // 2, shells)))
    far = list(range(shells // 2))
    for i, source in enumerate(near):
        pass_on(source)
        if i > 0:
            partner_block(near[i - 1])
        own_block(source)
    partner_block(near[-1])
    for source in far:
        pass_on(source)
        own_block(source)
        partner_block(source)

    for copy in consts[3:]:
        copy.wait()

    piece = 16

    def product_rows(i, _):
        at_rows = pl.ds((i // 2) * piece, piece)
        at_lanes = pl.ds((i % 2) * width, width)
        e = [grid[0, c, at_rows, at_lanes] for c in range(12)]
        o = [grid[1, c, at_rows, at_lanes] for c in range(12)]
        sides = []
        for g in ([a + d for a, d in zip(e, o)], [a - d for a, d in zip(e, o)]):
            u, b, w, j = g[0:3], g[3:6], g[6:9], g[9:12]
            lamb, lorentz, induced = cross(u, w), cross(j, b), cross(u, b)
            sides.append([lamb[n] + lorentz[n] for n in range(3)] + induced)
        for c in range(6):
            prod[0, c, at_rows, at_lanes] = (sides[0][c] + sides[1][c]).astype(BF)
            prod[1, c, at_rows, at_lanes] = (sides[0][c] - sides[1][c]).astype(BF)
        return 0


    span = points // 2 // 3
    for part in range(3):
        at_part = slice(part * span, (part + 1) * span)
        for c in range(12):
            for par in range(2):
                grid[par, c, at_part] = jnp.dot(
                    trig_ref[par, at_part], modes_buf[par, c], preferred_element_type=F32)
        if part > 0:
            for i in range((part - 1) * span // piece * 2, part * span // piece * 2):
                product_rows(i, 0)
    for i in range(2 * span // piece * 2, 3 * span // piece * 2):
        product_rows(i, 0)

    def analyse(c, _):
        for par in range(2):
            a = jnp.dot(back_ref[par], prod[par, c], preferred_element_type=F32)
            a = a * w_ref[0:1, :]
            plus, minus = a[:, :width] + a[:, width:], a[:, :width] - a[:, width:]
            for r in range(2):
                cut = slice(r * top, (r + 1) * top)
                asc[par, 2 * c + r] = plus[cut]
                asc[par, 16 + 2 * c + r] = minus[cut]
        return 0

    lax.fori_loop(0, 6, analyse, 0, unroll=True)

    out_lane = lax.broadcasted_iota(jnp.int32, (16, degrees), 1) % 2

    sides = (slice(0, top), slice(top, degrees), slice(0, degrees))

    def spectrum(b, part):
        cut = sides[part]
        for par in range(2):
            here = pl.ds(pl.multiple_of(b * half_modes, half_modes), half_modes)
            turned = jnp.swapaxes(asc[par, :, here, :], 0, 1).astype(BF)
            for i in range(half_modes):
                m = b * modes + 2 * i + par
                both = lax.dot_general(
                    turned[i], tab[m, cut, :], (((1,), (1,)), ((), ())), preferred_element_type=F32)
                souts[2 * i + par, :, cut] = jnp.where(out_lane[:, cut] == par, both[:16], both[16:])
        return jnp.swapaxes(souts[:, :, cut], 0, 1)[:12]

    def ycopy(target, part):
        here = pl.ds(0, degrees) if part == 2 else pl.ds(part * top, top)
        return pltpu.make_async_remote_copy(
            src_ref=ysend.at[target, :, :, here], dst_ref=yrecv.at[target, :, :, here],
            send_sem=yss.at[target, part % 2], recv_sem=yrs.at[target, part % 2],
            device_id=partner, device_id_type=MESH,
        )

    def bcopy(target, shell, part):
        here = pl.ds(part * top, top)
        return pltpu.make_async_remote_copy(
            src_ref=zsend.at[target, :, :, :, here], dst_ref=land.at[shell, :, :, :, here],
            send_sem=bss.at[target, part], recv_sem=brs.at[shell, part],
            device_id=mate(target), device_id_type=MESH,
        )

    def bpack(target, shell):
        return pltpu.make_async_remote_copy(
            src_ref=zpack, dst_ref=landp.at[shell],
            send_sem=bps.at[0], recv_sem=bpr.at[shell],
            device_id=mate(target), device_id_type=MESH,
        )

    @pl.when(z * block >= top)
    def _():
        land[:, :, :, :, 0:top] = jnp.zeros((shells, 6, 2, modes, top), BF)

    def returned(target, part, shell):
        copies = []
        if part != 0:
            copies.append(bcopy(target, shell, 1))
        if part != 1:
            copies.append(bpack(target, shell) if packed[target] else bcopy(target, shell, 0))
        return copies

    def finish(target, part):
        cut = sides[part]
        ycopy(target, part).wait_recv()
        total = (own[target, :, :, cut] + yrecv[target, :, :, cut].astype(F32)).astype(BF)
        total = total.reshape(6, 2, modes, total.shape[-1])
        stays = jnp.logical_and(straight, z == target)

        @pl.when(stays)
        def _():
            land[target, :, :, :, cut] = total

        @pl.when(jnp.logical_not(stays))
        def _():
            zsend[target, :, :, :, cut] = total
            if part != 1 and packed[target]:
                zpack[...] = jnp.concatenate([total[:, 1, :, mid:top], total[:, 0, :, mid:top]], axis=2)
            for copy in returned(target, part, z):
                copy.start()

    upper = lax.broadcasted_iota(jnp.int32, (modes, top), 1) >= mid

    def arrived(shell):
        moved = jnp.logical_not(jnp.logical_and(straight, z == shell))
        @pl.when(moved)
        def _():
            bcopy(shell, shell, 1).wait_recv()

        @pl.when(jnp.logical_and(moved, is_whole))
        def _():
            bcopy(shell, shell, 0).wait_recv()

        @pl.when(jnp.logical_and(moved, packs))
        def _():
            bpack(shell, shell).wait_recv()
            for k in range(6):
                first = landp[shell, k].astype(F32)
                second = jnp.concatenate([first[:, mid:], first[:, :mid]], axis=1)
                land[shell, k, 0, :, 0:top] = jnp.where(upper, first, 0.0).astype(BF)
                land[shell, k, 1, :, 0:top] = jnp.where(upper, second, 0.0).astype(BF)

    def hcopy(side):
        shell = shells - 1 if side == 0 else 0
        return pltpu.make_async_remote_copy(
            src_ref=land.at[shell, pl.ds(3, 3)], dst_ref=halo.at[side],
            send_sem=hss.at[side], recv_sem=hrs.at[side],
            device_id=rad_up if side == 0 else rad_down, device_id_type=MESH,
        )

    def out_copy(shell):
        return pltpu.make_async_copy(land.at[shell], land_out.at[:, shell], osem.at[shell])

    def halo_copy(side):
        return pltpu.make_async_copy(halo.at[side], halo_out.at[side], osem.at[shells + side])

    def edges_out():
        arrived(shells - 1)
        hcopy(0).start()
        out_copy(shells - 1).start()
        arrived(0)
        hcopy(1).start()
        out_copy(0).start()

    late = z == shells // 2
    pieces = [(0, 1), (0, 0)] + [(target, 2 if low_half[target] else 1) for target in range(1, shells)]
    for i, (target, part) in enumerate(pieces):
        ysend[target, :, :, sides[part]] = spectrum(target * groups + other, part).astype(BF)
        ycopy(target, part).start()
        if i > 0:
            finish(*pieces[i - 1])
        own[target, :, :, sides[part]] = spectrum(target * groups + core, part)
        if i == len(pieces) - 2:
            pl.when(late)(edges_out)
    finish(*pieces[-1])
    pl.when(jnp.logical_not(late))(edges_out)

    for step in range(1, harm):
        energy_copy(step).wait_recv()
    energy_out[...] = jnp.sum(energy_all[...], axis=0)
    energy_done = pltpu.make_async_copy(energy_out, energy_hbm, osem.at[shells + 2])
    energy_done.start()
    for shell in range(1, shells - 1):
        arrived(shell)
        out_copy(shell).start()
    for side in range(2):
        hcopy(side).wait_recv()
        halo_copy(side).start()
    for shell in range(shells):
        out_copy(shell).wait()
    for side in range(2):
        halo_copy(side).wait()
    energy_done.wait()
    hcopy(0).wait_send()
    hcopy(1).wait_send()
    for step in range(1, harm):
        energy_copy(step).wait_send()
    def ended(copy):
        copy.wait_send()

    for phase in range(2):
        plain_sends(phase, ended)
        packed_sends(phase, ended)
    for source in range(shells):
        for f in range(4):
            relay(f, source, core).wait_send()
            if packed[source]:
                relay_packed(f, core).wait_send()

    for target, part in pieces:
        ycopy(target, part).wait_send()

        @pl.when(jnp.logical_not(jnp.logical_and(straight, z == target)))
        def _(target=target, part=part):
            for copy in returned(target, part, z):
                copy.wait_send()


def closing_kernel(
    rads, shells, landed, halo, energy, adv_out, grad_out, energy_out, adv, ind, grad, rim, total, isem, osem
):
    rad = lax.axis_index("rad")
    copy = pltpu.make_async_copy
    halos = copy(halo, rim, isem.at[0])
    induced = [copy(landed.at[pl.ds(3, 3), s], ind.at[:, s], isem.at[3 + s]) for s in range(shells)]
    advected = copy(landed.at[pl.ds(0, 3)], adv, isem.at[1])
    energies = copy(energy, total, isem.at[2])
    advected.start()
    energies.start()
    halos.start()
    for shell in induced:
        shell.start()
    outs = [copy(grad.at[:, s], grad_out.at[:, s], osem.at[2 + s]) for s in range(shells)]
    outs += [copy(adv, adv_out, osem.at[0]), copy(total, energy_out, osem.at[1])]
    advected.wait()
    outs[shells].start()
    energies.wait()
    outs[shells + 1].start()
    halos.wait()
    induced[0].wait()
    for s in range(shells):
        if s + 1 < shells:
            induced[s + 1].wait()
            after = ind[:, s + 1].astype(F32)
        else:
            after = jnp.where(rad < rads - 1, rim[1].astype(F32), 0.0)
        before = ind[:, s - 1].astype(F32) if s > 0 else jnp.where(rad > 0, rim[0].astype(F32), 0.0)
        grad[:, s] = ((after - before) * 0.5).astype(BF)
        outs[s].start()
    for out in outs:
        out.wait()


def local_relay(velocity, magnetic, vorticity, current):
    harm, rads = lax.axis_size("harm"), lax.axis_size("rad")
    _, shells, _, modes, degrees = velocity.shape
    thetas, points = 3 * degrees // 2, 3 * degrees
    groups = harm // shells
    x, sect, unscale, w, synthesis, analysis = relay_tables(degrees, thetas, points, groups)
    width = x.shape[2]
    block = groups * modes
    hbm = pl.BlockSpec(memory_space=pl.ANY)
    dims = (rads, harm, shells, groups, modes, degrees, thetas, points)
    dma = pltpu.SemaphoreType.DMA
    consts = (x, sect, unscale, w, synthesis, analysis)
    landed, halo, energy = pl.pallas_call(
        functools.partial(relay_kernel, dims),
        name="dynamo",
        out_shape=(
            jax.ShapeDtypeStruct((6, shells, 2, modes, degrees), BF),
            jax.ShapeDtypeStruct((2, 3, 2, modes, degrees), BF),
            jax.ShapeDtypeStruct((2, shells, degrees), F32),
        ),
        in_specs=[hbm] * 10,
        out_specs=(hbm, hbm, hbm),
        scratch_shapes=[
            *(pltpu.VMEM(c.shape[1:], c.dtype) for c in consts[:4]),
            *(pltpu.VMEM(c.shape, c.dtype) for c in consts[4:]),
            pltpu.VMEM((degrees, degrees, width), BF),
            pltpu.VMEM((16, block, width), F32),
            pltpu.VMEM((harm, 4, 3, 2, modes, degrees), BF),
            pltpu.VMEM((modes, 24, degrees), F32),
            pltpu.VMEM((modes // 2, 24, 2 * width), F32),
            pltpu.VMEM((2, 12, degrees, 2 * width), BF),
            pltpu.VMEM((2, 12, points // 2, 2 * width), F32),
            pltpu.VMEM((2, 6, points // 2, 2 * width), BF),
            pltpu.VMEM((2, 32, degrees // 2, width), F32),
            pltpu.VMEM((modes, 16, degrees), F32),
            pltpu.VMEM((shells, 12, modes, degrees), F32),
            pltpu.VMEM((shells, 12, modes, degrees), BF),
            pltpu.VMEM((shells, 12, modes, degrees), BF),
            pltpu.VMEM((shells, 6, 2, modes, degrees), BF),
            pltpu.VMEM((shells, 6, 2, modes, degrees), BF),
            pltpu.VMEM((2, 3, 2, modes, degrees), BF),
            pltpu.VMEM((harm, 2, shells, degrees), F32),
            pltpu.VMEM((4,) + velocity.shape, BF),
            pltpu.VMEM((4, 3, shells, modes, degrees // 2), BF),
            pltpu.VMEM((groups, 4, 3, modes, degrees // 2), BF),
            pltpu.VMEM((6, modes, degrees // 2), BF),
            pltpu.VMEM((shells, 6, modes, degrees // 2), BF),
            pltpu.VMEM((2, shells, degrees), F32),
            dma((6,)), dma((shells + 3,)), dma((4,)), dma((4,)), dma((shells, 4)), dma((shells, 4)), dma((shells, 4)), dma((shells, 4)),
            dma((shells, 2)), dma((shells, 2)), dma((shells, 2)), dma((shells, 2)),
            dma((2,)), dma((2,)), dma((harm,)), dma((harm,)),
            dma((shells, 4)), dma((4,)), dma((4,)), dma((4,)), dma((1,)), dma((shells,)),
        ],
        compiler_params=pltpu.CompilerParams(
            collective_id=0, has_side_effects=True, vmem_limit_bytes=62 * 1024 * 1024
        ),
    )(velocity, magnetic, vorticity, current, *(jnp.asarray(c) for c in consts))

    half = (3,) + landed.shape[1:]
    return pl.pallas_call(
        functools.partial(closing_kernel, rads, shells),
        name="closing",
        out_shape=(
            jax.ShapeDtypeStruct(half, BF),
            jax.ShapeDtypeStruct(half, BF),
            jax.ShapeDtypeStruct(energy.shape, F32),
        ),
        in_specs=[hbm] * 3,
        out_specs=(hbm, hbm, hbm),
        scratch_shapes=[
            pltpu.VMEM(half, BF), pltpu.VMEM(half, BF), pltpu.VMEM(half, BF),
            pltpu.VMEM(halo.shape, BF), pltpu.VMEM(energy.shape, F32), dma((5 + shells,)), dma((2 + shells,)),
        ],
    )(landed, halo, energy)


def relay_fits(mesh, args):
    _, total, _, degrees, _ = args[0].shape
    rads, harm = mesh.shape["rad"], mesh.shape["harm"]
    shells, modes = total // rads, degrees // harm
    return harm == 2 * shells and rads > 2 and rads % 2 == 0 and modes % 32 == 0 and degrees % (2 * LANES) == 0


def solution(mesh):
    spec = P(None, "rad", None, "harm", None)

    def run(*args):
        body = local_relay if relay_fits(mesh, args) else local
        return jax.shard_map(
            body,
            mesh=mesh,
            in_specs=(spec,) * 4,
            out_specs=(spec, spec, P(None, "rad", None)),
            check_vma=False,
        )(*args)

    return run
```
